16 devices in a mesh: dp: 2 (over y, z), tp: 8 (over x, core).
Axes of the slice: x: 4, y: 2, z: 1, core: 2. Of those that a mesh axis runs over, the one named last changes fastest.
The devices are a block of a 4x4x8 slice.
Arguments:
- x_in: bfloat16 [3072, 3072], P(('dp', 'tp')), parts along dimension 0
- grad_y: bfloat16 [3072, 3072], P(('dp', 'tp')), parts along dimension 0
- norm_gain: float32 [2, 3072], replicated
- w_qkv: bfloat16 [2, 3072, 5120], P(None, None, 'tp')
- w_out: bfloat16 [2, 3072, 3072], P(None, 'tp')
- w_gate: bfloat16 [2, 3072, 8192], P(None, None, 'tp')
- w_up: bfloat16 [2, 3072, 8192], P(None, None, 'tp')
- w_down: bfloat16 [2, 8192, 3072], P(None, 'tp')
Outputs:
- output 1: bfloat16 [3072, 3072], P(('dp', 'tp')), parts along dimension 0
- output 2: float32 [4, 3072], P('dp'), parts along dimension 0
- output 3: bfloat16 [4, 3072, 5120], P('dp', None, 'tp'), parts along dimension 0
- output 4: bfloat16 [4, 3072, 3072], P('dp', 'tp'), parts along dimension 0
- output 5: bfloat16 [4, 3072, 8192], P('dp', None, 'tp'), parts along dimension 0
- output 6: bfloat16 [4, 3072, 8192], P('dp', None, 'tp'), parts along dimension 0
- output 7: bfloat16 [4, 8192, 3072], P('dp', 'tp'), parts along dimension 0
There are 2 independent parts. The reference program is written for one: setup_inputs(seed, part) draws one part's arguments, and reference() takes and returns one part's arrays. A program takes and returns all parts, laid end to end along the dimension named above; an argument that names none is the same for every part.
All inputs are finite; a program needn't handle non-finite values.
Results may differ from the reference program's by a relative error of at most 0.0172757.
Values are sent between devices in bfloat16 or wider.
A program may use at most 768 MiB of HBM per device.

```python
import jax
import jax.numpy as jnp
from jax import lax

SEQ_LEN = 1536
D_MODEL = 3072
D_FF = 8192
HEADS = 24
KV_HEADS = 8
HEAD_DIM = 128
LAYERS = 2

GROUP_SIZE = HEADS // KV_HEADS
QKV_COLS = (HEADS + 2 * KV_HEADS) * HEAD_DIM
NORM_EPS = 1e-5
ROPE_BASE = 10000.0


def setup_inputs(seed: int = 0, part: int = 0) -> dict:
    data_keys = jax.random.split(jax.random.fold_in(jax.random.key(seed), part), 2)
    weight_keys = jax.random.split(jax.random.key(seed + 1), 6)
    x_in = jax.random.normal(data_keys[0], (SEQ_LEN, D_MODEL), jnp.float32)
    grad_y = jax.random.normal(data_keys[1], (SEQ_LEN, D_MODEL), jnp.float32)
    norm_gain = 1.0 + 0.3 * jax.random.normal(weight_keys[0], (LAYERS, D_MODEL), jnp.float32)
    w_qkv = jax.random.normal(weight_keys[1], (LAYERS, D_MODEL, QKV_COLS), jnp.float32) * D_MODEL ** -0.5
    w_out = jax.random.normal(weight_keys[2], (LAYERS, HEADS * HEAD_DIM, D_MODEL), jnp.float32) * (HEADS * HEAD_DIM) ** -0.5
    w_gate = jax.random.normal(weight_keys[3], (LAYERS, D_MODEL, D_FF), jnp.float32) * D_MODEL ** -0.5
    w_up = jax.random.normal(weight_keys[4], (LAYERS, D_MODEL, D_FF), jnp.float32) * D_MODEL ** -0.5
    w_down = jax.random.normal(weight_keys[5], (LAYERS, D_FF, D_MODEL), jnp.float32) * D_FF ** -0.5
    return {'x_in': x_in.astype(jnp.bfloat16), 'grad_y': grad_y.astype(jnp.bfloat16), 'norm_gain': norm_gain, 'w_qkv': w_qkv.astype(jnp.bfloat16), 'w_out': w_out.astype(jnp.bfloat16), 'w_gate': w_gate.astype(jnp.bfloat16), 'w_up': w_up.astype(jnp.bfloat16), 'w_down': w_down.astype(jnp.bfloat16)}


def rope_tables():
    half_dim = HEAD_DIM // 2
    freqs = ROPE_BASE ** (-2.0 * jnp.arange(half_dim, dtype=jnp.float32) / HEAD_DIM)
    angles = jnp.arange(SEQ_LEN, dtype=jnp.float32)[:, None] * freqs[None, :]
    return jnp.cos(angles)[:, None, None, :], jnp.sin(angles)[:, None, None, :]


def rotate(values, cos_tab, sin_tab):
    half_dim = values.shape[-1] // 2
    lower_half = values[..., :half_dim]
    upper_half = values[..., half_dim:]
    return jnp.concatenate([lower_half * cos_tab - upper_half * sin_tab, upper_half * cos_tab + lower_half * sin_tab], axis=-1)


def rms_scale(x_f32, gain_row):
    inv_rms = lax.rsqrt(jnp.mean(x_f32 * x_f32, axis=-1, keepdims=True) + NORM_EPS)
    return x_f32 * inv_rms * gain_row


def group_attention(operands):
    query, keys_rot, values_v = operands
    causal = jnp.arange(SEQ_LEN)[:, None] >= jnp.arange(SEQ_LEN)[None, :]
    scores = jnp.einsum('sgd,td->gst', query.astype(jnp.float32), keys_rot.astype(jnp.float32)) * HEAD_DIM ** -0.5
    attn_prob = jax.nn.softmax(jnp.where(causal, scores, -1e30), axis=-1).astype(jnp.bfloat16)
    return jnp.einsum('gst,td->sgd', attn_prob.astype(jnp.float32), values_v.astype(jnp.float32)).astype(jnp.bfloat16)


def decoder_block(x_cur, gain_row, w_qkv_l, w_out_l, w_gate_l, w_up_l, w_down_l, cos_tab, sin_tab):
    x_f32 = x_cur.astype(jnp.float32)
    normed = rms_scale(x_f32, gain_row).astype(jnp.bfloat16).astype(jnp.float32)
    qkv_all = jnp.dot(normed, w_qkv_l.astype(jnp.float32), preferred_element_type=jnp.float32).astype(jnp.bfloat16)
    qkv_all = qkv_all.reshape(SEQ_LEN, KV_HEADS, GROUP_SIZE + 2, HEAD_DIM)
    rotated = rotate(qkv_all[:, :, :GROUP_SIZE + 1].astype(jnp.float32), cos_tab, sin_tab).astype(jnp.bfloat16)
    operands = (jnp.moveaxis(rotated[:, :, :GROUP_SIZE], 1, 0), jnp.moveaxis(rotated[:, :, GROUP_SIZE], 1, 0), jnp.moveaxis(qkv_all[:, :, GROUP_SIZE + 1], 1, 0))
    attn_out = lax.map(jax.checkpoint(group_attention), operands)
    attn_out = jnp.moveaxis(attn_out, 0, 1).reshape(SEQ_LEN, HEADS * HEAD_DIM)
    gate_act = jnp.dot(normed, w_gate_l.astype(jnp.float32), preferred_element_type=jnp.float32).astype(jnp.bfloat16)
    up_act = jnp.dot(normed, w_up_l.astype(jnp.float32), preferred_element_type=jnp.float32).astype(jnp.bfloat16)
    hidden = (jax.nn.silu(gate_act.astype(jnp.float32)) * up_act.astype(jnp.float32)).astype(jnp.bfloat16)
    block_sum = x_f32 + jnp.dot(attn_out.astype(jnp.float32), w_out_l.astype(jnp.float32), preferred_element_type=jnp.float32) + jnp.dot(hidden.astype(jnp.float32), w_down_l.astype(jnp.float32), preferred_element_type=jnp.float32)
    return block_sum.astype(jnp.bfloat16)


def stack_forward(x_in, norm_gain, w_qkv, w_out, w_gate, w_up, w_down):
    cos_tab, sin_tab = rope_tables()

    def body(x_cur, layer_weights):
        gain_row, w_qkv_l, w_out_l, w_gate_l, w_up_l, w_down_l = layer_weights
        return decoder_block(x_cur, gain_row, w_qkv_l, w_out_l, w_gate_l, w_up_l, w_down_l, cos_tab, sin_tab), None

    return lax.scan(body, x_in, (norm_gain, w_qkv, w_out, w_gate, w_up, w_down))[0]


def reference(x_in, grad_y, norm_gain, w_qkv, w_out, w_gate, w_up, w_down):
    pullback = jax.vjp(stack_forward, x_in, norm_gain, w_qkv, w_out, w_gate, w_up, w_down)[1]
    grad_x, grad_gain, grad_qkv, grad_out, grad_gate, grad_up, grad_down = pullback(grad_y)
    return (grad_x, grad_gain, grad_qkv, grad_out, grad_gate, grad_up, grad_down)
```

```python
import functools

import jax
import jax.numpy as jnp
from jax import lax
from jax.experimental import pallas as pl
from jax.experimental.pallas import tpu as pltpu
from jax.sharding import PartitionSpec as P

HEAD_DIM = 128
NORM_EPS = 1e-5
ROPE_BASE = 10000.0
Q_BLOCK = 256
VMEM_LIMIT = 60 * 1024 * 1024
F32 = jnp.float32
BF16 = jnp.bfloat16

CONTRACT_LAST = (((1,), (1,)), ((), ()))
CONTRACT_FIRST = (((0,), (0,)), ((), ()))
MATMUL = (((1,), (0,)), ((), ()))


def dot(lhs, rhs, dims):
    return lax.dot_general(lhs, rhs, dims, preferred_element_type=F32)


def params():
    return pltpu.CompilerParams(vmem_limit_bytes=VMEM_LIMIT)


def cost(flops, bytes_accessed, transcendentals=0):
    return pl.CostEstimate(flops=int(flops), bytes_accessed=int(bytes_accessed), transcendentals=int(transcendentals))


def rope_tables(seq_len):
    half_dim = HEAD_DIM // 2
    freqs = ROPE_BASE ** (-2.0 * jnp.arange(half_dim, dtype=F32) / HEAD_DIM)
    angles = jnp.arange(seq_len, dtype=F32)[:, None] * freqs[None, :]
    cos, sin = jnp.cos(angles), jnp.sin(angles)
    return jnp.concatenate([cos, cos], axis=-1), jnp.concatenate([-sin, sin], axis=-1)


def rms_scale(x_f32, gain_row):
    inv_rms = lax.rsqrt(jnp.mean(x_f32 * x_f32, axis=-1, keepdims=True) + NORM_EPS)
    return x_f32 * inv_rms * gain_row


def gated(gate_f32, up_f32):
    return jax.nn.silu(gate_f32) * up_f32


def head_cols(index):
    return pl.ds(pl.multiple_of(index * HEAD_DIM, HEAD_DIM), HEAD_DIM)


def diagonal_mask():
    return lax.broadcasted_iota(jnp.int32, (Q_BLOCK, Q_BLOCK), 0) >= lax.broadcasted_iota(jnp.int32, (Q_BLOCK, Q_BLOCK), 1)


def attn_fwd_kernel(group, qkv_ref, cos_ref, sin_ref, rot_ref, out_ref, lse_ref):
    seq_len = qkv_ref.shape[0]
    scale = HEAD_DIM ** -0.5
    key, val = pl.ds(group * HEAD_DIM, HEAD_DIM), pl.ds((group + 1) * HEAD_DIM, HEAD_DIM)

    def rotate_head(head, carry):
        values = qkv_ref[:, head_cols(head)].astype(F32)
        rot_ref[:, head_cols(head)] = (values * cos_ref[...] + pltpu.roll(values, HEAD_DIM // 2, 1) * sin_ref[...]).astype(BF16)
        return carry

    lax.fori_loop(0, group + 1, rotate_head, 0)
    rot_ref[:, val] = qkv_ref[:, val]
    for block in range(seq_len // Q_BLOCK):
        start = block * Q_BLOCK
        rows = pl.ds(start, Q_BLOCK)

        def one_head(head, carry):
            query = rot_ref[rows, head_cols(head)]
            diag = jnp.where(diagonal_mask(), dot(query, rot_ref[rows, key], CONTRACT_LAST) * scale, -1e30)
            row_max = jnp.max(diag, axis=-1, keepdims=True)
            if start:
                past = dot(query, rot_ref[pl.ds(0, start), key], CONTRACT_LAST) * scale
                row_max = jnp.maximum(row_max, jnp.max(past, axis=-1, keepdims=True))
            diag = jnp.exp(diag - row_max)
            total = jnp.sum(diag, axis=-1, keepdims=True)
            if start:
                past = jnp.exp(past - row_max)
                total = total + jnp.sum(past, axis=-1, keepdims=True)
            inverse = 1.0 / total
            acc = dot((diag * inverse).astype(BF16), rot_ref[rows, val], MATMUL)
            if start:
                acc = acc + dot((past * inverse).astype(BF16), rot_ref[pl.ds(0, start), val], MATMUL)
            out_ref[rows, head_cols(head)] = acc.astype(BF16)
            lse_ref[rows, head_cols(head)] = jnp.broadcast_to(row_max + jnp.log(total), (Q_BLOCK, HEAD_DIM))
            return carry

        lax.fori_loop(0, group, one_head, 0)


def attn_fwd(qkv, cos_tab, sin_tab, group):
    seq_len = qkv.shape[0]
    pairs = group * seq_len * seq_len
    return pl.pallas_call(
        functools.partial(attn_fwd_kernel, group),
        out_shape=(
            jax.ShapeDtypeStruct(qkv.shape, BF16),
            jax.ShapeDtypeStruct((seq_len, group * HEAD_DIM), BF16),
            jax.ShapeDtypeStruct((seq_len, group * HEAD_DIM), F32),
        ),
        compiler_params=params(),
        cost_estimate=cost(4 * pairs * HEAD_DIM, 8 * qkv.size, pairs // 2),
        name="attn_fwd",
    )(qkv, cos_tab, sin_tab)


def attn_bwd_kernel(group, rot_ref, lse_ref, dout_ref, cos_ref, sin_ref, dqkv_ref, dkey_ref, dval_ref):
    seq_len = rot_ref.shape[0]
    scale = HEAD_DIM ** -0.5
    key, val = pl.ds(group * HEAD_DIM, HEAD_DIM), pl.ds((group + 1) * HEAD_DIM, HEAD_DIM)
    dkey_ref[...] = jnp.zeros_like(dkey_ref)
    dval_ref[...] = jnp.zeros_like(dval_ref)

    def unrotate(values, rows):
        values = values.astype(BF16).astype(F32)
        return (values * cos_ref[rows, :] - pltpu.roll(values, HEAD_DIM // 2, 1) * sin_ref[rows, :]).astype(BF16)

    for block in range(seq_len // Q_BLOCK):
        start = block * Q_BLOCK
        rows = pl.ds(start, Q_BLOCK)

        def one_head(head, carry):
            query = rot_ref[rows, head_cols(head)]
            dout = dout_ref[rows, head_cols(head)]
            lse = lse_ref[rows, head_cols(head)][:, :1]

            def probs(cols, masked):
                scores = dot(query, rot_ref[cols, key], CONTRACT_LAST) * scale
                if masked:
                    scores = jnp.where(diagonal_mask(), scores, -1e30)
                prob = jnp.exp(scores - lse)
                dprob = dot(dout, rot_ref[cols, val], CONTRACT_LAST).astype(BF16).astype(F32)
                dval_ref[cols, :] += dot(prob.astype(BF16), dout, CONTRACT_FIRST)
                return prob, dprob, jnp.sum(prob * dprob, axis=-1, keepdims=True)

            def finish(cols, prob, dprob, delta):
                dscore = (prob * (dprob - delta) * scale).astype(BF16)
                dkey_ref[cols, :] += dot(dscore, query, CONTRACT_FIRST)
                return dot(dscore, rot_ref[cols, key], MATMUL)

            prob, dprob, delta = probs(rows, True)
            if start:
                past = pl.ds(0, start)
                past_prob, past_dprob, past_delta = probs(past, False)
                delta = delta + past_delta
            dquery = finish(rows, prob, dprob, delta)
            if start:
                dquery = dquery + finish(past, past_prob, past_dprob, delta)
            dqkv_ref[rows, head_cols(head)] = unrotate(dquery, rows)
            return carry

        lax.fori_loop(0, group, one_head, 0)
    dqkv_ref[:, key] = unrotate(dkey_ref[...], pl.ds(0, seq_len))
    dqkv_ref[:, val] = dval_ref[...].astype(BF16)


def attn_bwd(rot, lse, dout, cos_tab, sin_tab, group):
    seq_len = rot.shape[0]
    pairs = group * seq_len * seq_len
    return pl.pallas_call(
        functools.partial(attn_bwd_kernel, group),
        out_shape=jax.ShapeDtypeStruct(rot.shape, BF16),
        scratch_shapes=[pltpu.VMEM((seq_len, HEAD_DIM), F32)] * 2,
        compiler_params=params(),
        cost_estimate=cost(10 * pairs * HEAD_DIM, 8 * rot.size, pairs // 2),
        name="attn_bwd",
    )(rot, lse, dout, cos_tab, sin_tab)


def sum_of_dots_kernel(dims, n_terms, *refs):
    out_ref = refs[-1]
    total = dot(refs[0][...], refs[n_terms][...], dims)
    for term in range(1, n_terms):
        total = total + dot(refs[term][...], refs[n_terms + term][...], dims)
    out_ref[...] = total


def sum_of_dots(terms, layer, dims, first_col, n_cols, tile, name):
    seq_len = terms[0][0].shape[0]
    flops = sum(2 * seq_len * lhs.shape[1] * n_cols for lhs, _ in terms)
    n_bytes = sum(2 * lhs.shape[1] * (seq_len + n_cols) for lhs, _ in terms) + 4 * seq_len * n_cols
    first_tile = first_col // tile
    lhs_specs = [pl.BlockSpec(lhs.shape, lambda step: (0, 0)) for lhs, _ in terms]
    if dims is MATMUL:
        rhs_specs = [pl.BlockSpec((None, rhs.shape[1], tile), lambda step: (layer, 0, first_tile + step)) for _, rhs in terms]
    else:
        rhs_specs = [pl.BlockSpec((None, tile, rhs.shape[2]), lambda step: (layer, first_tile + step, 0)) for _, rhs in terms]
    return pl.pallas_call(
        functools.partial(sum_of_dots_kernel, dims, len(terms)),
        out_shape=jax.ShapeDtypeStruct((seq_len, n_cols), F32),
        grid=(n_cols // tile,),
        in_specs=lhs_specs + rhs_specs,
        out_specs=pl.BlockSpec((seq_len, tile), lambda step: (0, step)),
        compiler_params=params(),
        cost_estimate=cost(flops, n_bytes),
        name=name,
    )(*[lhs for lhs, _ in terms], *[rhs for _, rhs in terms])


def grad_in_kernel(n_rhs, *refs):
    lhs = refs[0][...]
    rhs_refs, out_refs = refs[1:1 + n_rhs], refs[-n_rhs:]
    for rhs_ref, out_ref in zip(rhs_refs, out_refs):
        out_ref[...] = dot(lhs, rhs_ref[...], CONTRACT_FIRST).astype(BF16)


def grad_in(lhs, rhs_list, layer, n_layers, previous, tile=512):
    seq_len, depth = lhs.shape
    n_rhs = len(rhs_list)
    shapes = tuple(jax.ShapeDtypeStruct((n_layers, depth, rhs.shape[1]), BF16) for rhs in rhs_list)
    width = sum(rhs.shape[1] for rhs in rhs_list)
    aliases = {1 + n_rhs + idx: idx for idx in range(n_rhs)} if previous else {}
    return pl.pallas_call(
        functools.partial(grad_in_kernel, n_rhs),
        out_shape=shapes,
        grid=(depth // tile,),
        in_specs=[pl.BlockSpec((seq_len, tile), lambda step: (0, step))]
        + [pl.BlockSpec(rhs.shape, lambda step: (0, 0)) for rhs in rhs_list]
        + [pl.BlockSpec(memory_space=pl.ANY) for _ in previous],
        out_specs=[pl.BlockSpec((None, tile, rhs.shape[1]), lambda step: (layer, step, 0)) for rhs in rhs_list],
        input_output_aliases=aliases,
        compiler_params=params(),
        cost_estimate=cost(2 * seq_len * depth * width, 2 * (seq_len * depth + seq_len * width + depth * width)),
        name="grad_in",
    )(lhs, *rhs_list, *previous)


def grad_out_kernel(attn_ref, hidden_ref, dy_ref, *refs):
    out_ref, down_ref = refs[-2:]

    @pl.when(pl.program_id(0) == 0)
    def _():
        out_ref[...] = dot(attn_ref[...], dy_ref[...], CONTRACT_FIRST).astype(BF16)

    down_ref[...] = dot(hidden_ref[...], dy_ref[...], CONTRACT_FIRST).astype(BF16)


def grad_out(attn_out, hidden, dy_full, layer, n_layers, previous, tile=512):
    seq_len, depth = dy_full.shape
    heads, ff = attn_out.shape[1], hidden.shape[1]
    return pl.pallas_call(
        grad_out_kernel,
        out_shape=(jax.ShapeDtypeStruct((n_layers, heads, depth), BF16), jax.ShapeDtypeStruct((n_layers, ff, depth), BF16)),
        grid=(ff // tile,),
        in_specs=[
            pl.BlockSpec((seq_len, heads), lambda step: (0, 0)),
            pl.BlockSpec((seq_len, tile), lambda step: (0, step)),
            pl.BlockSpec((seq_len, depth), lambda step: (0, 0), pipeline_mode=pl.Buffered(1)),
        ]
        + [pl.BlockSpec(memory_space=pl.ANY) for _ in previous],
        out_specs=[
            pl.BlockSpec((None, heads, depth), lambda step: (layer, 0, 0)),
            pl.BlockSpec((None, tile, depth), lambda step: (layer, step, 0)),
        ],
        input_output_aliases={3: 0, 4: 1} if previous else {},
        compiler_params=params(),
        cost_estimate=cost(2 * seq_len * depth * (heads + ff), 2 * (seq_len * depth + (seq_len + depth) * (heads + ff))),
        name="grad_out",
    )(attn_out, hidden, dy_full, *previous)


def gather_rows(rows_loc):
    return lax.all_gather(rows_loc, 'tp', axis=0, tiled=True)


def after(value, *others):
    return lax.optimization_barrier((value,) + others)[0]


def reduce_rows(chunks):
    return jnp.concatenate([lax.psum_scatter(chunk, 'tp', scatter_dimension=0, tiled=True) for chunk in chunks], axis=1)


def solution(mesh):
    tp_size = mesh.shape['tp']
    row_spec = P(('dp', 'tp'), None)
    col_spec = P(None, None, 'tp')
    inner_spec = P(None, 'tp', None)

    def sum_over_tp(value):
        stride = 1
        while stride < tp_size:
            value = value + lax.ppermute(value, 'tp', [(idx, idx ^ stride) for idx in range(tp_size)])
            stride *= 2
        return value

    def device_program(x_loc, dy_loc, norm_gain, w_qkv, w_out, w_gate, w_up, w_down):
        n_layers, depth = w_qkv.shape[0], w_qkv.shape[1]
        group = w_out.shape[1] // HEAD_DIM
        seq_len = x_loc.shape[0] * tp_size
        n_chunks = 2
        chunk_cols = depth // n_chunks
        cos_tab, sin_tab = rope_tables(seq_len)
        saved_all = []
        x_cur = x_loc
        dy_full = None
        for layer in range(n_layers):
            last = layer == n_layers - 1
            x_f32 = x_cur.astype(F32)
            u_loc = rms_scale(x_f32, norm_gain[layer]).astype(BF16)
            u_full = gather_rows(u_loc)
            if dy_full is None:
                dy_full = gather_rows(after(dy_loc, u_full))
            qkv = jnp.dot(u_full, w_qkv[layer], preferred_element_type=F32).astype(BF16)
            rot, attn_out, lse = attn_fwd(qkv, cos_tab, sin_tab, group)
            gate = jnp.dot(u_full, w_gate[layer], preferred_element_type=F32).astype(BF16)
            up = jnp.dot(u_full, w_up[layer], preferred_element_type=F32).astype(BF16)
            saved_all.append((x_cur, u_loc, rot, attn_out, lse, gate, up))
            if not last:
                hidden = gated(gate.astype(F32), up.astype(F32)).astype(BF16)
                parts = [
                    sum_of_dots([(attn_out, w_out), (hidden, w_down)], layer, MATMUL, idx * chunk_cols, chunk_cols, 512, "block_out")
                    for idx in range(n_chunks)
                ]
                x_cur = (x_f32 + reduce_rows(parts)).astype(BF16)

        in_grads, out_grads, gain_grads = (), (), []
        for layer in reversed(range(n_layers)):
            x_in, u_loc, rot, attn_out, lse, gate, up = saved_all[layer]
            if layer < n_layers - 1:
                dy_full, in_grads, out_grads = lax.optimization_barrier((gather_rows(dy_loc), in_grads, out_grads))
            d_attn = lax.dot_general(dy_full, w_out[layer], CONTRACT_LAST, preferred_element_type=F32).astype(BF16)
            d_hidden = lax.dot_general(dy_full, w_down[layer], CONTRACT_LAST, preferred_element_type=F32).astype(BF16)
            hidden_f32, gated_pull = jax.vjp(gated, gate.astype(F32), up.astype(F32))
            hidden = hidden_f32.astype(BF16)
            d_gate, d_up = [item.astype(BF16) for item in gated_pull(d_hidden.astype(F32))]
            u_full = gather_rows(after(u_loc, attn_out, d_attn))
            d_qkv = attn_bwd(rot, lse, d_attn, cos_tab, sin_tab, group)
            d_qkv, d_gate, d_up, hidden, u_full = lax.optimization_barrier((d_qkv, d_gate, d_up, hidden, u_full))
            parts = [
                sum_of_dots([(d_qkv, w_qkv), (d_gate, w_gate), (d_up, w_up)], layer, CONTRACT_LAST, idx * chunk_cols, chunk_cols, 512, "block_in_back")
                for idx in range(n_chunks)
            ]
            held = lax.optimization_barrier((parts[-1], d_qkv, d_gate, d_up, hidden, attn_out))
            parts[-1] = held[0]
            in_grads = grad_in(u_full, held[1:4], layer, n_layers, in_grads)
            out_grads = grad_out(held[5], held[4], dy_full, layer, n_layers, out_grads)
            d_normed = reduce_rows(parts).astype(BF16)
            norm_pull = jax.vjp(rms_scale, x_in.astype(F32), norm_gain[layer])[1]
            d_x_norm, gain_grad = norm_pull(d_normed.astype(F32))
            dy_loc = (dy_loc.astype(F32) + d_x_norm).astype(BF16)
            gain_grads.insert(0, gain_grad)
        grad_gain = sum_over_tp(jnp.stack(gain_grads))
        return (dy_loc, grad_gain, in_grads[0], out_grads[0], in_grads[1], in_grads[2], out_grads[1])

    return jax.shard_map(device_program, mesh=mesh, in_specs=(row_spec, row_spec, P(None, None), col_spec, inner_spec, col_spec, col_spec, inner_spec), out_specs=(row_spec, P('dp', None), P('dp', None, 'tp'), P('dp', 'tp', None), P('dp', None, 'tp'), P('dp', None, 'tp'), P('dp', 'tp', None)), check_vma=False)
```

```python
import functools

import jax
import jax.numpy as jnp
from jax import lax
from jax.experimental import pallas as pl
from jax.experimental.pallas import tpu as pltpu
from jax.sharding import PartitionSpec as P

HEAD_DIM = 128
NORM_EPS = 1e-5
ROPE_BASE = 10000.0
Q_BLOCK = 256
VMEM_LIMIT = 60 * 1024 * 1024
F32 = jnp.float32
BF16 = jnp.bfloat16

CONTRACT_LAST = (((1,), (1,)), ((), ()))
CONTRACT_FIRST = (((0,), (0,)), ((), ()))
MATMUL = (((1,), (0,)), ((), ()))


def dot(lhs, rhs, dims):
    return lax.dot_general(lhs, rhs, dims, preferred_element_type=F32)


def params():
    return pltpu.CompilerParams(vmem_limit_bytes=VMEM_LIMIT)


def cost(flops, bytes_accessed, transcendentals=0):
    return pl.CostEstimate(flops=int(flops), bytes_accessed=int(bytes_accessed), transcendentals=int(transcendentals))


def rope_tables(seq_len):
    half_dim = HEAD_DIM // 2
    freqs = ROPE_BASE ** (-2.0 * jnp.arange(half_dim, dtype=F32) / HEAD_DIM)
    angles = jnp.arange(seq_len, dtype=F32)[:, None] * freqs[None, :]
    cos, sin = jnp.cos(angles), jnp.sin(angles)
    return jnp.concatenate([cos, cos], axis=-1), jnp.concatenate([-sin, sin], axis=-1)


def rms_scale(x_f32, gain_row):
    inv_rms = lax.rsqrt(jnp.mean(x_f32 * x_f32, axis=-1, keepdims=True) + NORM_EPS)
    return x_f32 * inv_rms * gain_row


def gated(gate_f32, up_f32):
    return jax.nn.silu(gate_f32) * up_f32


def head_cols(index):
    return pl.ds(pl.multiple_of(index * HEAD_DIM, HEAD_DIM), HEAD_DIM)


def diagonal_mask():
    return lax.broadcasted_iota(jnp.int32, (Q_BLOCK, Q_BLOCK), 0) >= lax.broadcasted_iota(jnp.int32, (Q_BLOCK, Q_BLOCK), 1)


def attn_fwd_kernel(group, qkv_ref, cos_ref, sin_ref, rot_ref, out_ref, lse_ref):
    seq_len = qkv_ref.shape[0]
    scale = HEAD_DIM ** -0.5
    key, val = pl.ds(group * HEAD_DIM, HEAD_DIM), pl.ds((group + 1) * HEAD_DIM, HEAD_DIM)

    def rotate_head(head, carry):
        values = qkv_ref[:, head_cols(head)].astype(F32)
        rot_ref[:, head_cols(head)] = (values * cos_ref[...] + pltpu.roll(values, HEAD_DIM // 2, 1) * sin_ref[...]).astype(BF16)
        return carry

    lax.fori_loop(0, group + 1, rotate_head, 0)
    rot_ref[:, val] = qkv_ref[:, val]
    for block in range(seq_len // Q_BLOCK):
        start = block * Q_BLOCK
        rows = pl.ds(start, Q_BLOCK)

        def one_head(head, carry):
            query = rot_ref[rows, head_cols(head)]
            diag = jnp.where(diagonal_mask(), dot(query, rot_ref[rows, key], CONTRACT_LAST) * scale, -1e30)
            row_max = jnp.max(diag, axis=-1, keepdims=True)
            if start:
                past = dot(query, rot_ref[pl.ds(0, start), key], CONTRACT_LAST) * scale
                row_max = jnp.maximum(row_max, jnp.max(past, axis=-1, keepdims=True))
            diag = jnp.exp(diag - row_max)
            total = jnp.sum(diag, axis=-1, keepdims=True)
            if start:
                past = jnp.exp(past - row_max)
                total = total + jnp.sum(past, axis=-1, keepdims=True)
            inverse = 1.0 / total
            acc = dot((diag * inverse).astype(BF16), rot_ref[rows, val], MATMUL)
            if start:
                acc = acc + dot((past * inverse).astype(BF16), rot_ref[pl.ds(0, start), val], MATMUL)
            out_ref[rows, head_cols(head)] = acc.astype(BF16)
            lse_ref[rows, head_cols(head)] = jnp.broadcast_to(row_max + jnp.log(total), (Q_BLOCK, HEAD_DIM))
            return carry

        lax.fori_loop(0, group, one_head, 0)


def attn_fwd(qkv, cos_tab, sin_tab, group):
    seq_len = qkv.shape[0]
    pairs = group * seq_len * seq_len
    return pl.pallas_call(
        functools.partial(attn_fwd_kernel, group),
        out_shape=(
            jax.ShapeDtypeStruct(qkv.shape, BF16),
            jax.ShapeDtypeStruct((seq_len, group * HEAD_DIM), BF16),
            jax.ShapeDtypeStruct((seq_len, group * HEAD_DIM), F32),
        ),
        compiler_params=params(),
        cost_estimate=cost(4 * pairs * HEAD_DIM, 8 * qkv.size, pairs // 2),
        name="attn_fwd",
    )(qkv, cos_tab, sin_tab)


def attn_bwd_kernel(group, rot_ref, lse_ref, dout_ref, cos_ref, sin_ref, dqkv_ref, dkey_ref, dval_ref):
    seq_len = rot_ref.shape[0]
    scale = HEAD_DIM ** -0.5
    key, val = pl.ds(group * HEAD_DIM, HEAD_DIM), pl.ds((group + 1) * HEAD_DIM, HEAD_DIM)
    dkey_ref[...] = jnp.zeros_like(dkey_ref)
    dval_ref[...] = jnp.zeros_like(dval_ref)

    def unrotate(values, rows):
        values = values.astype(BF16).astype(F32)
        return (values * cos_ref[rows, :] - pltpu.roll(values, HEAD_DIM // 2, 1) * sin_ref[rows, :]).astype(BF16)

    for block in range(seq_len // Q_BLOCK):
        start = block * Q_BLOCK
        rows = pl.ds(start, Q_BLOCK)

        def one_head(head, carry):
            query = rot_ref[rows, head_cols(head)]
            dout = dout_ref[rows, head_cols(head)]
            lse = lse_ref[rows, head_cols(head)][:, :1]

            def probs(cols, masked):
                scores = dot(query, rot_ref[cols, key], CONTRACT_LAST) * scale
                if masked:
                    scores = jnp.where(diagonal_mask(), scores, -1e30)
                prob = jnp.exp(scores - lse)
                dprob = dot(dout, rot_ref[cols, val], CONTRACT_LAST).astype(BF16).astype(F32)
                dval_ref[cols, :] += dot(prob.astype(BF16), dout, CONTRACT_FIRST)
                return prob, dprob, jnp.sum(prob * dprob, axis=-1, keepdims=True)

            def finish(cols, prob, dprob, delta):
                dscore = (prob * (dprob - delta) * scale).astype(BF16)
                dkey_ref[cols, :] += dot(dscore, query, CONTRACT_FIRST)
                return dot(dscore, rot_ref[cols, key], MATMUL)

            prob, dprob, delta = probs(rows, True)
            if start:
                past = pl.ds(0, start)
                past_prob, past_dprob, past_delta = probs(past, False)
                delta = delta + past_delta
            dquery = finish(rows, prob, dprob, delta)
            if start:
                dquery = dquery + finish(past, past_prob, past_dprob, delta)
            dqkv_ref[rows, head_cols(head)] = unrotate(dquery, rows)
            return carry

        lax.fori_loop(0, group, one_head, 0)
    dqkv_ref[:, key] = unrotate(dkey_ref[...], pl.ds(0, seq_len))
    dqkv_ref[:, val] = dval_ref[...].astype(BF16)


def attn_bwd(rot, lse, dout, cos_tab, sin_tab, group):
    seq_len = rot.shape[0]
    pairs = group * seq_len * seq_len
    return pl.pallas_call(
        functools.partial(attn_bwd_kernel, group),
        out_shape=jax.ShapeDtypeStruct(rot.shape, BF16),
        scratch_shapes=[pltpu.VMEM((seq_len, HEAD_DIM), F32)] * 2,
        compiler_params=params(),
        cost_estimate=cost(10 * pairs * HEAD_DIM, 8 * rot.size, pairs // 2),
        name="attn_bwd",
    )(rot, lse, dout, cos_tab, sin_tab)


def sum_of_dots_kernel(dims, n_terms, *refs):
    out_ref = refs[-1]
    total = dot(refs[0][...], refs[n_terms][...], dims)
    for term in range(1, n_terms):
        total = total + dot(refs[term][...], refs[n_terms + term][...], dims)
    out_ref[...] = total


def sum_of_dots(terms, layer, dims, first_col, n_cols, tile, name):
    seq_len = terms[0][0].shape[0]
    flops = sum(2 * seq_len * lhs.shape[1] * n_cols for lhs, _ in terms)
    n_bytes = sum(2 * lhs.shape[1] * (seq_len + n_cols) for lhs, _ in terms) + 4 * seq_len * n_cols
    first_tile = first_col // tile
    lhs_specs = [pl.BlockSpec(lhs.shape, lambda step: (0, 0)) for lhs, _ in terms]
    if dims is MATMUL:
        rhs_specs = [pl.BlockSpec((None, rhs.shape[1], tile), lambda step: (layer, 0, first_tile + step)) for _, rhs in terms]
    else:
        rhs_specs = [pl.BlockSpec((None, tile, rhs.shape[2]), lambda step: (layer, first_tile + step, 0)) for _, rhs in terms]
    return pl.pallas_call(
        functools.partial(sum_of_dots_kernel, dims, len(terms)),
        out_shape=jax.ShapeDtypeStruct((seq_len, n_cols), F32),
        grid=(n_cols // tile,),
        in_specs=lhs_specs + rhs_specs,
        out_specs=pl.BlockSpec((seq_len, tile), lambda step: (0, step)),
        compiler_params=params(),
        cost_estimate=cost(flops, n_bytes),
        name=name,
    )(*[lhs for lhs, _ in terms], *[rhs for _, rhs in terms])


def grad_in_kernel(n_rhs, *refs):
    lhs = refs[0][...]
    rhs_refs, out_refs = refs[1:1 + n_rhs], refs[-n_rhs:]
    for rhs_ref, out_ref in zip(rhs_refs, out_refs):
        out_ref[...] = dot(lhs, rhs_ref[...], CONTRACT_FIRST).astype(BF16)


def grad_in(lhs, rhs_list, layer, n_layers, previous, tile=512):
    seq_len, depth = lhs.shape
    n_rhs = len(rhs_list)
    shapes = tuple(jax.ShapeDtypeStruct((n_layers, depth, rhs.shape[1]), BF16) for rhs in rhs_list)
    width = sum(rhs.shape[1] for rhs in rhs_list)
    aliases = {1 + n_rhs + idx: idx for idx in range(n_rhs)} if previous else {}
    return pl.pallas_call(
        functools.partial(grad_in_kernel, n_rhs),
        out_shape=shapes,
        grid=(depth // tile,),
        in_specs=[pl.BlockSpec((seq_len, tile), lambda step: (0, step))]
        + [pl.BlockSpec(rhs.shape, lambda step: (0, 0)) for rhs in rhs_list]
        + [pl.BlockSpec(memory_space=pl.ANY) for _ in previous],
        out_specs=[pl.BlockSpec((None, tile, rhs.shape[1]), lambda step: (layer, step, 0)) for rhs in rhs_list],
        input_output_aliases=aliases,
        compiler_params=params(),
        cost_estimate=cost(2 * seq_len * depth * width, 2 * (seq_len * depth + seq_len * width + depth * width)),
        name="grad_in",
    )(lhs, *rhs_list, *previous)


def grad_out_kernel(attn_ref, hidden_ref, dy_ref, *refs):
    out_ref, down_ref = refs[-2:]

    @pl.when(pl.program_id(0) == 0)
    def _():
        out_ref[...] = dot(attn_ref[...], dy_ref[...], CONTRACT_FIRST).astype(BF16)

    down_ref[...] = dot(hidden_ref[...], dy_ref[...], CONTRACT_FIRST).astype(BF16)


def grad_out(attn_out, hidden, dy_full, layer, n_layers, previous, tile=512):
    seq_len, depth = dy_full.shape
    heads, ff = attn_out.shape[1], hidden.shape[1]
    return pl.pallas_call(
        grad_out_kernel,
        out_shape=(jax.ShapeDtypeStruct((n_layers, heads, depth), BF16), jax.ShapeDtypeStruct((n_layers, ff, depth), BF16)),
        grid=(ff // tile,),
        in_specs=[
            pl.BlockSpec((seq_len, heads), lambda step: (0, 0)),
            pl.BlockSpec((seq_len, tile), lambda step: (0, step)),
            pl.BlockSpec((seq_len, depth), lambda step: (0, 0), pipeline_mode=pl.Buffered(1)),
        ]
        + [pl.BlockSpec(memory_space=pl.ANY) for _ in previous],
        out_specs=[
            pl.BlockSpec((None, heads, depth), lambda step: (layer, 0, 0)),
            pl.BlockSpec((None, tile, depth), lambda step: (layer, step, 0)),
        ],
        input_output_aliases={3: 0, 4: 1} if previous else {},
        compiler_params=params(),
        cost_estimate=cost(2 * seq_len * depth * (heads + ff), 2 * (seq_len * depth + (seq_len + depth) * (heads + ff))),
        name="grad_out",
    )(attn_out, hidden, dy_full, *previous)


MESH = pl.DeviceIdType.MESH
CORES = 2


def ring_place(chips):
    me = lax.axis_index('tp')
    chip, core = me // CORES, lax.rem(me, CORES)
    left, right = lax.rem(chip + chips - 1, chips), lax.rem(chip + 1, chips)
    return chip, core, (chip * CORES + 1 - core, left * CORES + core, right * CORES + core)


def enter_ring(peers):
    barrier = pltpu.get_barrier_semaphore()
    for peer in peers:
        pl.semaphore_signal(barrier, inc=1, device_id={'tp': peer}, device_id_type=MESH)
    pl.semaphore_wait(barrier, len(peers))


def remote(src, dst, send, recv, index, peer):
    return pltpu.make_async_remote_copy(src_ref=src, dst_ref=dst, send_sem=send.at[index], recv_sem=recv.at[index], device_id={'tp': peer}, device_id_type=MESH)


def ring_gather(chips, loc_ref, full, send, recv, consume):
    n_rows = loc_ref.shape[0]
    half = n_rows // 2
    chip, core, (partner, left, right) = ring_place(chips)
    left_chip, right_chip, far_chip = lax.rem(chip + chips - 1, chips), lax.rem(chip + 1, chips), lax.rem(chip + 2, chips)

    def rows(chip_idx, core_idx, first=0, count=n_rows):
        return full.at[pl.ds(pl.multiple_of((chip_idx * CORES + core_idx) * n_rows + first, half), count)]

    low, high = (0, half), (half, half)
    own_low, own_high = loc_ref.at[pl.ds(0, half)], loc_ref.at[pl.ds(half, half)]
    sends = [
        remote(own_low, rows(chip, core, *low), send, recv, 0, right),
        remote(own_high, rows(chip, core, *high), send, recv, 1, left),
        remote(own_high, rows(chip, core, *high), send, recv, 2, right),
        remote(own_low, rows(chip, core, *low), send, recv, 3, left),
        remote(rows(left_chip, core, *low), rows(left_chip, core, *low), send, recv, 4, right),
        remote(rows(right_chip, core, *high), rows(right_chip, core, *high), send, recv, 5, left),
        remote(loc_ref, rows(chip, core), send, recv, 6, partner),
        remote(rows(left_chip, core), rows(left_chip, core), send, recv, 7, partner),
        remote(rows(right_chip, core), rows(right_chip, core), send, recv, 8, partner),
        remote(rows(far_chip, core), rows(far_chip, core), send, recv, 9, partner),
    ]
    landing = [
        rows(left_chip, core, *low), rows(right_chip, core, *high), rows(left_chip, core, *high), rows(right_chip, core, *low),
        rows(far_chip, core, *low), rows(far_chip, core, *high), rows(chip, 1 - core), rows(left_chip, 1 - core), rows(right_chip, 1 - core),
        rows(far_chip, 1 - core),
    ]

    def arrived(index):
        remote(landing[index], landing[index], send, recv, index, partner).wait_recv()

    enter_ring((partner, left, right))
    for index in (0, 1, 2, 3, 6):
        sends[index].start()
    full[pl.ds(pl.multiple_of((chip * CORES + core) * n_rows, n_rows), n_rows), :] = loc_ref[...]
    arrived(6)
    consume(0, chip)
    arrived(0)
    sends[4].start()
    arrived(1)
    sends[5].start()
    arrived(2)
    sends[7].start()
    arrived(3)
    sends[8].start()
    arrived(7)
    consume(1, left_chip)
    arrived(8)
    consume(2, right_chip)
    arrived(4)
    arrived(5)
    sends[9].start()
    arrived(9)
    consume(3, far_chip)
    for copy in sends:
        copy.wait_send()


def gather_dots_kernel(chips, layer, forward, n_outs, tile, loc_ref, *refs):
    n_weights = 3 if forward else 2
    n_inputs = 3 if forward else 4
    inputs, outs = refs[:n_inputs], refs[n_inputs:n_inputs + n_outs]
    full, scratch = refs[n_inputs + n_outs], refs[n_inputs + n_outs + 1:]
    held, staged = scratch[:n_inputs], scratch[n_inputs:-4]
    load_sem, store_sem, send, recv = scratch[-4:]
    chip_rows = CORES * loc_ref.shape[0]
    loads = [pltpu.make_async_copy(src.at[layer] if idx < n_weights else src, dst, load_sem.at[idx]) for idx, (src, dst) in enumerate(zip(inputs, held))]
    for load in loads:
        load.start()
    stores = []

    def consume(step, chip_idx):
        rows = pl.ds(pl.multiple_of(chip_idx * chip_rows, chip_rows), chip_rows)
        if not step:
            loads[0].wait()
        first = staged[0]
        first[rows, :] = dot(full[rows, :], held[0][...], MATMUL if forward else CONTRACT_LAST).astype(BF16)
        if not step:
            for load in loads[1:]:
                load.wait()

        def one_tile(idx, carry):
            cols = pl.ds(pl.multiple_of(idx * tile, tile), tile)
            if forward:
                gate = dot(full[rows, :], held[1][:, cols], MATMUL).astype(BF16)
                up = dot(full[rows, :], held[2][:, cols], MATMUL).astype(BF16)
                staged[1][rows, cols] = gate
                staged[2][rows, cols] = up
                if n_outs > 3:
                    staged[3][rows, cols] = gated(gate.astype(F32), up.astype(F32)).astype(BF16)
            else:
                d_hidden = dot(full[rows, :], held[1][cols, :], CONTRACT_LAST).astype(BF16).astype(F32)
                hidden, pull = jax.vjp(gated, held[2][rows, cols].astype(F32), held[3][rows, cols].astype(F32))
                d_gate, d_up = pull(d_hidden)
                staged[1][rows, cols] = hidden.astype(BF16)
                staged[2][rows, cols] = d_gate.astype(BF16)
                staged[3][rows, cols] = d_up.astype(BF16)
            return carry

        lax.fori_loop(0, staged[1].shape[1] // tile, one_tile, 0)
        for idx, out in enumerate(outs):
            source = full if idx == len(staged) else staged[idx]
            copy = pltpu.make_async_copy(source.at[rows], out.at[rows], store_sem.at[step, idx])
            copy.start()
            stores.append(copy)

    ring_gather(chips, loc_ref, full, send, recv, consume)
    for copy in stores:
        copy.wait()


def gather_dots(loc, inputs, layer, forward, with_hidden, tp_size, collective_id, name, tile=256):
    n_rows, depth = loc.shape
    seq_len, chips = n_rows * tp_size, tp_size // CORES
    n_weights = 3 if forward else 2
    weights, saved = inputs[:n_weights], inputs[n_weights:]
    if forward:
        widths = [weight.shape[2] for weight in weights] + ([weights[1].shape[2]] if with_hidden else [])
    else:
        widths = [weights[0].shape[1]] + [weights[1].shape[1]] * 3
    staged = [pltpu.VMEM((seq_len, width), BF16) for width in widths]
    outs = [jax.ShapeDtypeStruct((seq_len, width), BF16) for width in widths + ([] if forward else [depth])]
    n_cols = sum(weight.size // (weight.shape[0] * depth) for weight in weights)
    return pl.pallas_call(
        functools.partial(gather_dots_kernel, chips, layer, forward, len(outs), tile),
        out_shape=outs,
        in_specs=[pl.BlockSpec(memory_space=pltpu.VMEM)] + [pl.BlockSpec(memory_space=pl.ANY)] * len(inputs),
        out_specs=[pl.BlockSpec(memory_space=pl.ANY)] * len(outs),
        scratch_shapes=[pltpu.VMEM((seq_len, depth), BF16)]
        + [pltpu.VMEM(weight.shape[1:], BF16) for weight in weights]
        + [pltpu.VMEM(item.shape, BF16) for item in saved]
        + staged
        + [pltpu.SemaphoreType.DMA((len(inputs),)), pltpu.SemaphoreType.DMA((4, len(outs))), pltpu.SemaphoreType.DMA((10,)), pltpu.SemaphoreType.DMA((10,))],
        compiler_params=pltpu.CompilerParams(vmem_limit_bytes=VMEM_LIMIT, collective_id=collective_id, has_side_effects=True),
        cost_estimate=cost(2 * seq_len * depth * n_cols, 2 * (seq_len * depth + depth * n_cols + seq_len * n_cols)),
        name=name,
    )(loc, *inputs)


SCATTER_ORDER = ((0, 0), (0, 1), (1, 0), (2, 1), (1, 1), (2, 0), (3, 0), (3, 1))


def dots_scatter_kernel(chips, layer, dims, n_terms, tile, *refs):
    lhs_refs, rhs_refs, out_ref = refs[:n_terms], refs[n_terms:2 * n_terms], refs[2 * n_terms]
    held, scratch = refs[2 * n_terms + 1:3 * n_terms + 1], refs[3 * n_terms + 1:]
    part, from_core, acc, from_far, from_side, load_sem, core_send, core_recv, send, recv = scratch
    n_rows, n_cols = out_ref.shape
    half = n_cols // 2
    chip, core, (partner, left, right) = ring_place(chips)
    dest_chips = [lax.rem(chip + offset, chips) for offset in (2, chips - 1, 1, 0)]

    def half_of(ref, which):
        cols = pl.ds(which * half, half)
        return ref.at[:, cols] if dims is MATMUL else ref.at[cols, :]

    loads = [
        [pltpu.make_async_copy(half_of(src.at[layer], which), half_of(dst, which), load_sem.at[idx, which]) for idx, (src, dst) in enumerate(zip(rhs_refs, held))]
        for which in range(2)
    ]
    for group in loads:
        for load in group:
            load.start()
    enter_ring((partner, left, right))
    to_core = [remote(part.at[item % 2, 1 - core], from_core.at[item], core_send, core_recv, item, partner) for item in range(len(SCATTER_ORDER))]
    hops = {
        (0, 0): remote(acc.at[0, 0], from_far.at[0], send, recv, 0, right),
        (0, 1): remote(acc.at[0, 1], from_far.at[1], send, recv, 1, left),
        (1, 0): remote(acc.at[1, 0], from_side.at[1, 0], send, recv, 2, left),
        (2, 1): remote(acc.at[2, 1], from_side.at[0, 1], send, recv, 3, right),
        (1, 1): remote(acc.at[1, 1], from_side.at[1, 1], send, recv, 4, left),
        (2, 0): remote(acc.at[2, 0], from_side.at[0, 0], send, recv, 5, right),
    }

    def compute(item):
        step, which = SCATTER_ORDER[item]
        rows = pl.ds(pl.multiple_of(dest_chips[step] * (CORES * n_rows), CORES * n_rows), CORES * n_rows)
        if item < 2:
            for load in loads[which]:
                load.wait()
        if item >= 2:
            to_core[item - 2].wait_send()

        def one_tile(idx, carry):
            first = pl.multiple_of(idx * tile, tile)
            rhs_cols = pl.ds(which * half + first, tile)
            total = None
            for lhs_ref, rhs_ref in zip(lhs_refs, held):
                rhs = rhs_ref[:, rhs_cols] if dims is MATMUL else rhs_ref[rhs_cols, :]
                product = dot(lhs_ref[rows, :], rhs, dims)
                total = product if total is None else total + product
            for idx_core in range(CORES):
                part[item % 2, idx_core, :, pl.ds(first, tile)] = total[idx_core * n_rows:(idx_core + 1) * n_rows]
            return carry

        lax.fori_loop(0, half // tile, one_tile, 0)
        to_core[item].start()

    def add_core(item):
        step, which = SCATTER_ORDER[item]
        to_core[item].wait_recv()
        acc[step, which] = part[item % 2, core] + from_core[item]
        if item < 4:
            hops[step, which].start()

    n_items = len(SCATTER_ORDER)
    for item in range(n_items):
        compute(item)
        if item:
            add_core(item - 1)
    add_core(n_items - 1)
    for which, step in ((0, 2), (1, 1)):
        hops[0, which].wait_recv()
        acc[step, which] = acc[step, which] + from_far[which]
        hops[step, which].start()
    for key in ((1, 0), (2, 1), (1, 1), (2, 0)):
        hops[key].wait_recv()
    for which in range(2):
        out_ref[:, pl.ds(which * half, half)] = acc[3, which] + from_side[0, which] + from_side[1, which]
    for copy in to_core[-2:]:
        copy.wait_send()
    for copy in hops.values():
        copy.wait_send()


def dots_scatter(terms, layer, dims, tp_size, collective_id, name, tile=512):
    seq_len = terms[0][0].shape[0]
    n_cols = terms[0][1].shape[2] if dims is MATMUL else terms[0][1].shape[1]
    n_rows, half = seq_len // tp_size, n_cols // 2
    depth = sum(lhs.shape[1] for lhs, _ in terms)
    return pl.pallas_call(
        functools.partial(dots_scatter_kernel, tp_size // CORES, layer, dims, len(terms), tile),
        out_shape=jax.ShapeDtypeStruct((n_rows, n_cols), F32),
        in_specs=[pl.BlockSpec(memory_space=pltpu.VMEM)] * len(terms) + [pl.BlockSpec(memory_space=pl.ANY)] * len(terms),
        out_specs=pl.BlockSpec(memory_space=pltpu.VMEM),
        scratch_shapes=[pltpu.VMEM(rhs.shape[1:], BF16) for _, rhs in terms]
        + [
            pltpu.VMEM((2, CORES, n_rows, half), F32),
            pltpu.VMEM((len(SCATTER_ORDER), n_rows, half), F32),
            pltpu.VMEM((4, 2, n_rows, half), F32),
            pltpu.VMEM((2, n_rows, half), F32),
            pltpu.VMEM((2, 2, n_rows, half), F32),
            pltpu.SemaphoreType.DMA((len(terms), 2)),
            pltpu.SemaphoreType.DMA((len(SCATTER_ORDER),)),
            pltpu.SemaphoreType.DMA((len(SCATTER_ORDER),)),
            pltpu.SemaphoreType.DMA((6,)),
            pltpu.SemaphoreType.DMA((6,)),
        ],
        compiler_params=pltpu.CompilerParams(vmem_limit_bytes=VMEM_LIMIT, collective_id=collective_id, has_side_effects=True),
        cost_estimate=cost(2 * seq_len * depth * n_cols, 2 * depth * (seq_len + n_cols) + 4 * n_rows * n_cols),
        name=name,
    )(*[lhs for lhs, _ in terms], *[rhs for _, rhs in terms])


def gather_rows(rows_loc):
    return lax.all_gather(rows_loc, 'tp', axis=0, tiled=True)


def after(value, *others):
    return lax.optimization_barrier((value,) + others)[0]


def reduce_rows(chunks):
    return jnp.concatenate([lax.psum_scatter(chunk, 'tp', scatter_dimension=0, tiled=True) for chunk in chunks], axis=1)


def solution(mesh):
    tp_size = mesh.shape['tp']
    row_spec = P(('dp', 'tp'), None)
    col_spec = P(None, None, 'tp')
    inner_spec = P(None, 'tp', None)

    def sum_over_tp(value):
        stride = 1
        while stride < tp_size:
            value = value + lax.ppermute(value, 'tp', [(idx, idx ^ stride) for idx in range(tp_size)])
            stride *= 2
        return value

    def device_program(x_loc, dy_loc, norm_gain, w_qkv, w_out, w_gate, w_up, w_down):
        n_layers, depth = w_qkv.shape[0], w_qkv.shape[1]
        group = w_out.shape[1] // HEAD_DIM
        seq_len = x_loc.shape[0] * tp_size
        n_chunks = 2
        chunk_cols = depth // n_chunks
        cos_tab, sin_tab = rope_tables(seq_len)
        saved_all = []
        x_cur = x_loc
        for layer in range(n_layers):
            last = layer == n_layers - 1
            x_f32 = x_cur.astype(F32)
            u_loc = rms_scale(x_f32, norm_gain[layer]).astype(BF16)
            outs = gather_dots(u_loc, (w_qkv, w_gate, w_up), layer, True, not last, tp_size, layer, "gather_in")
            qkv, gate, up = outs[:3]
            rot, attn_out, lse = attn_fwd(qkv, cos_tab, sin_tab, group)
            saved_all.append((x_cur, u_loc, rot, attn_out, lse, gate, up))
            if not last:
                block_sum = dots_scatter([(attn_out, w_out), (outs[3], w_down)], layer, MATMUL, tp_size, n_layers + layer, "scatter_out")
                x_cur = (x_f32 + block_sum).astype(BF16)

        in_grads, out_grads, gain_grads = (), (), []
        for layer in reversed(range(n_layers)):
            x_in, u_loc, rot, attn_out, lse, gate, up = saved_all[layer]
            dy_send, rot = lax.optimization_barrier((dy_loc, rot))
            d_attn, hidden, d_gate, d_up, dy_full = gather_dots(dy_send, (w_out, w_down, gate, up), layer, False, True, tp_size, 2 * n_layers + layer, "gather_back")
            u_full = gather_rows(after(u_loc, attn_out, d_attn))
            d_qkv = attn_bwd(rot, lse, d_attn, cos_tab, sin_tab, group)
            d_qkv, u_full = lax.optimization_barrier((d_qkv, u_full))
            parts = [
                sum_of_dots([(d_qkv, w_qkv), (d_gate, w_gate), (d_up, w_up)], layer, CONTRACT_LAST, idx * chunk_cols, chunk_cols, 512, "block_in_back")
                for idx in range(n_chunks)
            ]
            held = lax.optimization_barrier((parts[-1], d_qkv, d_gate, d_up, hidden, attn_out))
            parts[-1] = held[0]
            in_grads = grad_in(u_full, held[1:4], layer, n_layers, in_grads)
            out_grads = grad_out(held[5], held[4], dy_full, layer, n_layers, out_grads)
            d_normed, in_grads, out_grads = lax.optimization_barrier((reduce_rows(parts), in_grads, out_grads))
            d_normed = d_normed.astype(BF16)
            norm_pull = jax.vjp(rms_scale, x_in.astype(F32), norm_gain[layer])[1]
            d_x_norm, gain_grad = norm_pull(d_normed.astype(F32))
            dy_loc = (dy_loc.astype(F32) + d_x_norm).astype(BF16)
            gain_grads.insert(0, gain_grad)
        grad_gain = sum_over_tp(jnp.stack(gain_grads))
        return (dy_loc, grad_gain, in_grads[0], out_grads[0], in_grads[1], in_grads[2], out_grads[1])

    return jax.shard_map(device_program, mesh=mesh, in_specs=(row_spec, row_spec, P(None, None), col_spec, inner_spec, col_spec, col_spec, inner_spec), out_specs=(row_spec, P('dp', None), P('dp', None, 'tp'), P('dp', 'tp', None), P('dp', None, 'tp'), P('dp', None, 'tp'), P('dp', 'tp', None)), check_vma=False)
```

```python
import functools

import jax
import jax.numpy as jnp
import numpy as np
from jax import lax
from jax.experimental import pallas as pl
from jax.experimental.pallas import tpu as pltpu
from jax.sharding import PartitionSpec as P

HEAD_DIM = 128
NORM_EPS = 1e-5
ROPE_BASE = 10000.0
Q_BLOCK = 256
VMEM_LIMIT = 63 * 1024 * 1024
F32 = jnp.float32
BF16 = jnp.bfloat16

CONTRACT_LAST = (((1,), (1,)), ((), ()))
CONTRACT_FIRST = (((0,), (0,)), ((), ()))
MATMUL = (((1,), (0,)), ((), ()))


def dot(lhs, rhs, dims):
    return lax.dot_general(lhs, rhs, dims, preferred_element_type=F32)


def params():
    return pltpu.CompilerParams(vmem_limit_bytes=VMEM_LIMIT)


def cost(flops, bytes_accessed, transcendentals=0):
    return pl.CostEstimate(flops=int(flops), bytes_accessed=int(bytes_accessed), transcendentals=int(transcendentals))


def rope_tables(seq_len):
    half_dim = HEAD_DIM // 2
    freqs = (ROPE_BASE ** (-2.0 * np.arange(half_dim) / HEAD_DIM)).astype(np.float32)
    angles = (np.arange(seq_len, dtype=np.float32)[:, None] * freqs[None, :]).astype(np.float64)
    cos, sin = np.cos(angles).astype(np.float32), np.sin(angles).astype(np.float32)
    return jnp.asarray(np.concatenate([cos, cos], axis=-1)), jnp.asarray(np.concatenate([-sin, sin], axis=-1))


def rms_scale(x_f32, gain_row):
    inv_rms = lax.rsqrt(jnp.mean(x_f32 * x_f32, axis=-1, keepdims=True) + NORM_EPS)
    return x_f32 * inv_rms * gain_row


def gated(gate_f32, up_f32):
    return jax.nn.silu(gate_f32) * up_f32


def head_cols(index):
    return pl.ds(pl.multiple_of(index * HEAD_DIM, HEAD_DIM), HEAD_DIM)


def diagonal_mask():
    return lax.broadcasted_iota(jnp.int32, (Q_BLOCK, Q_BLOCK), 0) >= lax.broadcasted_iota(jnp.int32, (Q_BLOCK, Q_BLOCK), 1)


def attn_fwd_kernel(group, qkv_ref, cos_ref, sin_ref, rot_ref, out_ref, lse_ref):
    seq_len = qkv_ref.shape[0]
    scale = HEAD_DIM ** -0.5
    key, val = pl.ds(group * HEAD_DIM, HEAD_DIM), pl.ds((group + 1) * HEAD_DIM, HEAD_DIM)

    def rotate_head(head, carry):
        values = qkv_ref[:, head_cols(head)].astype(F32)
        rot_ref[:, head_cols(head)] = (values * cos_ref[...] + pltpu.roll(values, HEAD_DIM // 2, 1) * sin_ref[...]).astype(BF16)
        return carry

    lax.fori_loop(0, group + 1, rotate_head, 0)
    rot_ref[:, val] = qkv_ref[:, val]
    for block in range(seq_len // Q_BLOCK):
        start = block * Q_BLOCK
        rows = pl.ds(start, Q_BLOCK)

        def one_head(head, carry):
            query = rot_ref[rows, head_cols(head)]
            diag = jnp.where(diagonal_mask(), dot(query, rot_ref[rows, key], CONTRACT_LAST) * scale, -1e30)
            row_max = jnp.max(diag, axis=-1, keepdims=True)
            if start:
                past = dot(query, rot_ref[pl.ds(0, start), key], CONTRACT_LAST) * scale
                row_max = jnp.maximum(row_max, jnp.max(past, axis=-1, keepdims=True))
            diag = jnp.exp(diag - row_max)
            total = jnp.sum(diag, axis=-1, keepdims=True)
            if start:
                past = jnp.exp(past - row_max)
                total = total + jnp.sum(past, axis=-1, keepdims=True)
            inverse = 1.0 / total
            acc = dot((diag * inverse).astype(BF16), rot_ref[rows, val], MATMUL)
            if start:
                acc = acc + dot((past * inverse).astype(BF16), rot_ref[pl.ds(0, start), val], MATMUL)
            out_ref[rows, head_cols(head)] = acc.astype(BF16)
            lse_ref[rows, head_cols(head)] = jnp.broadcast_to(row_max + jnp.log(total), (Q_BLOCK, HEAD_DIM))
            return carry

        lax.fori_loop(0, group, one_head, 0)


def attn_fwd(qkv, cos_tab, sin_tab, group):
    seq_len = qkv.shape[0]
    pairs = group * seq_len * seq_len
    return pl.pallas_call(
        functools.partial(attn_fwd_kernel, group),
        out_shape=(
            jax.ShapeDtypeStruct(qkv.shape, BF16),
            jax.ShapeDtypeStruct((seq_len, group * HEAD_DIM), BF16),
            jax.ShapeDtypeStruct((seq_len, group * HEAD_DIM), F32),
        ),
        compiler_params=params(),
        cost_estimate=cost(4 * pairs * HEAD_DIM, 8 * qkv.size, pairs // 2),
        name="attn_fwd",
    )(qkv, cos_tab, sin_tab)


def attn_bwd_kernel(group, rot_ref, lse_ref, dout_ref, cos_ref, sin_ref, dqkv_ref, dkey_ref, dval_ref):
    seq_len = rot_ref.shape[0]
    scale = HEAD_DIM ** -0.5
    key, val = pl.ds(group * HEAD_DIM, HEAD_DIM), pl.ds((group + 1) * HEAD_DIM, HEAD_DIM)
    dkey_ref[...] = jnp.zeros_like(dkey_ref)
    dval_ref[...] = jnp.zeros_like(dval_ref)

    def unrotate(values, rows):
        values = values.astype(BF16).astype(F32)
        return (values * cos_ref[rows, :] - pltpu.roll(values, HEAD_DIM // 2, 1) * sin_ref[rows, :]).astype(BF16)

    for block in range(seq_len // Q_BLOCK):
        start = block * Q_BLOCK
        rows = pl.ds(start, Q_BLOCK)

        def one_head(head, carry):
            query = rot_ref[rows, head_cols(head)]
            dout = dout_ref[rows, head_cols(head)]
            lse = lse_ref[rows, head_cols(head)][:, :1]

            def probs(cols, masked):
                scores = dot(query, rot_ref[cols, key], CONTRACT_LAST) * scale
                if masked:
                    scores = jnp.where(diagonal_mask(), scores, -1e30)
                prob = jnp.exp(scores - lse)
                dprob = dot(dout, rot_ref[cols, val], CONTRACT_LAST).astype(BF16).astype(F32)
                dval_ref[cols, :] += dot(prob.astype(BF16), dout, CONTRACT_FIRST)
                return prob, dprob, jnp.sum(prob * dprob, axis=-1, keepdims=True)

            def finish(cols, prob, dprob, delta):
                dscore = (prob * (dprob - delta) * scale).astype(BF16)
                dkey_ref[cols, :] += dot(dscore, query, CONTRACT_FIRST)
                return dot(dscore, rot_ref[cols, key], MATMUL)

            prob, dprob, delta = probs(rows, True)
            if start:
                past = pl.ds(0, start)
                past_prob, past_dprob, past_delta = probs(past, False)
                delta = delta + past_delta
            dquery = finish(rows, prob, dprob, delta)
            if start:
                dquery = dquery + finish(past, past_prob, past_dprob, delta)
            dqkv_ref[rows, head_cols(head)] = unrotate(dquery, rows)
            return carry

        lax.fori_loop(0, group, one_head, 0)
    dqkv_ref[:, key] = unrotate(dkey_ref[...], pl.ds(0, seq_len))
    dqkv_ref[:, val] = dval_ref[...].astype(BF16)


def attn_bwd(rot, lse, dout, cos_tab, sin_tab, group):
    seq_len = rot.shape[0]
    pairs = group * seq_len * seq_len
    return pl.pallas_call(
        functools.partial(attn_bwd_kernel, group),
        out_shape=jax.ShapeDtypeStruct(rot.shape, BF16),
        scratch_shapes=[pltpu.VMEM((seq_len, HEAD_DIM), F32)] * 2,
        compiler_params=params(),
        cost_estimate=cost(10 * pairs * HEAD_DIM, 8 * rot.size, pairs // 2),
        name="attn_bwd",
    )(rot, lse, dout, cos_tab, sin_tab)


def grad_in_kernel(n_rhs, *refs):
    lhs = refs[0][...]
    rhs_refs, done_refs, out_refs = refs[1:1 + n_rhs], refs[1 + n_rhs:-n_rhs], refs[-n_rhs:]
    for idx, (rhs_ref, out_ref) in enumerate(zip(rhs_refs, out_refs)):
        out_ref[0] = dot(lhs, rhs_ref[...], CONTRACT_FIRST).astype(BF16)
        for place, done_ref in enumerate(done_refs[idx::n_rhs]):
            out_ref[1 + place] = done_ref[...]


def grad_in(lhs, rhs_list, done, tile=512):
    seq_len, depth = lhs.shape
    n_rhs, n_layers = len(rhs_list), 1 + len(done)
    width = sum(rhs.shape[1] for rhs in rhs_list)
    return pl.pallas_call(
        functools.partial(grad_in_kernel, n_rhs),
        out_shape=[jax.ShapeDtypeStruct((n_layers, depth, rhs.shape[1]), BF16) for rhs in rhs_list],
        grid=(depth // tile,),
        in_specs=[pl.BlockSpec((seq_len, tile), lambda step: (0, step))]
        + [pl.BlockSpec(rhs.shape, lambda step: (0, 0), pipeline_mode=pl.Buffered(1)) for rhs in rhs_list]
        + [pl.BlockSpec((tile, item.shape[1]), lambda step: (step, 0)) for layer_done in done for item in layer_done],
        out_specs=[pl.BlockSpec((n_layers, tile, rhs.shape[1]), lambda step: (0, step, 0)) for rhs in rhs_list],
        compiler_params=params(),
        cost_estimate=cost(2 * seq_len * depth * width, 2 * (seq_len * depth + seq_len * width + (2 * n_layers - 1) * depth * width)),
        name="grad_in",
    )(lhs, *rhs_list, *[item for layer_done in done for item in layer_done])


def grad_out_kernel(attn_ref, hidden_ref, dy_ref, *refs):
    out_ref, down_ref = refs[-2:]

    @pl.when(pl.program_id(0) == 0)
    def _():
        out_ref[...] = dot(attn_ref[...], dy_ref[...], CONTRACT_FIRST).astype(BF16)

    down_ref[...] = dot(hidden_ref[...], dy_ref[...], CONTRACT_FIRST).astype(BF16)


def grad_out(attn_out, hidden, dy_full, layer, n_layers, previous, tile=512):
    seq_len, depth = dy_full.shape
    heads, ff = attn_out.shape[1], hidden.shape[1]
    return pl.pallas_call(
        grad_out_kernel,
        out_shape=(jax.ShapeDtypeStruct((n_layers, heads, depth), BF16), jax.ShapeDtypeStruct((n_layers, ff, depth), BF16)),
        grid=(ff // tile,),
        in_specs=[
            pl.BlockSpec((seq_len, heads), lambda step: (0, 0)),
            pl.BlockSpec((seq_len, tile), lambda step: (0, step)),
            pl.BlockSpec((seq_len, depth), lambda step: (0, 0), pipeline_mode=pl.Buffered(1)),
        ]
        + [pl.BlockSpec(memory_space=pl.ANY) for _ in previous],
        out_specs=[
            pl.BlockSpec((None, heads, depth), lambda step: (layer, 0, 0)),
            pl.BlockSpec((None, tile, depth), lambda step: (layer, step, 0)),
        ],
        input_output_aliases={3: 0, 4: 1} if previous else {},
        compiler_params=params(),
        cost_estimate=cost(2 * seq_len * depth * (heads + ff), 2 * (seq_len * depth + (seq_len + depth) * (heads + ff))),
        name="grad_out",
    )(attn_out, hidden, dy_full, *previous)


MESH = pl.DeviceIdType.MESH
CORES = 2


def ring_place(chips):
    me = lax.axis_index('tp')
    chip, core = me // CORES, lax.rem(me, CORES)
    left, right = lax.rem(chip + chips - 1, chips), lax.rem(chip + 1, chips)
    return chip, core, (chip * CORES + 1 - core, left * CORES + core, right * CORES + core)


def enter_ring(peers):
    barrier = pltpu.get_barrier_semaphore()
    for peer in peers:
        pl.semaphore_signal(barrier, inc=1, device_id={'tp': peer}, device_id_type=MESH)
    pl.semaphore_wait(barrier, len(peers))


def remote(src, dst, send, recv, index, peer):
    return pltpu.make_async_remote_copy(src_ref=src, dst_ref=dst, send_sem=send.at[index], recv_sem=recv.at[index], device_id={'tp': peer}, device_id_type=MESH)


def ring_gather(chips, loc_ref, full, send, recv, consume):
    n_rows = loc_ref.shape[0]
    half = n_rows // 2
    chip, core, (partner, left, right) = ring_place(chips)
    left_chip, right_chip, far_chip = lax.rem(chip + chips - 1, chips), lax.rem(chip + 1, chips), lax.rem(chip + 2, chips)

    def first_row(chip_idx, core_idx, which):
        return pl.multiple_of((chip_idx * CORES + core_idx) * n_rows + which * half, half)

    def piece(chip_idx, core_idx, which):
        return full.at[pl.ds(first_row(chip_idx, core_idx, which), half)]

    def own(which):
        return loc_ref.at[pl.ds(which * half, half)]

    received = [(left_chip, 0), (right_chip, 1), (left_chip, 1), (right_chip, 0), (far_chip, 0), (far_chip, 1)]
    sends = [
        remote(own(0), piece(chip, core, 0), send, recv, 0, right),
        remote(own(1), piece(chip, core, 1), send, recv, 1, left),
        remote(own(1), piece(chip, core, 1), send, recv, 2, right),
        remote(own(0), piece(chip, core, 0), send, recv, 3, left),
        remote(piece(left_chip, core, 0), piece(left_chip, core, 0), send, recv, 4, right),
        remote(piece(right_chip, core, 1), piece(right_chip, core, 1), send, recv, 5, left),
    ]
    landing = [piece(item[0], core, item[1]) for item in received]
    for idx, item in enumerate(received):
        sends.append(remote(piece(item[0], core, item[1]), piece(item[0], core, item[1]), send, recv, 6 + idx, partner))
        landing.append(piece(item[0], 1 - core, item[1]))
    for which in range(2):
        sends.append(remote(own(which), piece(chip, core, which), send, recv, 12 + which, partner))
        landing.append(piece(chip, 1 - core, which))

    def arrived(index):
        remote(landing[index], landing[index], send, recv, index, partner).wait_recv()

    def hand_over(*indices):
        for index in indices:
            arrived(index)
            if index < 2:
                sends[4 + index].start()
            sends[6 + index].start()

    def group_rows(*items):
        return [first_row(item[0], idx, item[1]) for item in items for idx in range(CORES)]

    enter_ring((partner, left, right))
    for index in (0, 1, 2, 3, 12, 13):
        sends[index].start()
    full[pl.ds(pl.multiple_of((chip * CORES + core) * n_rows, n_rows), n_rows), :] = loc_ref[...]
    arrived(12)
    arrived(13)
    consume(0, group_rows((chip, 0), (chip, 1)))
    hand_over(0, 1)
    arrived(6)
    arrived(7)
    consume(1, group_rows(received[0], received[1]))
    hand_over(2, 3)
    arrived(8)
    arrived(9)
    consume(2, group_rows(received[2], received[3]))
    hand_over(4, 5)
    arrived(10)
    arrived(11)
    consume(3, group_rows(received[4], received[5]))
    for copy in sends:
        copy.wait_send()


def gather_dots_kernel(chips, layer, forward, n_outs, tile, loc_ref, *refs):
    n_weights = 3 if forward else 2
    n_inputs = 3 if forward else 4
    inputs, outs = refs[:n_inputs], refs[n_inputs:n_inputs + n_outs]
    full, scratch = refs[n_inputs + n_outs], refs[n_inputs + n_outs + 1:]
    held, staged = scratch[:n_inputs], scratch[n_inputs:-4]
    load_sem, store_sem, send, recv = scratch[-4:]
    half = loc_ref.shape[0] // 2
    loads = [pltpu.make_async_copy(src.at[layer] if idx < n_weights else src, dst, load_sem.at[idx]) for idx, (src, dst) in enumerate(zip(inputs, held))]
    for load in loads:
        load.start()
    stores = []

    def consume(group, first_rows):
        pieces = [pl.ds(first, half) for first in first_rows]

        def rows_of(ref, cols=slice(None)):
            return jnp.concatenate([ref[rows, cols] for rows in pieces], axis=0)

        def put(ref, cols, value):
            for idx, rows in enumerate(pieces):
                ref[rows, cols] = value[idx * half:(idx + 1) * half]

        if not group:
            loads[0].wait()
        put(staged[0], slice(None), dot(rows_of(full), held[0][...], MATMUL if forward else CONTRACT_LAST).astype(BF16))
        if not group:
            for load in loads[1:]:
                load.wait()

        def one_tile(idx, carry):
            cols = pl.ds(pl.multiple_of(idx * tile, tile), tile)
            if forward:
                gate = dot(rows_of(full), held[1][:, cols], MATMUL).astype(BF16)
                up = dot(rows_of(full), held[2][:, cols], MATMUL).astype(BF16)
                put(staged[1], cols, gate)
                put(staged[2], cols, up)
                if n_outs > 3:
                    put(staged[3], cols, gated(gate.astype(F32), up.astype(F32)).astype(BF16))
            else:
                d_hidden = dot(rows_of(full), held[1][cols, :], CONTRACT_LAST).astype(BF16).astype(F32)
                hidden, pull = jax.vjp(gated, rows_of(held[2], cols).astype(F32), rows_of(held[3], cols).astype(F32))
                d_gate, d_up = pull(d_hidden)
                put(staged[1], cols, hidden.astype(BF16))
                put(staged[2], cols, d_gate.astype(BF16))
                put(staged[3], cols, d_up.astype(BF16))
            return carry

        lax.fori_loop(0, staged[1].shape[1] // tile, one_tile, 0)
        for idx, out in enumerate(outs):
            source = full if idx == len(staged) else staged[idx]
            for place, rows in enumerate(pieces):
                copy = pltpu.make_async_copy(source.at[rows], out.at[rows], store_sem.at[group, place, idx])
                copy.start()
                stores.append(copy)

    ring_gather(chips, loc_ref, full, send, recv, consume)
    for copy in stores:
        copy.wait()


def gather_dots(loc, inputs, layer, forward, with_hidden, tp_size, collective_id, name, tile=256):
    n_rows, depth = loc.shape
    seq_len, chips = n_rows * tp_size, tp_size // CORES
    n_weights = 3 if forward else 2
    weights, saved = inputs[:n_weights], inputs[n_weights:]
    if forward:
        widths = [weight.shape[2] for weight in weights] + ([weights[1].shape[2]] if with_hidden else [])
    else:
        widths = [weights[0].shape[1]] + [weights[1].shape[1]] * 3
    staged = [pltpu.VMEM((seq_len, width), BF16) for width in widths]
    outs = [jax.ShapeDtypeStruct((seq_len, width), BF16) for width in widths + ([] if forward else [depth])]
    n_cols = sum(weight.size // (weight.shape[0] * depth) for weight in weights)
    return pl.pallas_call(
        functools.partial(gather_dots_kernel, chips, layer, forward, len(outs), tile),
        out_shape=outs,
        in_specs=[pl.BlockSpec(memory_space=pltpu.VMEM)] + [pl.BlockSpec(memory_space=pl.ANY)] * len(inputs),
        out_specs=[pl.BlockSpec(memory_space=pl.ANY)] * len(outs),
        scratch_shapes=[pltpu.VMEM((seq_len, depth), BF16)]
        + [pltpu.VMEM(weight.shape[1:], BF16) for weight in weights]
        + [pltpu.VMEM(item.shape, BF16) for item in saved]
        + staged
        + [pltpu.SemaphoreType.DMA((len(inputs),)), pltpu.SemaphoreType.DMA((4, 2 * CORES, len(outs))), pltpu.SemaphoreType.DMA((14,)), pltpu.SemaphoreType.DMA((14,))],
        compiler_params=pltpu.CompilerParams(vmem_limit_bytes=VMEM_LIMIT, collective_id=collective_id, has_side_effects=True),
        cost_estimate=cost(2 * seq_len * depth * n_cols, 2 * (seq_len * depth + depth * n_cols + seq_len * n_cols)),
        name=name,
    )(loc, *inputs)


SCATTER_ORDER = ((0, 0), (0, 1), (1, 0), (2, 1), (1, 1), (2, 0), (3, 0), (3, 1))


def weight_grads(u_ref, rhs_refs, grad_refs, u_held, grads_held, u_sem, grad_sem):
    tile = u_held.shape[2]
    n_tiles = u_ref.shape[1] // tile
    starts = [sum(rhs.shape[1] for rhs in rhs_refs[:idx]) for idx in range(len(rhs_refs))]

    def load(idx, slot):
        return pltpu.make_async_copy(u_ref.at[:, pl.ds(pl.multiple_of(idx * tile, tile), tile)], u_held.at[slot], u_sem.at[slot])

    def stores(idx, slot):
        rows = pl.ds(pl.multiple_of(idx * tile, tile), tile)
        return [
            pltpu.make_async_copy(grads_held.at[slot, :, pl.ds(start, rhs.shape[1])], grad.at[rows, :], grad_sem.at[slot, place])
            for place, (start, rhs, grad) in enumerate(zip(starts, rhs_refs, grad_refs))
        ]

    load(0, 0).start()

    def one_tile(idx, carry):
        slot = lax.rem(idx, 2)

        @pl.when(idx + 1 < n_tiles)
        def _():
            load(idx + 1, 1 - slot).start()

        @pl.when(idx >= 2)
        def _():
            for store in stores(idx - 2, slot):
                store.wait()

        load(idx, slot).wait()
        lhs = u_held[slot]
        for start, rhs in zip(starts, rhs_refs):
            grads_held[slot, :, pl.ds(start, rhs.shape[1])] = dot(lhs, rhs[...], CONTRACT_FIRST).astype(BF16)
        for store in stores(idx, slot):
            store.start()
        return carry

    lax.fori_loop(0, n_tiles, one_tile, 0)
    for idx in range(max(n_tiles - 2, 0), n_tiles):
        for store in stores(idx, idx % 2):
            store.wait()


def dots_scatter_kernel(chips, layer, dims, n_terms, tile, with_grads, *refs):
    lhs_refs, rhs_refs, refs = refs[:n_terms], refs[n_terms:2 * n_terms], refs[2 * n_terms:]
    if with_grads:
        u_ref, refs = refs[0], refs[1:]
    out_ref, refs = refs[0], refs[1:]
    if with_grads:
        grad_refs, refs = refs[:n_terms], refs[n_terms:]
    held, scratch = refs[:n_terms], refs[n_terms:]
    part, acc, from_far, from_side, load_sem, core_send, core_recv, send, recv = scratch[:9]
    n_rows, n_cols = out_ref.shape
    half = n_cols // 2
    chip, core, (partner, left, right) = ring_place(chips)
    dest_chips = [lax.rem(chip + offset, chips) for offset in (2, chips - 1, 1, 0)]

    def half_of(ref, which):
        cols = pl.ds(which * half, half)
        return ref.at[:, cols] if dims is MATMUL else ref.at[cols, :]

    loads = [
        [pltpu.make_async_copy(half_of(src.at[layer], which), half_of(dst, which), load_sem.at[idx, which]) for idx, (src, dst) in enumerate(zip(rhs_refs, held))]
        for which in range(2)
    ]
    for group in loads:
        for load in group:
            load.start()
    enter_ring((partner, left, right))
    to_core = [
        remote(part.at[item % 2, 1 - core], acc.at[step, which], core_send, core_recv, item, partner) for item, (step, which) in enumerate(SCATTER_ORDER)
    ]
    hops = {
        (0, 0): remote(acc.at[0, 0], from_far.at[0], send, recv, 0, right),
        (0, 1): remote(acc.at[0, 1], from_far.at[1], send, recv, 1, left),
        (1, 0): remote(acc.at[1, 0], from_side.at[1, 0], send, recv, 2, left),
        (2, 1): remote(acc.at[2, 1], from_side.at[0, 1], send, recv, 3, right),
        (1, 1): remote(acc.at[1, 1], from_side.at[1, 1], send, recv, 4, left),
        (2, 0): remote(acc.at[2, 0], from_side.at[0, 0], send, recv, 5, right),
    }

    def compute(item):
        step, which = SCATTER_ORDER[item]
        rows = pl.ds(pl.multiple_of(dest_chips[step] * (CORES * n_rows), CORES * n_rows), CORES * n_rows)
        if item < 2:
            for load in loads[which]:
                load.wait()
        if item >= 2:
            to_core[item - 2].wait_send()

        def one_tile(idx, carry):
            first = pl.multiple_of(idx * tile, tile)
            rhs_cols = pl.ds(which * half + first, tile)
            total = None
            for lhs_ref, rhs_ref in zip(lhs_refs, held):
                rhs = rhs_ref[:, rhs_cols] if dims is MATMUL else rhs_ref[rhs_cols, :]
                product = dot(lhs_ref[rows, :], rhs, dims)
                total = product if total is None else total + product
            for idx_core in range(CORES):
                part[item % 2, idx_core, :, pl.ds(first, tile)] = total[idx_core * n_rows:(idx_core + 1) * n_rows]
            return carry

        lax.fori_loop(0, half // tile, one_tile, 0)
        to_core[item].start()

    def add_core(item):
        step, which = SCATTER_ORDER[item]
        to_core[item].wait_recv()
        acc[step, which] = acc[step, which] + part[item % 2, core]
        if item < 4:
            hops[step, which].start()

    n_items = len(SCATTER_ORDER)
    for item in range(n_items):
        compute(item)
        if item:
            add_core(item - 1)
    add_core(n_items - 1)
    for which, step in ((0, 2), (1, 1)):
        hops[0, which].wait_recv()
        acc[step, which] = acc[step, which] + from_far[which]
        hops[step, which].start()
    if with_grads:
        weight_grads(u_ref, lhs_refs, grad_refs, *scratch[9:])
    for key in ((1, 0), (2, 1), (1, 1), (2, 0)):
        hops[key].wait_recv()
    for which in range(2):
        out_ref[:, pl.ds(which * half, half)] = acc[3, which] + from_side[0, which] + from_side[1, which]
    for copy in to_core[-2:]:
        copy.wait_send()
    for copy in hops.values():
        copy.wait_send()


def dots_scatter(terms, layer, dims, tp_size, collective_id, name, u_full=None, tile=512, grad_tile=512):
    seq_len = terms[0][0].shape[0]
    n_cols = terms[0][1].shape[2] if dims is MATMUL else terms[0][1].shape[1]
    n_rows, half = seq_len // tp_size, n_cols // 2
    depth = sum(lhs.shape[1] for lhs, _ in terms)
    with_grads = u_full is not None
    n_terms = len(terms)
    any_spec, vmem_spec = pl.BlockSpec(memory_space=pl.ANY), pl.BlockSpec(memory_space=pltpu.VMEM)
    outs, extra_inputs, extra_scratch = [jax.ShapeDtypeStruct((n_rows, n_cols), F32)], (), []
    if with_grads:
        outs += [jax.ShapeDtypeStruct((n_cols, lhs.shape[1]), BF16) for lhs, _ in terms]
        extra_inputs = (u_full,)
        extra_scratch = [
            pltpu.VMEM((2, seq_len, grad_tile), BF16),
            pltpu.VMEM((2, grad_tile, depth), BF16),
            pltpu.SemaphoreType.DMA((2,)),
            pltpu.SemaphoreType.DMA((2, n_terms)),
        ]
    results = pl.pallas_call(
        functools.partial(dots_scatter_kernel, tp_size // CORES, layer, dims, n_terms, tile, with_grads),
        out_shape=outs,
        in_specs=[vmem_spec] * n_terms + [any_spec] * (n_terms + len(extra_inputs)),
        out_specs=[vmem_spec] + [any_spec] * (len(outs) - 1),
        scratch_shapes=[pltpu.VMEM(rhs.shape[1:], BF16) for _, rhs in terms]
        + [
            pltpu.VMEM((2, CORES, n_rows, half), F32),
            pltpu.VMEM((4, 2, n_rows, half), F32),
            pltpu.VMEM((2, n_rows, half), F32),
            pltpu.VMEM((2, 2, n_rows, half), F32),
            pltpu.SemaphoreType.DMA((n_terms, 2)),
            pltpu.SemaphoreType.DMA((len(SCATTER_ORDER),)),
            pltpu.SemaphoreType.DMA((len(SCATTER_ORDER),)),
            pltpu.SemaphoreType.DMA((6,)),
            pltpu.SemaphoreType.DMA((6,)),
        ]
        + extra_scratch,
        compiler_params=pltpu.CompilerParams(vmem_limit_bytes=VMEM_LIMIT, collective_id=collective_id, has_side_effects=True),
        cost_estimate=cost(2 * seq_len * depth * n_cols * (2 if with_grads else 1), 2 * depth * (seq_len + n_cols) + 4 * n_rows * n_cols),
        name=name,
    )(*[lhs for lhs, _ in terms], *[rhs for _, rhs in terms], *extra_inputs)
    return (results[0], tuple(results[1:])) if with_grads else results[0]


def gather_rows(rows_loc):
    return lax.all_gather(rows_loc, 'tp', axis=0, tiled=True)


def after(value, *others):
    return lax.optimization_barrier((value,) + others)[0]


def solution(mesh):
    tp_size = mesh.shape['tp']
    row_spec = P(('dp', 'tp'), None)
    col_spec = P(None, None, 'tp')
    inner_spec = P(None, 'tp', None)

    def sum_over_tp(value):
        stride = 1
        while stride < tp_size:
            value = value + lax.ppermute(value, 'tp', [(idx, idx ^ stride) for idx in range(tp_size)])
            stride *= 2
        return value

    def device_program(x_loc, dy_loc, norm_gain, w_qkv, w_out, w_gate, w_up, w_down):
        n_layers, depth = w_qkv.shape[0], w_qkv.shape[1]
        group = w_out.shape[1] // HEAD_DIM
        seq_len = x_loc.shape[0] * tp_size
        cos_tab, sin_tab = rope_tables(seq_len)
        saved_all = []
        x_cur = x_loc
        for layer in range(n_layers):
            last = layer == n_layers - 1
            x_f32 = x_cur.astype(F32)
            u_loc = rms_scale(x_f32, norm_gain[layer]).astype(BF16)
            outs = gather_dots(u_loc, (w_qkv, w_gate, w_up), layer, True, not last, tp_size, layer, "gather_in")
            qkv, gate, up = outs[:3]
            rot, attn_out, lse = attn_fwd(qkv, cos_tab, sin_tab, group)
            saved_all.append((x_cur, u_loc, rot, attn_out, lse, gate, up))
            if not last:
                block_sum = dots_scatter([(attn_out, w_out), (outs[3], w_down)], layer, MATMUL, tp_size, n_layers + layer, "scatter_out")
                x_cur = (x_f32 + block_sum).astype(BF16)

        out_grads, gain_grads, done_grads = (), [], []
        for layer in reversed(range(n_layers)):
            x_in, u_loc, rot, attn_out, lse, gate, up = saved_all[layer]
            dy_send, rot = lax.optimization_barrier((dy_loc, rot))
            d_attn, hidden, d_gate, d_up, dy_full = gather_dots(dy_send, (w_out, w_down, gate, up), layer, False, True, tp_size, 2 * n_layers + layer, "gather_back")
            u_full = gather_rows(after(u_loc, attn_out, d_attn))
            d_qkv = attn_bwd(rot, lse, d_attn, cos_tab, sin_tab, group)
            out_grads = grad_out(attn_out, hidden, dy_full, layer, n_layers, out_grads)
            d_qkv, u_full, out_grads = lax.optimization_barrier((d_qkv, u_full, out_grads))
            terms = [(d_qkv, w_qkv), (d_gate, w_gate), (d_up, w_up)]
            if layer:
                d_normed, done = dots_scatter(terms, layer, CONTRACT_LAST, tp_size, 3 * n_layers + layer, "scatter_back", u_full)
                done_grads.insert(0, done)
            else:
                d_normed = dots_scatter(terms, layer, CONTRACT_LAST, tp_size, 3 * n_layers + layer, "scatter_back")
                d_normed, u_full, d_qkv, d_gate, d_up = lax.optimization_barrier((d_normed, u_full, d_qkv, d_gate, d_up))
                in_grads = grad_in(u_full, (d_qkv, d_gate, d_up), done_grads)
            d_normed = d_normed.astype(BF16)
            norm_pull = jax.vjp(rms_scale, x_in.astype(F32), norm_gain[layer])[1]
            d_x_norm, gain_grad = norm_pull(d_normed.astype(F32))
            dy_loc = (dy_loc.astype(F32) + d_x_norm).astype(BF16)
            gain_grads.insert(0, gain_grad)
        grad_gain = sum_over_tp(jnp.stack(gain_grads))
        return (dy_loc, grad_gain, in_grads[0], out_grads[0], in_grads[1], in_grads[2], out_grads[1])

    return jax.shard_map(device_program, mesh=mesh, in_specs=(row_spec, row_spec, P(None, None), col_spec, inner_spec, col_spec, col_spec, inner_spec), out_specs=(row_spec, P('dp', None), P('dp', None, 'tp'), P('dp', 'tp', None), P('dp', None, 'tp'), P('dp', None, 'tp'), P('dp', 'tp', None)), check_vma=False)
```

```python
import functools

import jax
import jax.numpy as jnp
import numpy as np
from jax import lax
from jax.experimental import pallas as pl
from jax.experimental.pallas import tpu as pltpu
from jax.sharding import PartitionSpec as P

HEAD_DIM = 128
NORM_EPS = 1e-5
ROPE_BASE = 10000.0
Q_BLOCK = 256
VMEM_LIMIT = 63 * 1024 * 1024
F32 = jnp.float32
BF16 = jnp.bfloat16

CONTRACT_LAST = (((1,), (1,)), ((), ()))
CONTRACT_FIRST = (((0,), (0,)), ((), ()))
MATMUL = (((1,), (0,)), ((), ()))


def dot(lhs, rhs, dims):
    return lax.dot_general(lhs, rhs, dims, preferred_element_type=F32)


def params():
    return pltpu.CompilerParams(vmem_limit_bytes=VMEM_LIMIT)


def cost(flops, bytes_accessed, transcendentals=0):
    return pl.CostEstimate(flops=int(flops), bytes_accessed=int(bytes_accessed), transcendentals=int(transcendentals))


def rope_tables(seq_len):
    half_dim = HEAD_DIM // 2
    freqs = (ROPE_BASE ** (-2.0 * np.arange(half_dim) / HEAD_DIM)).astype(np.float32)
    angles = (np.arange(seq_len, dtype=np.float32)[:, None] * freqs[None, :]).astype(np.float64)
    cos, sin = np.cos(angles).astype(np.float32), np.sin(angles).astype(np.float32)
    return jnp.asarray(np.concatenate([cos, cos], axis=-1)), jnp.asarray(np.concatenate([-sin, sin], axis=-1))


def rms_scale(x_f32, gain_row):
    inv_rms = lax.rsqrt(jnp.mean(x_f32 * x_f32, axis=-1, keepdims=True) + NORM_EPS)
    return x_f32 * inv_rms * gain_row


def gated(gate_f32, up_f32):
    return jax.nn.silu(gate_f32) * up_f32


def head_cols(index):
    return pl.ds(pl.multiple_of(index * HEAD_DIM, HEAD_DIM), HEAD_DIM)


def diagonal_mask():
    return lax.broadcasted_iota(jnp.int32, (Q_BLOCK, Q_BLOCK), 0) >= lax.broadcasted_iota(jnp.int32, (Q_BLOCK, Q_BLOCK), 1)


def attn_fwd_kernel(group, qkv_ref, cos_ref, sin_ref, rot_ref, out_ref, lse_ref):
    seq_len = qkv_ref.shape[0]
    scale = HEAD_DIM ** -0.5
    key, val = pl.ds(group * HEAD_DIM, HEAD_DIM), pl.ds((group + 1) * HEAD_DIM, HEAD_DIM)

    def rotate_head(head, carry):
        values = qkv_ref[:, head_cols(head)].astype(F32)
        rot_ref[:, head_cols(head)] = (values * cos_ref[...] + pltpu.roll(values, HEAD_DIM // 2, 1) * sin_ref[...]).astype(BF16)
        return carry

    lax.fori_loop(0, group + 1, rotate_head, 0)
    rot_ref[:, val] = qkv_ref[:, val]
    for block in range(seq_len // Q_BLOCK):
        start = block * Q_BLOCK
        rows = pl.ds(start, Q_BLOCK)

        def one_head(head, carry):
            query = rot_ref[rows, head_cols(head)]
            diag = jnp.where(diagonal_mask(), dot(query, rot_ref[rows, key], CONTRACT_LAST) * scale, -1e30)
            row_max = jnp.max(diag, axis=-1, keepdims=True)
            if start:
                past = dot(query, rot_ref[pl.ds(0, start), key], CONTRACT_LAST) * scale
                row_max = jnp.maximum(row_max, jnp.max(past, axis=-1, keepdims=True))
            diag = jnp.exp(diag - row_max)
            total = jnp.sum(diag, axis=-1, keepdims=True)
            if start:
                past = jnp.exp(past - row_max)
                total = total + jnp.sum(past, axis=-1, keepdims=True)
            inverse = 1.0 / total
            acc = dot((diag * inverse).astype(BF16), rot_ref[rows, val], MATMUL)
            if start:
                acc = acc + dot((past * inverse).astype(BF16), rot_ref[pl.ds(0, start), val], MATMUL)
            out_ref[rows, head_cols(head)] = acc.astype(BF16)
            lse_ref[rows, head_cols(head)] = jnp.broadcast_to(row_max + jnp.log(total), (Q_BLOCK, HEAD_DIM))
            return carry

        lax.fori_loop(0, group, one_head, 0)


def attn_fwd(qkv, cos_tab, sin_tab, group):
    seq_len = qkv.shape[0]
    pairs = group * seq_len * seq_len
    return pl.pallas_call(
        functools.partial(attn_fwd_kernel, group),
        out_shape=(
            jax.ShapeDtypeStruct(qkv.shape, BF16),
            jax.ShapeDtypeStruct((seq_len, group * HEAD_DIM), BF16),
            jax.ShapeDtypeStruct((seq_len, group * HEAD_DIM), F32),
        ),
        compiler_params=params(),
        cost_estimate=cost(4 * pairs * HEAD_DIM, 8 * qkv.size, pairs // 2),
        name="attn_fwd",
    )(qkv, cos_tab, sin_tab)


def attn_bwd_kernel(group, rot_ref, lse_ref, dout_ref, cos_ref, sin_ref, dqkv_ref, dkey_ref, dval_ref):
    seq_len = rot_ref.shape[0]
    scale = HEAD_DIM ** -0.5
    key, val = pl.ds(group * HEAD_DIM, HEAD_DIM), pl.ds((group + 1) * HEAD_DIM, HEAD_DIM)
    dkey_ref[...] = jnp.zeros_like(dkey_ref)
    dval_ref[...] = jnp.zeros_like(dval_ref)

    def unrotate(values, rows):
        values = values.astype(BF16).astype(F32)
        return (values * cos_ref[rows, :] - pltpu.roll(values, HEAD_DIM // 2, 1) * sin_ref[rows, :]).astype(BF16)

    for block in range(seq_len // Q_BLOCK):
        start = block * Q_BLOCK
        rows = pl.ds(start, Q_BLOCK)

        def one_head(head, carry):
            query = rot_ref[rows, head_cols(head)]
            dout = dout_ref[rows, head_cols(head)]
            lse = lse_ref[rows, head_cols(head)][:, :1]

            def probs(cols, masked):
                scores = dot(query, rot_ref[cols, key], CONTRACT_LAST) * scale
                if masked:
                    scores = jnp.where(diagonal_mask(), scores, -1e30)
                prob = jnp.exp(scores - lse)
                dprob = dot(dout, rot_ref[cols, val], CONTRACT_LAST).astype(BF16).astype(F32)
                dval_ref[cols, :] += dot(prob.astype(BF16), dout, CONTRACT_FIRST)
                return prob, dprob, jnp.sum(prob * dprob, axis=-1, keepdims=True)

            def finish(cols, prob, dprob, delta):
                dscore = (prob * (dprob - delta) * scale).astype(BF16)
                dkey_ref[cols, :] += dot(dscore, query, CONTRACT_FIRST)
                return dot(dscore, rot_ref[cols, key], MATMUL)

            prob, dprob, delta = probs(rows, True)
            if start:
                past = pl.ds(0, start)
                past_prob, past_dprob, past_delta = probs(past, False)
                delta = delta + past_delta
            dquery = finish(rows, prob, dprob, delta)
            if start:
                dquery = dquery + finish(past, past_prob, past_dprob, delta)
            dqkv_ref[rows, head_cols(head)] = unrotate(dquery, rows)
            return carry

        lax.fori_loop(0, group, one_head, 0)
    dqkv_ref[:, key] = unrotate(dkey_ref[...], pl.ds(0, seq_len))
    dqkv_ref[:, val] = dval_ref[...].astype(BF16)


def attn_bwd(rot, lse, dout, cos_tab, sin_tab, group):
    seq_len = rot.shape[0]
    pairs = group * seq_len * seq_len
    return pl.pallas_call(
        functools.partial(attn_bwd_kernel, group),
        out_shape=jax.ShapeDtypeStruct(rot.shape, BF16),
        scratch_shapes=[pltpu.VMEM((seq_len, HEAD_DIM), F32)] * 2,
        compiler_params=params(),
        cost_estimate=cost(10 * pairs * HEAD_DIM, 8 * rot.size, pairs // 2),
        name="attn_bwd",
    )(rot, lse, dout, cos_tab, sin_tab)


def grad_in_kernel(n_rhs, *refs):
    lhs = refs[0][...]
    rhs_refs, done_refs, out_refs = refs[1:1 + n_rhs], refs[1 + n_rhs:-n_rhs], refs[-n_rhs:]
    for idx, (rhs_ref, out_ref) in enumerate(zip(rhs_refs, out_refs)):
        out_ref[0] = dot(lhs, rhs_ref[...], CONTRACT_FIRST).astype(BF16)
        for place, done_ref in enumerate(done_refs[idx::n_rhs]):
            out_ref[1 + place] = done_ref[...]


def grad_in(lhs, rhs_list, done, tile=512):
    seq_len, depth = lhs.shape
    n_rhs, n_layers = len(rhs_list), 1 + len(done)
    width = sum(rhs.shape[1] for rhs in rhs_list)
    return pl.pallas_call(
        functools.partial(grad_in_kernel, n_rhs),
        out_shape=[jax.ShapeDtypeStruct((n_layers, depth, rhs.shape[1]), BF16) for rhs in rhs_list],
        grid=(depth // tile,),
        in_specs=[pl.BlockSpec((seq_len, tile), lambda step: (0, step))]
        + [pl.BlockSpec(rhs.shape, lambda step: (0, 0), pipeline_mode=pl.Buffered(1)) for rhs in rhs_list]
        + [pl.BlockSpec((tile, item.shape[1]), lambda step: (step, 0)) for layer_done in done for item in layer_done],
        out_specs=[pl.BlockSpec((n_layers, tile, rhs.shape[1]), lambda step: (0, step, 0)) for rhs in rhs_list],
        compiler_params=params(),
        cost_estimate=cost(2 * seq_len * depth * width, 2 * (seq_len * depth + seq_len * width + (2 * n_layers - 1) * depth * width)),
        name="grad_in",
    )(lhs, *rhs_list, *[item for layer_done in done for item in layer_done])


def grad_out_kernel(attn_ref, hidden_ref, dy_ref, *refs):
    out_ref, down_ref = refs[-2:]

    @pl.when(pl.program_id(0) == 0)
    def _():
        out_ref[...] = dot(attn_ref[...], dy_ref[...], CONTRACT_FIRST).astype(BF16)

    down_ref[...] = dot(hidden_ref[...], dy_ref[...], CONTRACT_FIRST).astype(BF16)


def grad_out(attn_out, hidden, dy_full, layer, n_layers, previous, tile=512):
    seq_len, depth = dy_full.shape
    heads, ff = attn_out.shape[1], hidden.shape[1]
    return pl.pallas_call(
        grad_out_kernel,
        out_shape=(jax.ShapeDtypeStruct((n_layers, heads, depth), BF16), jax.ShapeDtypeStruct((n_layers, ff, depth), BF16)),
        grid=(ff // tile,),
        in_specs=[
            pl.BlockSpec((seq_len, heads), lambda step: (0, 0)),
            pl.BlockSpec((seq_len, tile), lambda step: (0, step)),
            pl.BlockSpec((seq_len, depth), lambda step: (0, 0), pipeline_mode=pl.Buffered(1)),
        ]
        + [pl.BlockSpec(memory_space=pl.ANY) for _ in previous],
        out_specs=[
            pl.BlockSpec((None, heads, depth), lambda step: (layer, 0, 0)),
            pl.BlockSpec((None, tile, depth), lambda step: (layer, step, 0)),
        ],
        input_output_aliases={3: 0, 4: 1} if previous else {},
        compiler_params=params(),
        cost_estimate=cost(2 * seq_len * depth * (heads + ff), 2 * (seq_len * depth + (seq_len + depth) * (heads + ff))),
        name="grad_out",
    )(attn_out, hidden, dy_full, *previous)


MESH = pl.DeviceIdType.MESH
CORES = 2


def ring_place(chips):
    me = lax.axis_index('tp')
    chip, core = me // CORES, lax.rem(me, CORES)
    left, right = lax.rem(chip + chips - 1, chips), lax.rem(chip + 1, chips)
    return chip, core, (chip * CORES + 1 - core, left * CORES + core, right * CORES + core)


def enter_ring(peers):
    barrier = pltpu.get_barrier_semaphore()
    for peer in peers:
        pl.semaphore_signal(barrier, inc=1, device_id={'tp': peer}, device_id_type=MESH)
    pl.semaphore_wait(barrier, len(peers))


def remote(src, dst, send, recv, index, peer):
    return pltpu.make_async_remote_copy(src_ref=src, dst_ref=dst, send_sem=send.at[index], recv_sem=recv.at[index], device_id={'tp': peer}, device_id_type=MESH)


def ring_gather(chips, loc_ref, full, send, recv, consume, meanwhile=None):
    n_rows = loc_ref.shape[0]
    half, quarter = n_rows // 2, n_rows // 4
    chip, core, (partner, left, right) = ring_place(chips)
    left_chip, right_chip, far_chip = lax.rem(chip + chips - 1, chips), lax.rem(chip + 1, chips), lax.rem(chip + 2, chips)

    def first_row(core_idx, item):
        return pl.multiple_of((item[0] * CORES + core_idx) * n_rows + item[1], item[2])

    def piece(core_idx, item):
        return full.at[pl.ds(first_row(core_idx, item), item[2])]

    low, high = (chip, 0, half), (chip, half, half)
    received = [
        (left_chip, 0, half), (right_chip, half, half), (left_chip, half, half), (right_chip, 0, half),
        (far_chip, 0, quarter), (far_chip, half, quarter), (far_chip, quarter, quarter), (far_chip, half + quarter, quarter),
    ]
    passed_on = [(left_chip, 0, quarter), (right_chip, half, quarter), (left_chip, quarter, quarter), (right_chip, half + quarter, quarter)]
    sends = [
        remote(loc_ref.at[pl.ds(item[1], half)], piece(core, item), send, recv, idx, peer)
        for idx, (item, peer) in enumerate([(low, right), (high, left), (high, right), (low, left)])
    ]
    sends += [remote(piece(core, item), piece(core, item), send, recv, 4 + idx, (right, left)[idx % 2]) for idx, item in enumerate(passed_on)]
    sends += [remote(piece(core, item), piece(core, item), send, recv, 8 + idx, partner) for idx, item in enumerate(received)]
    own = full.at[pl.ds(pl.multiple_of((chip * CORES + core) * n_rows, n_rows), n_rows)]
    other = full.at[pl.ds(pl.multiple_of((chip * CORES + 1 - core) * n_rows, n_rows), n_rows)]
    sends.append(remote(loc_ref, own, send, recv, 16, partner))
    landing = [piece(core, item) for item in received] + [piece(1 - core, item) for item in received] + [other]

    def arrived(index):
        remote(landing[index], landing[index], send, recv, index, partner).wait_recv()

    def hand_over(*indices):
        for index in indices:
            arrived(index)
            if index < 2:
                sends[4 + index].start()
                sends[6 + index].start()
            sends[8 + index].start()

    def use(group, items):
        consume(group, [first_row(idx, item) for item in items for idx in range(CORES)], items[0][2])

    enter_ring((partner, left, right))
    for index in (0, 1, 2, 3, 16):
        sends[index].start()
    own[...] = loc_ref[...]
    if meanwhile is not None:
        meanwhile()
        hand_over(0, 1)
    arrived(16)
    use(0, (low, high))
    if meanwhile is None:
        hand_over(0, 1)
    for group in range(1, 5):
        pair = (2 * group - 2, 2 * group - 1)
        if group > 1:
            hand_over(*pair)
        for index in pair:
            arrived(8 + index)
        use(group, received[2 * group - 2:2 * group])
    for copy in sends:
        copy.wait_send()


def gather_dots_kernel(chips, layer, forward, with_hidden, attn_group, tile, n_inputs, n_outs, loc_ref, *refs):
    n_weights = 3 if forward else 2
    inputs, outs = refs[:n_inputs], refs[n_inputs:n_inputs + n_outs]
    full, scratch = refs[n_inputs + n_outs], refs[n_inputs + n_outs + 1:]
    held, staged = scratch[:n_inputs], scratch[n_inputs:-5]
    load_sem, store_sem, attn_sem, send, recv = scratch[-5:]
    loads = [pltpu.make_async_copy(src.at[layer] if idx < n_weights else src, dst, load_sem.at[idx]) for idx, (src, dst) in enumerate(zip(inputs, held))]
    n_dots = n_weights + (1 if with_hidden else 0) if forward else 4
    attn_loads = loads[4:] if attn_group else []
    dot_loads = loads[:len(loads) - len(attn_loads)]
    for load in attn_loads + dot_loads:
        load.start()
    stores = []

    def attention():
        for load in attn_loads:
            load.wait()
        attn_fwd_kernel(attn_group, *held[4:], *staged[n_dots:])
        for idx, (src, dst) in enumerate(zip(staged[n_dots:], outs[-3:])):
            copy = pltpu.make_async_copy(src, dst, attn_sem.at[idx])
            copy.start()
            stores.append(copy)

    def consume(group, first_rows, count):
        pieces = [pl.ds(first, count) for first in first_rows]

        def rows_of(ref, cols=slice(None)):
            return jnp.concatenate([ref[rows, cols] for rows in pieces], axis=0)

        def put(ref, cols, value):
            for idx, rows in enumerate(pieces):
                ref[rows, cols] = value[idx * count:(idx + 1) * count]

        if not group:
            dot_loads[0].wait()
        put(staged[0], slice(None), dot(rows_of(full), held[0][...], MATMUL if forward else CONTRACT_LAST).astype(BF16))
        if not group:
            for load in dot_loads[1:]:
                load.wait()

        def one_tile(idx, carry):
            cols = pl.ds(pl.multiple_of(idx * tile, tile), tile)
            if forward:
                gate = dot(rows_of(full), held[1][:, cols], MATMUL).astype(BF16)
                up = dot(rows_of(full), held[2][:, cols], MATMUL).astype(BF16)
                put(staged[1], cols, gate)
                put(staged[2], cols, up)
                if with_hidden:
                    put(staged[3], cols, gated(gate.astype(F32), up.astype(F32)).astype(BF16))
            else:
                d_hidden = dot(rows_of(full), held[1][cols, :], CONTRACT_LAST).astype(BF16).astype(F32)
                hidden, pull = jax.vjp(gated, rows_of(held[2], cols).astype(F32), rows_of(held[3], cols).astype(F32))
                d_gate, d_up = pull(d_hidden)
                put(staged[1], cols, hidden.astype(BF16))
                put(staged[2], cols, d_gate.astype(BF16))
                put(staged[3], cols, d_up.astype(BF16))
            return carry

        lax.fori_loop(0, staged[1].shape[1] // tile, one_tile, 0)
        sources = list(staged[:n_dots]) + ([] if forward else [full])
        for idx, source in enumerate(sources):
            for place, rows in enumerate(pieces):
                copy = pltpu.make_async_copy(source.at[rows], outs[idx].at[rows], store_sem.at[group, place, idx])
                copy.start()
                stores.append(copy)

    ring_gather(chips, loc_ref, full, send, recv, consume, attention if attn_group else None)
    for copy in stores:
        copy.wait()


def gather_dots(loc, inputs, layer, forward, with_hidden, tp_size, collective_id, name, attn_inputs=(), tile=256):
    n_rows, depth = loc.shape
    seq_len, chips = n_rows * tp_size, tp_size // CORES
    n_weights = 3 if forward else 2
    weights, saved = inputs[:n_weights], tuple(inputs[n_weights:]) + tuple(attn_inputs)
    if forward:
        widths = [weight.shape[2] for weight in weights] + ([weights[1].shape[2]] if with_hidden else [])
    else:
        widths = [weights[0].shape[1]] + [weights[1].shape[1]] * 3
    staged = [((seq_len, width), BF16) for width in widths]
    attn_group = weights[0].shape[1] // HEAD_DIM if attn_inputs else 0
    attn_outs = []
    if attn_inputs:
        attn_outs = [(attn_inputs[0].shape, BF16), ((seq_len, weights[0].shape[1]), BF16), ((seq_len, weights[0].shape[1]), F32)]
    outs = staged + ([] if forward else [((seq_len, depth), BF16)]) + attn_outs
    n_cols = sum(weight.size // (weight.shape[0] * depth) for weight in weights)
    all_inputs = tuple(inputs) + tuple(attn_inputs)
    return pl.pallas_call(
        functools.partial(gather_dots_kernel, chips, layer, forward, with_hidden, attn_group, tile, len(all_inputs), len(outs)),
        out_shape=[jax.ShapeDtypeStruct(*item) for item in outs],
        in_specs=[pl.BlockSpec(memory_space=pltpu.VMEM)] + [pl.BlockSpec(memory_space=pl.ANY)] * len(all_inputs),
        out_specs=[pl.BlockSpec(memory_space=pl.ANY)] * len(outs),
        scratch_shapes=[pltpu.VMEM((seq_len, depth), BF16)]
        + [pltpu.VMEM(weight.shape[1:], BF16) for weight in weights]
        + [pltpu.VMEM(item.shape, item.dtype) for item in saved]
        + [pltpu.VMEM(*item) for item in staged + attn_outs]
        + [
            pltpu.SemaphoreType.DMA((len(all_inputs),)),
            pltpu.SemaphoreType.DMA((5, 2 * CORES, len(outs))),
            pltpu.SemaphoreType.DMA((3,)),
            pltpu.SemaphoreType.DMA((17,)),
            pltpu.SemaphoreType.DMA((17,)),
        ],
        compiler_params=pltpu.CompilerParams(vmem_limit_bytes=VMEM_LIMIT, collective_id=collective_id, has_side_effects=True),
        cost_estimate=cost(2 * seq_len * depth * n_cols, 2 * (seq_len * depth + depth * n_cols + seq_len * n_cols)),
        name=name,
    )(loc, *all_inputs)


def weight_grads(u_ref, rhs_refs, grad_refs, u_held, grads_held, u_sem, grad_sem):
    tile = u_held.shape[2]
    n_tiles = u_ref.shape[1] // tile
    starts = [sum(rhs.shape[1] for rhs in rhs_refs[:idx]) for idx in range(len(rhs_refs))]

    def load(idx, slot):
        return pltpu.make_async_copy(u_ref.at[:, pl.ds(pl.multiple_of(idx * tile, tile), tile)], u_held.at[slot], u_sem.at[slot])

    def stores(idx, slot):
        rows = pl.ds(pl.multiple_of(idx * tile, tile), tile)
        return [
            pltpu.make_async_copy(grads_held.at[slot, :, pl.ds(start, rhs.shape[1])], grad.at[rows, :], grad_sem.at[slot, place])
            for place, (start, rhs, grad) in enumerate(zip(starts, rhs_refs, grad_refs))
        ]

    load(0, 0).start()

    def one_tile(idx, carry):
        slot = lax.rem(idx, 2)

        @pl.when(idx + 1 < n_tiles)
        def _():
            load(idx + 1, 1 - slot).start()

        @pl.when(idx >= 2)
        def _():
            for store in stores(idx - 2, slot):
                store.wait()

        load(idx, slot).wait()
        lhs = u_held[slot]
        for start, rhs in zip(starts, rhs_refs):
            grads_held[slot, :, pl.ds(start, rhs.shape[1])] = dot(lhs, rhs[...], CONTRACT_FIRST).astype(BF16)
        for store in stores(idx, slot):
            store.start()
        return carry

    lax.fori_loop(0, n_tiles, one_tile, 0)
    for idx in range(max(n_tiles - 2, 0), n_tiles):
        for store in stores(idx, idx % 2):
            store.wait()


def dots_scatter_kernel(chips, layer, dims, n_terms, tile, with_grads, *refs):
    lhs_hbm, rhs_refs, refs = refs[:n_terms], refs[n_terms:2 * n_terms], refs[2 * n_terms:]
    if with_grads:
        u_ref, refs = refs[0], refs[1:]
    out_ref, refs = refs[0], refs[1:]
    if with_grads:
        grad_refs, refs = refs[:n_terms], refs[n_terms:]
    lhs_refs, held, scratch = refs[:n_terms], refs[n_terms:2 * n_terms], refs[2 * n_terms:]
    part, acc, from_far, from_side, lhs_sem, load_sem, core_send, core_recv, send, recv = scratch[:10]
    n_rows, n_cols = out_ref.shape
    half = n_cols // 2
    n_tiles = half // tile
    chip, core, (partner, left, right) = ring_place(chips)
    dest_chips = [lax.rem(chip + offset, chips) for offset in (2, chips - 1, 1, 0)]

    chip_rows = CORES * n_rows

    def rows_of(step):
        return pl.ds(pl.multiple_of(dest_chips[step] * chip_rows, chip_rows), chip_rows)

    def cols_of(which, idx):
        return pl.ds(pl.multiple_of(which * half + idx * tile, tile), tile)

    def lhs_loads(step):
        return [pltpu.make_async_copy(src.at[rows_of(step)], dst.at[rows_of(step)], lhs_sem.at[step, place]) for place, (src, dst) in enumerate(zip(lhs_hbm, lhs_refs))]

    def rhs_loads(which, idx):
        cols = cols_of(which, idx)
        if dims is MATMUL:
            pairs = [(src.at[layer, :, cols], dst.at[:, cols]) for src, dst in zip(rhs_refs, held)]
        else:
            pairs = [(src.at[layer, cols, :], dst.at[cols, :]) for src, dst in zip(rhs_refs, held)]
        return [pltpu.make_async_copy(src, dst, load_sem.at[which * n_tiles + idx, place]) for place, (src, dst) in enumerate(pairs)]

    for load in lhs_loads(0):
        load.start()
    for idx in range(n_tiles):
        for which in range(2):
            for load in rhs_loads(which, idx):
                load.start()
    for step in range(1, 4):
        for load in lhs_loads(step):
            load.start()
    enter_ring((partner, left, right))

    def to_core(step, which, idx):
        slot = which * n_tiles + idx
        return remote(part.at[which, 1 - core], acc.at[step, slot], core_send, core_recv, step * 2 * n_tiles + slot, partner)

    def hop(step, which, idx):
        slot = which * n_tiles + idx
        if not step:
            return remote(acc.at[0, slot], from_far.at[slot], send, recv, slot, left if which else right)
        side = 1 if step == 1 else 0
        return remote(acc.at[step, slot], from_side.at[side, slot], send, recv, step * 2 * n_tiles + slot, left if side else right)

    def compute(step, which, idx):
        rows, rhs_cols = rows_of(step), cols_of(which, idx)
        if not step:
            for load in rhs_loads(which, idx):
                load.wait()
        total = None
        for lhs_ref, rhs_ref in zip(lhs_refs, held):
            rhs = rhs_ref[:, rhs_cols] if dims is MATMUL else rhs_ref[rhs_cols, :]
            product = dot(lhs_ref[rows, :], rhs, dims)
            total = product if total is None else total + product
        for idx_core in range(CORES):
            part[which, idx_core] = total[idx_core * n_rows:(idx_core + 1) * n_rows]
        to_core(step, which, idx).start()

    def add_core(step, which, idx, hop_now):
        copy = to_core(step, which, idx)
        copy.wait_recv()
        slot = which * n_tiles + idx
        acc[step, slot] = acc[step, slot] + part[which, core]
        copy.wait_send()
        if hop_now:
            hop(step, which, idx).start()

    for first, second, hop_now in (((0, 0), (0, 1), True), ((1, 0), (2, 1), True), ((2, 0), (1, 1), False), ((3, 0), (3, 1), False)):
        for step in {first[0]: 0, second[0]: 0} if hop_now else ():
            for load in lhs_loads(step):
                load.wait()
        if first[0] == 3:
            for load in lhs_loads(3):
                load.wait()

        def one_pair(idx, carry):
            compute(*first, idx)

            @pl.when(idx > 0)
            def _():
                add_core(*second, idx - 1, hop_now)

            compute(*second, idx)
            add_core(*first, idx, hop_now)
            return carry

        lax.fori_loop(0, n_tiles, one_pair, 0)
        add_core(*second, n_tiles - 1, hop_now)

    def pass_on(idx, carry):
        for step, which in ((2, 0), (1, 1)):
            slot = which * n_tiles + idx
            hop(0, which, idx).wait_recv()
            acc[step, slot] = acc[step, slot] + from_far[slot]
            hop(step, which, idx).start()
        return carry

    lax.fori_loop(0, n_tiles, pass_on, 0)
    if with_grads:
        weight_grads(u_ref, lhs_refs, grad_refs, *scratch[10:])
    for which in range(2):
        for idx in range(n_tiles):
            slot = which * n_tiles + idx
            hop(1, which, idx).wait_recv()
            hop(2, which, idx).wait_recv()
            out_ref[:, pl.ds(slot * tile, tile)] = acc[3, slot] + from_side[0, slot] + from_side[1, slot]
    for step in range(3):
        for which in range(2):
            for idx in range(n_tiles):
                hop(step, which, idx).wait_send()


def dots_scatter(terms, layer, dims, tp_size, collective_id, name, u_full=None, tile=512, grad_tile=512):
    seq_len = terms[0][0].shape[0]
    n_cols = terms[0][1].shape[2] if dims is MATMUL else terms[0][1].shape[1]
    n_rows = seq_len // tp_size
    depth = sum(lhs.shape[1] for lhs, _ in terms)
    with_grads = u_full is not None
    n_terms = len(terms)
    any_spec, vmem_spec = pl.BlockSpec(memory_space=pl.ANY), pl.BlockSpec(memory_space=pltpu.VMEM)
    outs, extra_inputs, extra_scratch = [jax.ShapeDtypeStruct((n_rows, n_cols), F32)], (), []
    if with_grads:
        outs += [jax.ShapeDtypeStruct((n_cols, lhs.shape[1]), BF16) for lhs, _ in terms]
        extra_inputs = (u_full,)
        extra_scratch = [
            pltpu.VMEM((2, seq_len, grad_tile), BF16),
            pltpu.VMEM((2, grad_tile, depth), BF16),
            pltpu.SemaphoreType.DMA((2,)),
            pltpu.SemaphoreType.DMA((2, n_terms)),
        ]
    results = pl.pallas_call(
        functools.partial(dots_scatter_kernel, tp_size // CORES, layer, dims, n_terms, tile, with_grads),
        out_shape=outs,
        in_specs=[any_spec] * (2 * n_terms + len(extra_inputs)),
        out_specs=[vmem_spec] + [any_spec] * (len(outs) - 1),
        scratch_shapes=[pltpu.VMEM(lhs.shape, BF16) for lhs, _ in terms]
        + [pltpu.VMEM(rhs.shape[1:], BF16) for _, rhs in terms]
        + [
            pltpu.VMEM((2, CORES, n_rows, tile), F32),
            pltpu.VMEM((4, n_cols // tile, n_rows, tile), F32),
            pltpu.VMEM((n_cols // tile, n_rows, tile), F32),
            pltpu.VMEM((2, n_cols // tile, n_rows, tile), F32),
            pltpu.SemaphoreType.DMA((4, n_terms)),
            pltpu.SemaphoreType.DMA((n_cols // tile, n_terms)),
            pltpu.SemaphoreType.DMA((4 * n_cols // tile,)),
            pltpu.SemaphoreType.DMA((4 * n_cols // tile,)),
            pltpu.SemaphoreType.DMA((3 * n_cols // tile,)),
            pltpu.SemaphoreType.DMA((3 * n_cols // tile,)),
        ]
        + extra_scratch,
        compiler_params=pltpu.CompilerParams(vmem_limit_bytes=VMEM_LIMIT, collective_id=collective_id, has_side_effects=True),
        cost_estimate=cost(2 * seq_len * depth * n_cols * (2 if with_grads else 1), 2 * depth * (seq_len + n_cols) + 4 * n_rows * n_cols),
        name=name,
    )(*[lhs for lhs, _ in terms], *[rhs for _, rhs in terms], *extra_inputs)
    return (results[0], tuple(results[1:])) if with_grads else results[0]


def gather_rows(rows_loc):
    return lax.all_gather(rows_loc, 'tp', axis=0, tiled=True)


def after(value, *others):
    return lax.optimization_barrier((value,) + others)[0]


def solution(mesh):
    tp_size = mesh.shape['tp']
    row_spec = P(('dp', 'tp'), None)
    col_spec = P(None, None, 'tp')
    inner_spec = P(None, 'tp', None)

    def sum_over_tp(value):
        stride = 1
        while stride < tp_size:
            value = value + lax.ppermute(value, 'tp', [(idx, idx ^ stride) for idx in range(tp_size)])
            stride *= 2
        return value

    def device_program(x_loc, dy_loc, norm_gain, w_qkv, w_out, w_gate, w_up, w_down):
        n_layers, depth = w_qkv.shape[0], w_qkv.shape[1]
        group = w_out.shape[1] // HEAD_DIM
        seq_len = x_loc.shape[0] * tp_size
        cos_tab, sin_tab = rope_tables(seq_len)
        saved_all = []
        x_cur = x_loc
        for layer in range(n_layers):
            last = layer == n_layers - 1
            x_f32 = x_cur.astype(F32)
            u_loc = rms_scale(x_f32, norm_gain[layer]).astype(BF16)
            outs = gather_dots(u_loc, (w_qkv, w_gate, w_up), layer, True, not last, tp_size, layer, "gather_in")
            qkv, gate, up = outs[:3]
            rot, attn_out, lse = (qkv, None, None) if last else attn_fwd(qkv, cos_tab, sin_tab, group)
            saved_all.append((x_cur, u_loc, rot, attn_out, lse, gate, up))
            if not last:
                block_sum = dots_scatter([(attn_out, w_out), (outs[3], w_down)], layer, MATMUL, tp_size, n_layers + layer, "scatter_out")
                x_cur = (x_f32 + block_sum).astype(BF16)

        out_grads, gain_grads, done_grads = (), [], []
        for layer in reversed(range(n_layers)):
            x_in, u_loc, rot, attn_out, lse, gate, up = saved_all[layer]
            last = layer == n_layers - 1
            attn_inputs = (rot, cos_tab, sin_tab) if last else ()
            outs = gather_dots(dy_loc, (w_out, w_down, gate, up), layer, False, True, tp_size, 2 * n_layers + layer, "gather_back", attn_inputs)
            d_attn, hidden, d_gate, d_up, dy_full = outs[:5]
            if last:
                rot, attn_out, lse = outs[5:]
            u_full = gather_rows(after(u_loc, attn_out, d_attn))
            d_qkv = attn_bwd(rot, lse, d_attn, cos_tab, sin_tab, group)
            out_grads = grad_out(attn_out, hidden, dy_full, layer, n_layers, out_grads)
            d_qkv, u_full, out_grads = lax.optimization_barrier((d_qkv, u_full, out_grads))
            terms = [(d_qkv, w_qkv), (d_gate, w_gate), (d_up, w_up)]
            if layer:
                d_normed, done = dots_scatter(terms, layer, CONTRACT_LAST, tp_size, 3 * n_layers + layer, "scatter_back", u_full)
                done_grads.insert(0, done)
            else:
                d_normed = dots_scatter(terms, layer, CONTRACT_LAST, tp_size, 3 * n_layers + layer, "scatter_back")
                d_normed, u_full, d_qkv, d_gate, d_up = lax.optimization_barrier((d_normed, u_full, d_qkv, d_gate, d_up))
                in_grads = grad_in(u_full, (d_qkv, d_gate, d_up), done_grads)
            d_normed = d_normed.astype(BF16)
            norm_pull = jax.vjp(rms_scale, x_in.astype(F32), norm_gain[layer])[1]
            d_x_norm, gain_grad = norm_pull(d_normed.astype(F32))
            dy_loc = (dy_loc.astype(F32) + d_x_norm).astype(BF16)
            gain_grads.insert(0, gain_grad)
        grad_gain = sum_over_tp(jnp.stack(gain_grads))
        return (dy_loc, grad_gain, in_grads[0], out_grads[0], in_grads[1], in_grads[2], out_grads[1])

    return jax.shard_map(device_program, mesh=mesh, in_specs=(row_spec, row_spec, P(None, None), col_spec, inner_spec, col_spec, col_spec, inner_spec), out_specs=(row_spec, P('dp', None), P('dp', None, 'tp'), P('dp', 'tp', None), P('dp', None, 'tp'), P('dp', None, 'tp'), P('dp', 'tp', None)), check_vma=False)
```

```python
import functools

import jax
import jax.numpy as jnp
import numpy as np
from jax import lax
from jax.experimental import pallas as pl
from jax.experimental.pallas import tpu as pltpu
from jax.sharding import PartitionSpec as P

HEAD_DIM = 128
NORM_EPS = 1e-5
ROPE_BASE = 10000.0
Q_BLOCK = 256
FINISH_ROWS = 32
VMEM_LIMIT = 63 * 1024 * 1024
F32 = jnp.float32
BF16 = jnp.bfloat16

CONTRACT_LAST = (((1,), (1,)), ((), ()))
CONTRACT_FIRST = (((0,), (0,)), ((), ()))
MATMUL = (((1,), (0,)), ((), ()))


def dot(lhs, rhs, dims):
    return lax.dot_general(lhs, rhs, dims, preferred_element_type=F32)


def params():
    return pltpu.CompilerParams(vmem_limit_bytes=VMEM_LIMIT)


def cost(flops, bytes_accessed, transcendentals=0):
    return pl.CostEstimate(flops=int(flops), bytes_accessed=int(bytes_accessed), transcendentals=int(transcendentals))


def rope_tables(seq_len):
    half_dim = HEAD_DIM // 2
    freqs = (ROPE_BASE ** (-2.0 * np.arange(half_dim) / HEAD_DIM)).astype(np.float32)
    angles = (np.arange(seq_len, dtype=np.float32)[:, None] * freqs[None, :]).astype(np.float64)
    cos, sin = np.cos(angles).astype(np.float32), np.sin(angles).astype(np.float32)
    return jnp.asarray(np.concatenate([cos, cos], axis=-1)), jnp.asarray(np.concatenate([-sin, sin], axis=-1))


def rms_scale(x_f32, gain_row):
    inv_rms = lax.rsqrt(jnp.mean(x_f32 * x_f32, axis=-1, keepdims=True) + NORM_EPS)
    return x_f32 * inv_rms * gain_row


def gated(gate_f32, up_f32):
    return jax.nn.silu(gate_f32) * up_f32


def head_cols(index):
    return pl.ds(pl.multiple_of(index * HEAD_DIM, HEAD_DIM), HEAD_DIM)


def diagonal_mask():
    return lax.broadcasted_iota(jnp.int32, (Q_BLOCK, Q_BLOCK), 0) >= lax.broadcasted_iota(jnp.int32, (Q_BLOCK, Q_BLOCK), 1)


def attn_fwd_kernel(group, qkv_ref, cos_ref, sin_ref, rot_ref, out_ref, lse_ref):
    seq_len = qkv_ref.shape[0]
    scale = HEAD_DIM ** -0.5
    key, val = pl.ds(group * HEAD_DIM, HEAD_DIM), pl.ds((group + 1) * HEAD_DIM, HEAD_DIM)

    def rotate_head(head, carry):
        values = qkv_ref[:, head_cols(head)].astype(F32)
        rot_ref[:, head_cols(head)] = (values * cos_ref[...] + pltpu.roll(values, HEAD_DIM // 2, 1) * sin_ref[...]).astype(BF16)
        return carry

    lax.fori_loop(0, group + 1, rotate_head, 0)
    rot_ref[:, val] = qkv_ref[:, val]
    for block in range(seq_len // Q_BLOCK):
        start = block * Q_BLOCK
        rows = pl.ds(start, Q_BLOCK)

        def one_head(head, carry):
            query = rot_ref[rows, head_cols(head)]
            diag = jnp.where(diagonal_mask(), dot(query, rot_ref[rows, key], CONTRACT_LAST) * scale, -1e30)
            row_max = jnp.max(diag, axis=-1, keepdims=True)
            if start:
                past = dot(query, rot_ref[pl.ds(0, start), key], CONTRACT_LAST) * scale
                row_max = jnp.maximum(row_max, jnp.max(past, axis=-1, keepdims=True))
            diag = jnp.exp(diag - row_max)
            total = jnp.sum(diag, axis=-1, keepdims=True)
            if start:
                past = jnp.exp(past - row_max)
                total = total + jnp.sum(past, axis=-1, keepdims=True)
            inverse = 1.0 / total
            acc = dot((diag * inverse).astype(BF16), rot_ref[rows, val], MATMUL)
            if start:
                acc = acc + dot((past * inverse).astype(BF16), rot_ref[pl.ds(0, start), val], MATMUL)
            out_ref[rows, head_cols(head)] = acc.astype(BF16)
            lse_ref[rows, head_cols(head)] = jnp.broadcast_to(row_max + jnp.log(total), (Q_BLOCK, HEAD_DIM))
            return carry

        lax.fori_loop(0, group, one_head, 0)


def attn_fwd(qkv, cos_tab, sin_tab, group):
    seq_len = qkv.shape[0]
    pairs = group * seq_len * seq_len
    return pl.pallas_call(
        functools.partial(attn_fwd_kernel, group),
        out_shape=(
            jax.ShapeDtypeStruct(qkv.shape, BF16),
            jax.ShapeDtypeStruct((seq_len, group * HEAD_DIM), BF16),
            jax.ShapeDtypeStruct((seq_len, group * HEAD_DIM), F32),
        ),
        compiler_params=params(),
        cost_estimate=cost(4 * pairs * HEAD_DIM, 8 * qkv.size, pairs // 2),
        name="attn_fwd",
    )(qkv, cos_tab, sin_tab)


def attn_bwd_kernel(group, rot_ref, lse_ref, dout_ref, cos_ref, sin_ref, dqkv_ref, dkey_ref, dval_ref):
    seq_len = rot_ref.shape[0]
    scale = HEAD_DIM ** -0.5
    key, val = pl.ds(group * HEAD_DIM, HEAD_DIM), pl.ds((group + 1) * HEAD_DIM, HEAD_DIM)
    dkey_ref[...] = jnp.zeros_like(dkey_ref)
    dval_ref[...] = jnp.zeros_like(dval_ref)

    def unrotate(values, rows):
        values = values.astype(BF16).astype(F32)
        return (values * cos_ref[rows, :] - pltpu.roll(values, HEAD_DIM // 2, 1) * sin_ref[rows, :]).astype(BF16)

    for block in range(seq_len // Q_BLOCK):
        start = block * Q_BLOCK
        rows = pl.ds(start, Q_BLOCK)

        def one_head(head, carry):
            query = rot_ref[rows, head_cols(head)]
            dout = dout_ref[rows, head_cols(head)]
            lse = lse_ref[rows, head_cols(head)][:, :1]

            def probs(cols, masked):
                scores = dot(query, rot_ref[cols, key], CONTRACT_LAST) * scale
                if masked:
                    scores = jnp.where(diagonal_mask(), scores, -1e30)
                prob = jnp.exp(scores - lse)
                dprob = dot(dout, rot_ref[cols, val], CONTRACT_LAST).astype(BF16).astype(F32)
                dval_ref[cols, :] += dot(prob.astype(BF16), dout, CONTRACT_FIRST)
                return prob, dprob, jnp.sum(prob * dprob, axis=-1, keepdims=True)

            def finish(cols, prob, dprob, delta):
                dscore = (prob * (dprob - delta) * scale).astype(BF16)
                dkey_ref[cols, :] += dot(dscore, query, CONTRACT_FIRST)
                return dot(dscore, rot_ref[cols, key], MATMUL)

            prob, dprob, delta = probs(rows, True)
            if start:
                past = pl.ds(0, start)
                past_prob, past_dprob, past_delta = probs(past, False)
                delta = delta + past_delta
            dquery = finish(rows, prob, dprob, delta)
            if start:
                dquery = dquery + finish(past, past_prob, past_dprob, delta)
            dqkv_ref[rows, head_cols(head)] = unrotate(dquery, rows)
            return carry

        lax.fori_loop(0, group, one_head, 0)
    dqkv_ref[:, key] = unrotate(dkey_ref[...], pl.ds(0, seq_len))
    dqkv_ref[:, val] = dval_ref[...].astype(BF16)


def attn_bwd(rot, lse, dout, cos_tab, sin_tab, group):
    seq_len = rot.shape[0]
    pairs = group * seq_len * seq_len
    return pl.pallas_call(
        functools.partial(attn_bwd_kernel, group),
        out_shape=jax.ShapeDtypeStruct(rot.shape, BF16),
        scratch_shapes=[pltpu.VMEM((seq_len, HEAD_DIM), F32)] * 2,
        compiler_params=params(),
        cost_estimate=cost(10 * pairs * HEAD_DIM, 8 * rot.size, pairs // 2),
        name="attn_bwd",
    )(rot, lse, dout, cos_tab, sin_tab)


def grad_in_kernel(n_rhs, *refs):
    lhs = refs[0][...]
    rhs_refs, done_refs, out_refs = refs[1:1 + n_rhs], refs[1 + n_rhs:-n_rhs], refs[-n_rhs:]
    for idx, (rhs_ref, out_ref) in enumerate(zip(rhs_refs, out_refs)):
        out_ref[0] = dot(lhs, rhs_ref[...], CONTRACT_FIRST).astype(BF16)
        for place, done_ref in enumerate(done_refs[idx::n_rhs]):
            out_ref[1 + place] = done_ref[...]


def grad_in(lhs, rhs_list, done, tile=512):
    seq_len, depth = lhs.shape
    n_rhs, n_layers = len(rhs_list), 1 + len(done)
    width = sum(rhs.shape[1] for rhs in rhs_list)
    return pl.pallas_call(
        functools.partial(grad_in_kernel, n_rhs),
        out_shape=[jax.ShapeDtypeStruct((n_layers, depth, rhs.shape[1]), BF16) for rhs in rhs_list],
        grid=(depth // tile,),
        in_specs=[pl.BlockSpec((seq_len, tile), lambda step: (0, step))]
        + [pl.BlockSpec(rhs.shape, lambda step: (0, 0), pipeline_mode=pl.Buffered(1)) for rhs in rhs_list]
        + [pl.BlockSpec((tile, item.shape[1]), lambda step: (step, 0)) for layer_done in done for item in layer_done],
        out_specs=[pl.BlockSpec((n_layers, tile, rhs.shape[1]), lambda step: (0, step, 0)) for rhs in rhs_list],
        compiler_params=params(),
        cost_estimate=cost(2 * seq_len * depth * width, 2 * (seq_len * depth + seq_len * width + (2 * n_layers - 1) * depth * width)),
        name="grad_in",
    )(lhs, *rhs_list, *[item for layer_done in done for item in layer_done])


def grad_out_kernel(attn_ref, hidden_ref, dy_ref, *refs):
    out_ref, down_ref = refs[-2:]

    @pl.when(pl.program_id(0) == 0)
    def _():
        out_ref[...] = dot(attn_ref[...], dy_ref[...], CONTRACT_FIRST).astype(BF16)

    down_ref[...] = dot(hidden_ref[...], dy_ref[...], CONTRACT_FIRST).astype(BF16)


def grad_out(attn_out, hidden, dy_full, layer, n_layers, previous, tile=512):
    seq_len, depth = dy_full.shape
    heads, ff = attn_out.shape[1], hidden.shape[1]
    return pl.pallas_call(
        grad_out_kernel,
        out_shape=(jax.ShapeDtypeStruct((n_layers, heads, depth), BF16), jax.ShapeDtypeStruct((n_layers, ff, depth), BF16)),
        grid=(ff // tile,),
        in_specs=[
            pl.BlockSpec((seq_len, heads), lambda step: (0, 0)),
            pl.BlockSpec((seq_len, tile), lambda step: (0, step)),
            pl.BlockSpec((seq_len, depth), lambda step: (0, 0), pipeline_mode=pl.Buffered(1)),
        ]
        + [pl.BlockSpec(memory_space=pl.ANY) for _ in previous],
        out_specs=[
            pl.BlockSpec((None, heads, depth), lambda step: (layer, 0, 0)),
            pl.BlockSpec((None, tile, depth), lambda step: (layer, step, 0)),
        ],
        input_output_aliases={3: 0, 4: 1} if previous else {},
        compiler_params=params(),
        cost_estimate=cost(2 * seq_len * depth * (heads + ff), 2 * (seq_len * depth + (seq_len + depth) * (heads + ff))),
        name="grad_out",
    )(attn_out, hidden, dy_full, *previous)


MESH = pl.DeviceIdType.MESH
CORES = 2


def ring_place(chips):
    me = lax.axis_index('tp')
    chip, core = me // CORES, lax.rem(me, CORES)
    left, right = lax.rem(chip + chips - 1, chips), lax.rem(chip + 1, chips)
    return chip, core, (chip * CORES + 1 - core, left * CORES + core, right * CORES + core)


def enter_ring(peers):
    barrier = pltpu.get_barrier_semaphore()
    for peer in peers:
        pl.semaphore_signal(barrier, inc=1, device_id={'tp': peer}, device_id_type=MESH)
    pl.semaphore_wait(barrier, len(peers))


def remote(src, dst, send, recv, index, peer):
    return pltpu.make_async_remote_copy(src_ref=src, dst_ref=dst, send_sem=send.at[index], recv_sem=recv.at[index], device_id={'tp': peer}, device_id_type=MESH)


def ring_gather(chips, loc_ref, full, send, recv, consume, meanwhile=None):
    n_rows = loc_ref.shape[0]
    half, quarter = n_rows // 2, n_rows // 4
    chip, core, (partner, left, right) = ring_place(chips)
    left_chip, right_chip, far_chip = lax.rem(chip + chips - 1, chips), lax.rem(chip + 1, chips), lax.rem(chip + 2, chips)

    def first_row(core_idx, item):
        return pl.multiple_of((item[0] * CORES + core_idx) * n_rows + item[1], item[2])

    def piece(core_idx, item):
        return full.at[pl.ds(first_row(core_idx, item), item[2])]

    low, high = (chip, 0, half), (chip, half, half)
    received = [
        (left_chip, 0, half), (right_chip, half, half), (left_chip, half, half), (right_chip, 0, half),
        (far_chip, 0, quarter), (far_chip, half, quarter), (far_chip, quarter, quarter), (far_chip, half + quarter, quarter),
    ]
    passed_on = [(left_chip, 0, quarter), (right_chip, half, quarter), (left_chip, quarter, quarter), (right_chip, half + quarter, quarter)]
    sends = [
        remote(loc_ref.at[pl.ds(item[1], half)], piece(core, item), send, recv, idx, peer)
        for idx, (item, peer) in enumerate([(low, right), (high, left), (high, right), (low, left)])
    ]
    sends += [remote(piece(core, item), piece(core, item), send, recv, 4 + idx, (right, left)[idx % 2]) for idx, item in enumerate(passed_on)]
    sends += [remote(piece(core, item), piece(core, item), send, recv, 8 + idx, partner) for idx, item in enumerate(received)]
    own = full.at[pl.ds(pl.multiple_of((chip * CORES + core) * n_rows, n_rows), n_rows)]
    other = full.at[pl.ds(pl.multiple_of((chip * CORES + 1 - core) * n_rows, n_rows), n_rows)]
    sends.append(remote(loc_ref, own, send, recv, 16, partner))
    landing = [piece(core, item) for item in received] + [piece(1 - core, item) for item in received] + [other]

    def arrived(index):
        remote(landing[index], landing[index], send, recv, index, partner).wait_recv()

    def hand_over(*indices):
        for index in indices:
            arrived(index)
            if index < 2:
                sends[4 + index].start()
                sends[6 + index].start()
            sends[8 + index].start()

    def use(group, items):
        consume(group, [first_row(idx, item) for item in items for idx in range(CORES)], items[0][2])

    enter_ring((partner, left, right))
    for index in (0, 1, 2, 3, 16):
        sends[index].start()
    own[...] = loc_ref[...]
    if meanwhile is not None:
        meanwhile()
        hand_over(0, 1)
    arrived(16)
    use(0, (low, high))
    if meanwhile is None:
        hand_over(0, 1)
    for group in range(1, 5):
        pair = (2 * group - 2, 2 * group - 1)
        if group > 1:
            hand_over(*pair)
        for index in pair:
            arrived(8 + index)
        use(group, received[2 * group - 2:2 * group])
    for copy in sends:
        copy.wait_send()


def gather_dots_kernel(chips, layer, forward, with_hidden, attn_group, tile, n_inputs, n_outs, loc_ref, *refs):
    n_weights = 3 if forward else 2
    inputs, outs = refs[:n_inputs], refs[n_inputs:n_inputs + n_outs]
    full, scratch = refs[n_inputs + n_outs], refs[n_inputs + n_outs + 1:]
    held, staged = scratch[:n_inputs], scratch[n_inputs:-5]
    load_sem, store_sem, attn_sem, send, recv = scratch[-5:]
    n_tiles = staged[1].shape[1] // tile
    n_whole = 1 if forward else n_inputs
    loads = [
        pltpu.make_async_copy(src.at[layer] if idx < n_weights else src, dst, load_sem.at[idx, 0])
        for idx, (src, dst) in enumerate(zip(inputs[:n_whole], held[:n_whole]))
    ]

    def tile_loads(idx):
        cols = pl.ds(pl.multiple_of(idx * tile, tile), tile)
        return [pltpu.make_async_copy(inputs[place].at[layer, :, cols], held[place].at[:, cols], load_sem.at[place, idx]) for place in range(1, n_weights)]

    n_dots = n_weights + (1 if with_hidden else 0) if forward else 4
    attn_loads = loads[4:] if attn_group else []
    dot_loads = loads[:len(loads) - len(attn_loads)]
    for load in attn_loads + dot_loads:
        load.start()
    if forward:
        for idx in range(n_tiles):
            for load in tile_loads(idx):
                load.start()
    stores = []

    def attention():
        for load in attn_loads:
            load.wait()
        attn_fwd_kernel(attn_group, *held[4:], *staged[n_dots:])
        for idx, (src, dst) in enumerate(zip(staged[n_dots:], outs[-3:])):
            copy = pltpu.make_async_copy(src, dst, attn_sem.at[idx])
            copy.start()
            stores.append(copy)

    def consume(group, first_rows, count):
        pieces = [pl.ds(first, count) for first in first_rows]

        def rows_of(ref, cols=slice(None)):
            return jnp.concatenate([ref[rows, cols] for rows in pieces], axis=0)

        def put(ref, cols, value):
            for idx, rows in enumerate(pieces):
                ref[rows, cols] = value[idx * count:(idx + 1) * count]

        if not group:
            dot_loads[0].wait()
        put(staged[0], slice(None), dot(rows_of(full), held[0][...], MATMUL if forward else CONTRACT_LAST).astype(BF16))
        if not group:
            for load in dot_loads[1:]:
                load.wait()

        def one_tile(idx, carry):
            cols = pl.ds(pl.multiple_of(idx * tile, tile), tile)
            if forward and not group:
                for load in tile_loads(idx):
                    load.wait()
            if forward:
                gate = dot(rows_of(full), held[1][:, cols], MATMUL).astype(BF16)
                up = dot(rows_of(full), held[2][:, cols], MATMUL).astype(BF16)
                put(staged[1], cols, gate)
                put(staged[2], cols, up)
                if with_hidden:
                    put(staged[3], cols, gated(gate.astype(F32), up.astype(F32)).astype(BF16))
            else:
                d_hidden = dot(rows_of(full), held[1][cols, :], CONTRACT_LAST).astype(BF16).astype(F32)
                hidden, pull = jax.vjp(gated, rows_of(held[2], cols).astype(F32), rows_of(held[3], cols).astype(F32))
                d_gate, d_up = pull(d_hidden)
                put(staged[1], cols, hidden.astype(BF16))
                put(staged[2], cols, d_gate.astype(BF16))
                put(staged[3], cols, d_up.astype(BF16))
            return carry

        lax.fori_loop(0, n_tiles, one_tile, 0)
        sources = list(staged[:n_dots]) + ([] if forward else [full])
        for idx, source in enumerate(sources):
            for place, rows in enumerate(pieces):
                copy = pltpu.make_async_copy(source.at[rows], outs[idx].at[rows], store_sem.at[group, place, idx])
                copy.start()
                stores.append(copy)

    ring_gather(chips, loc_ref, full, send, recv, consume, attention if attn_group else None)
    for copy in stores:
        copy.wait()


def gather_dots(loc, inputs, layer, forward, with_hidden, tp_size, collective_id, name, attn_inputs=(), tile=256):
    n_rows, depth = loc.shape
    seq_len, chips = n_rows * tp_size, tp_size // CORES
    n_weights = 3 if forward else 2
    weights, saved = inputs[:n_weights], tuple(inputs[n_weights:]) + tuple(attn_inputs)
    if forward:
        widths = [weight.shape[2] for weight in weights] + ([weights[1].shape[2]] if with_hidden else [])
    else:
        widths = [weights[0].shape[1]] + [weights[1].shape[1]] * 3
    staged = [((seq_len, width), BF16) for width in widths]
    attn_group = weights[0].shape[1] // HEAD_DIM if attn_inputs else 0
    attn_outs = []
    if attn_inputs:
        attn_outs = [(attn_inputs[0].shape, BF16), ((seq_len, weights[0].shape[1]), BF16), ((seq_len, weights[0].shape[1]), F32)]
    outs = staged + ([] if forward else [((seq_len, depth), BF16)]) + attn_outs
    n_cols = sum(weight.size // (weight.shape[0] * depth) for weight in weights)
    all_inputs = tuple(inputs) + tuple(attn_inputs)
    return pl.pallas_call(
        functools.partial(gather_dots_kernel, chips, layer, forward, with_hidden, attn_group, tile, len(all_inputs), len(outs)),
        out_shape=[jax.ShapeDtypeStruct(*item) for item in outs],
        in_specs=[pl.BlockSpec(memory_space=pltpu.VMEM)] + [pl.BlockSpec(memory_space=pl.ANY)] * len(all_inputs),
        out_specs=[pl.BlockSpec(memory_space=pl.ANY)] * len(outs),
        scratch_shapes=[pltpu.VMEM((seq_len, depth), BF16)]
        + [pltpu.VMEM(weight.shape[1:], BF16) for weight in weights]
        + [pltpu.VMEM(item.shape, item.dtype) for item in saved]
        + [pltpu.VMEM(*item) for item in staged + attn_outs]
        + [
            pltpu.SemaphoreType.DMA((len(all_inputs), widths[1] // tile)),
            pltpu.SemaphoreType.DMA((5, 2 * CORES, len(outs))),
            pltpu.SemaphoreType.DMA((3,)),
            pltpu.SemaphoreType.DMA((17,)),
            pltpu.SemaphoreType.DMA((17,)),
        ],
        compiler_params=pltpu.CompilerParams(vmem_limit_bytes=VMEM_LIMIT, collective_id=collective_id, has_side_effects=True),
        cost_estimate=cost(2 * seq_len * depth * n_cols, 2 * (seq_len * depth + depth * n_cols + seq_len * n_cols)),
        name=name,
    )(loc, *all_inputs)


def weight_grads(u_ref, rhs_refs, grad_refs, u_held, grads_held, u_sem, grad_sem):
    tile = u_held.shape[2]
    n_tiles = u_ref.shape[1] // tile
    starts = [sum(rhs.shape[1] for rhs in rhs_refs[:idx]) for idx in range(len(rhs_refs))]

    def load(idx, slot):
        return pltpu.make_async_copy(u_ref.at[:, pl.ds(pl.multiple_of(idx * tile, tile), tile)], u_held.at[slot], u_sem.at[slot])

    def stores(idx, slot):
        rows = pl.ds(pl.multiple_of(idx * tile, tile), tile)
        return [
            pltpu.make_async_copy(grads_held.at[slot, :, pl.ds(start, rhs.shape[1])], grad.at[rows, :], grad_sem.at[slot, place])
            for place, (start, rhs, grad) in enumerate(zip(starts, rhs_refs, grad_refs))
        ]

    load(0, 0).start()

    def one_tile(idx, carry):
        slot = lax.rem(idx, 2)

        @pl.when(idx + 1 < n_tiles)
        def _():
            load(idx + 1, 1 - slot).start()

        @pl.when(idx >= 2)
        def _():
            for store in stores(idx - 2, slot):
                store.wait()

        load(idx, slot).wait()
        lhs = u_held[slot]
        for start, rhs in zip(starts, rhs_refs):
            grads_held[slot, :, pl.ds(start, rhs.shape[1])] = dot(lhs, rhs[...], CONTRACT_FIRST).astype(BF16)
        for store in stores(idx, slot):
            store.start()
        return carry

    lax.fori_loop(0, n_tiles, one_tile, 0)
    for idx in range(max(n_tiles - 2, 0), n_tiles):
        for store in stores(idx, idx % 2):
            store.wait()


def dots_scatter_kernel(chips, layer, dims, n_terms, n_rows_in, tile, with_grads, *refs):
    lhs_hbm, rhs_refs, refs = refs[:n_terms], refs[n_terms:2 * n_terms], refs[2 * n_terms:]
    rows_hbm, gain_ref, refs = refs[:n_rows_in], refs[n_rows_in], refs[n_rows_in + 1:]
    if with_grads:
        u_ref, refs = refs[0], refs[1:]
    out_ref, side_out_ref, refs = refs[0], refs[1], refs[2:]
    if with_grads:
        grad_refs, refs = refs[:n_terms], refs[n_terms:]
    lhs_refs, held, rows_in, row_sem, scratch = refs[:n_terms], refs[n_terms:2 * n_terms], refs[2 * n_terms:2 * n_terms + n_rows_in], refs[2 * n_terms + n_rows_in], refs[2 * n_terms + n_rows_in + 1:]
    part, acc, from_far, from_side, lhs_sem, load_sem, core_send, core_recv, send, recv = scratch[:10]
    n_rows, n_cols = out_ref.shape
    half = n_cols // 2
    n_tiles = half // tile
    chip, core, (partner, left, right) = ring_place(chips)
    dest_chips = [lax.rem(chip + offset, chips) for offset in (2, chips - 1, 1, 0)]

    chip_rows = CORES * n_rows

    def rows_of(step):
        return pl.ds(pl.multiple_of(dest_chips[step] * chip_rows, chip_rows), chip_rows)

    def cols_of(which, idx):
        return pl.ds(pl.multiple_of(which * half + idx * tile, tile), tile)

    def lhs_loads(step):
        return [pltpu.make_async_copy(src.at[rows_of(step)], dst.at[rows_of(step)], lhs_sem.at[step, place]) for place, (src, dst) in enumerate(zip(lhs_hbm, lhs_refs))]

    def rhs_loads(which, idx):
        cols = cols_of(which, idx)
        if dims is MATMUL:
            pairs = [(src.at[layer, :, cols], dst.at[:, cols]) for src, dst in zip(rhs_refs, held)]
        else:
            pairs = [(src.at[layer, cols, :], dst.at[cols, :]) for src, dst in zip(rhs_refs, held)]
        return [pltpu.make_async_copy(src, dst, load_sem.at[which * n_tiles + idx, place]) for place, (src, dst) in enumerate(pairs)]

    for load in lhs_loads(0):
        load.start()
    for idx in range(n_tiles):
        for which in range(2):
            for load in rhs_loads(which, idx):
                load.start()
    for step in range(1, 4):
        for load in lhs_loads(step):
            load.start()
    row_loads = [pltpu.make_async_copy(src, dst, row_sem.at[idx]) for idx, (src, dst) in enumerate(zip(rows_hbm, rows_in))]
    for load in row_loads:
        load.start()
    enter_ring((partner, left, right))

    def to_core(step, which, idx):
        slot = which * n_tiles + idx
        return remote(part.at[which, 1 - core], acc.at[step, slot], core_send, core_recv, step * 2 * n_tiles + slot, partner)

    def hop(step, which, idx):
        slot = which * n_tiles + idx
        if not step:
            return remote(acc.at[0, slot], from_far.at[slot], send, recv, slot, left if which else right)
        side = 1 if step == 1 else 0
        return remote(acc.at[step, slot], from_side.at[side, slot], send, recv, step * 2 * n_tiles + slot, left if side else right)

    def compute(step, which, idx):
        rows, rhs_cols = rows_of(step), cols_of(which, idx)
        if not step:
            for load in rhs_loads(which, idx):
                load.wait()
        total = None
        for lhs_ref, rhs_ref in zip(lhs_refs, held):
            rhs = rhs_ref[:, rhs_cols] if dims is MATMUL else rhs_ref[rhs_cols, :]
            product = dot(lhs_ref[rows, :], rhs, dims)
            total = product if total is None else total + product
        for idx_core in range(CORES):
            part[which, idx_core] = total[idx_core * n_rows:(idx_core + 1) * n_rows]
        to_core(step, which, idx).start()

    def add_core(step, which, idx, hop_now):
        copy = to_core(step, which, idx)
        copy.wait_recv()
        slot = which * n_tiles + idx
        acc[step, slot] = acc[step, slot] + part[which, core]
        copy.wait_send()
        if hop_now:
            hop(step, which, idx).start()

    for first, second, hop_now in (((0, 0), (0, 1), True), ((1, 0), (2, 1), True), ((2, 0), (1, 1), False), ((3, 0), (3, 1), False)):
        for step in {first[0]: 0, second[0]: 0} if hop_now else ():
            for load in lhs_loads(step):
                load.wait()
        if first[0] == 3:
            for load in lhs_loads(3):
                load.wait()

        def one_pair(idx, carry):
            compute(*first, idx)

            @pl.when(idx > 0)
            def _():
                add_core(*second, idx - 1, hop_now)

            compute(*second, idx)
            add_core(*first, idx, hop_now)
            return carry

        lax.fori_loop(0, n_tiles, one_pair, 0)
        add_core(*second, n_tiles - 1, hop_now)

    def pass_on(idx, carry):
        for step, which in ((2, 0), (1, 1)):
            slot = which * n_tiles + idx
            hop(0, which, idx).wait_recv()
            acc[step, slot] = acc[step, slot] + from_far[slot]
            hop(step, which, idx).start()
        return carry

    lax.fori_loop(0, n_tiles, pass_on, 0)
    if with_grads:
        weight_grads(u_ref, lhs_refs, grad_refs, *scratch[10:])
    for load in row_loads:
        load.wait()
    for which in range(2):
        for idx in range(n_tiles):
            hop(1, which, idx).wait_recv()
            hop(2, which, idx).wait_recv()
    if n_rows_in > 1:
        side_out_ref[...] = jnp.zeros_like(side_out_ref)

    def finish(idx, carry):
        rows = pl.ds(pl.multiple_of(idx * FINISH_ROWS, FINISH_ROWS), FINISH_ROWS)
        total = jnp.concatenate([acc[3, slot, rows, :] + from_side[0, slot, rows, :] + from_side[1, slot, rows, :] for slot in range(2 * n_tiles)], axis=1)
        x_rows = rows_in[0][rows, :].astype(F32)
        if n_rows_in == 1:
            x_next = (x_rows + total).astype(BF16)
            out_ref[rows, :] = x_next
            side_out_ref[rows, :] = rms_scale(x_next.astype(F32), gain_ref[...]).astype(BF16)
        else:
            d_x, gain_grad = jax.vjp(rms_scale, x_rows, gain_ref[...])[1](total.astype(BF16).astype(F32))
            out_ref[rows, :] = (rows_in[1][rows, :].astype(F32) + d_x).astype(BF16)
            side_out_ref[...] += gain_grad
        return carry

    lax.fori_loop(0, n_rows // FINISH_ROWS, finish, 0)
    for step in range(3):
        for which in range(2):
            for idx in range(n_tiles):
                hop(step, which, idx).wait_send()


def dots_scatter(terms, layer, dims, rows_in, gain_row, tp_size, collective_id, name, u_full=None, tile=512, grad_tile=512):
    seq_len = terms[0][0].shape[0]
    n_cols = terms[0][1].shape[2] if dims is MATMUL else terms[0][1].shape[1]
    n_rows = seq_len // tp_size
    depth = sum(lhs.shape[1] for lhs, _ in terms)
    with_grads = u_full is not None
    n_terms = len(terms)
    any_spec, vmem_spec = pl.BlockSpec(memory_space=pl.ANY), pl.BlockSpec(memory_space=pltpu.VMEM)
    side_out = jax.ShapeDtypeStruct((n_rows, n_cols), BF16) if len(rows_in) == 1 else jax.ShapeDtypeStruct((1, n_cols), F32)
    outs, extra_inputs, extra_scratch = [jax.ShapeDtypeStruct((n_rows, n_cols), BF16), side_out], (), []
    if with_grads:
        outs += [jax.ShapeDtypeStruct((n_cols, lhs.shape[1]), BF16) for lhs, _ in terms]
        extra_inputs = (u_full,)
        extra_scratch = [
            pltpu.VMEM((2, seq_len, grad_tile), BF16),
            pltpu.VMEM((2, grad_tile, depth), BF16),
            pltpu.SemaphoreType.DMA((2,)),
            pltpu.SemaphoreType.DMA((2, n_terms)),
        ]
    results = pl.pallas_call(
        functools.partial(dots_scatter_kernel, tp_size // CORES, layer, dims, n_terms, len(rows_in), tile, with_grads),
        out_shape=outs,
        in_specs=[any_spec] * (2 * n_terms + len(rows_in)) + [vmem_spec] + [any_spec] * len(extra_inputs),
        out_specs=[vmem_spec] * 2 + [any_spec] * (len(outs) - 2),
        scratch_shapes=[pltpu.VMEM(lhs.shape, BF16) for lhs, _ in terms]
        + [pltpu.VMEM(rhs.shape[1:], BF16) for _, rhs in terms]
        + [pltpu.VMEM((n_rows, n_cols), BF16)] * len(rows_in)
        + [
            pltpu.SemaphoreType.DMA((len(rows_in),)),
            pltpu.VMEM((2, CORES, n_rows, tile), F32),
            pltpu.VMEM((4, n_cols // tile, n_rows, tile), F32),
            pltpu.VMEM((n_cols // tile, n_rows, tile), F32),
            pltpu.VMEM((2, n_cols // tile, n_rows, tile), F32),
            pltpu.SemaphoreType.DMA((4, n_terms)),
            pltpu.SemaphoreType.DMA((n_cols // tile, n_terms)),
            pltpu.SemaphoreType.DMA((4 * n_cols // tile,)),
            pltpu.SemaphoreType.DMA((4 * n_cols // tile,)),
            pltpu.SemaphoreType.DMA((3 * n_cols // tile,)),
            pltpu.SemaphoreType.DMA((3 * n_cols // tile,)),
        ]
        + extra_scratch,
        compiler_params=pltpu.CompilerParams(vmem_limit_bytes=VMEM_LIMIT, collective_id=collective_id, has_side_effects=True),
        cost_estimate=cost(2 * seq_len * depth * n_cols * (2 if with_grads else 1), 2 * depth * (seq_len + n_cols) + 4 * n_rows * n_cols),
        name=name,
    )(*[lhs for lhs, _ in terms], *[rhs for _, rhs in terms], *rows_in, gain_row, *extra_inputs)
    return results[0], results[1], tuple(results[2:])


def gather_rows(rows_loc):
    return lax.all_gather(rows_loc, 'tp', axis=0, tiled=True)


def after(value, *others):
    return lax.optimization_barrier((value,) + others)[0]


def solution(mesh):
    tp_size = mesh.shape['tp']
    row_spec = P(('dp', 'tp'), None)
    col_spec = P(None, None, 'tp')
    inner_spec = P(None, 'tp', None)

    def sum_over_tp(value):
        stride = 1
        while stride < tp_size:
            value = value + lax.ppermute(value, 'tp', [(idx, idx ^ stride) for idx in range(tp_size)])
            stride *= 2
        return value

    def device_program(x_loc, dy_loc, norm_gain, w_qkv, w_out, w_gate, w_up, w_down):
        n_layers, depth = w_qkv.shape[0], w_qkv.shape[1]
        group = w_out.shape[1] // HEAD_DIM
        seq_len = x_loc.shape[0] * tp_size
        cos_tab, sin_tab = rope_tables(seq_len)
        saved_all = []
        x_cur = x_loc
        u_loc = rms_scale(x_loc.astype(F32), norm_gain[0]).astype(BF16)
        for layer in range(n_layers):
            last = layer == n_layers - 1
            outs = gather_dots(u_loc, (w_qkv, w_gate, w_up), layer, True, not last, tp_size, layer, "gather_in")
            qkv, gate, up = outs[:3]
            rot, attn_out, lse = (qkv, None, None) if last else attn_fwd(qkv, cos_tab, sin_tab, group)
            saved_all.append((x_cur, u_loc, rot, attn_out, lse, gate, up))
            if not last:
                terms = [(attn_out, w_out), (outs[3], w_down)]
                x_cur, u_loc, _ = dots_scatter(terms, layer, MATMUL, (x_cur,), norm_gain[layer + 1:layer + 2], tp_size, n_layers + layer, "scatter_out")

        out_grads, gain_grads, done_grads = (), [], []
        for layer in reversed(range(n_layers)):
            x_in, u_loc, rot, attn_out, lse, gate, up = saved_all[layer]
            last = layer == n_layers - 1
            attn_inputs = (rot, cos_tab, sin_tab) if last else ()
            outs = gather_dots(dy_loc, (w_out, w_down, gate, up), layer, False, True, tp_size, 2 * n_layers + layer, "gather_back", attn_inputs)
            d_attn, hidden, d_gate, d_up, dy_full = outs[:5]
            if last:
                rot, attn_out, lse = outs[5:]
            u_full = gather_rows(after(u_loc, attn_out, d_attn))
            d_qkv = attn_bwd(rot, lse, d_attn, cos_tab, sin_tab, group)
            out_grads = grad_out(attn_out, hidden, dy_full, layer, n_layers, out_grads)
            d_qkv, u_full, out_grads = lax.optimization_barrier((d_qkv, u_full, out_grads))
            terms = [(d_qkv, w_qkv), (d_gate, w_gate), (d_up, w_up)]
            dy_loc, gain_grad, done = dots_scatter(
                terms, layer, CONTRACT_LAST, (x_in, dy_loc), norm_gain[layer:layer + 1], tp_size, 3 * n_layers + layer, "scatter_back", u_full if layer else None
            )
            gain_grads.insert(0, gain_grad)
            if layer:
                done_grads.insert(0, done)
            else:
                gain_grads[0], u_full, d_qkv, d_gate, d_up = lax.optimization_barrier((gain_grad, u_full, d_qkv, d_gate, d_up))
                in_grads = grad_in(u_full, (d_qkv, d_gate, d_up), done_grads)
        grad_gain = sum_over_tp(jnp.concatenate(gain_grads))
        return (dy_loc, grad_gain, in_grads[0], out_grads[0], in_grads[1], in_grads[2], out_grads[1])

    return jax.shard_map(device_program, mesh=mesh, in_specs=(row_spec, row_spec, P(None, None), col_spec, inner_spec, col_spec, col_spec, inner_spec), out_specs=(row_spec, P('dp', None), P('dp', None, 'tp'), P('dp', 'tp', None), P('dp', None, 'tp'), P('dp', None, 'tp'), P('dp', 'tp', None)), check_vma=False)
```

```python
import functools

import jax
import jax.numpy as jnp
import numpy as np
from jax import lax
from jax.experimental import pallas as pl
from jax.experimental.pallas import tpu as pltpu
from jax.sharding import PartitionSpec as P

HEAD_DIM = 128
NORM_EPS = 1e-5
ROPE_BASE = 10000.0
Q_BLOCK = 256
FINISH_ROWS = 32
VMEM_LIMIT = 63 * 1024 * 1024
F32 = jnp.float32
BF16 = jnp.bfloat16

CONTRACT_LAST = (((1,), (1,)), ((), ()))
CONTRACT_FIRST = (((0,), (0,)), ((), ()))
MATMUL = (((1,), (0,)), ((), ()))


def dot(lhs, rhs, dims):
    return lax.dot_general(lhs, rhs, dims, preferred_element_type=F32)


def params():
    return pltpu.CompilerParams(vmem_limit_bytes=VMEM_LIMIT)


def cost(flops, bytes_accessed, transcendentals=0):
    return pl.CostEstimate(flops=int(flops), bytes_accessed=int(bytes_accessed), transcendentals=int(transcendentals))


def rope_tables(seq_len):
    half_dim = HEAD_DIM // 2
    freqs = (ROPE_BASE ** (-2.0 * np.arange(half_dim) / HEAD_DIM)).astype(np.float32)
    angles = (np.arange(seq_len, dtype=np.float32)[:, None] * freqs[None, :]).astype(np.float64)
    cos, sin = np.cos(angles).astype(np.float32), np.sin(angles).astype(np.float32)
    return jnp.asarray(np.concatenate([cos, cos], axis=-1)), jnp.asarray(np.concatenate([-sin, sin], axis=-1))


def rms_scale(x_f32, gain_row):
    inv_rms = lax.rsqrt(jnp.mean(x_f32 * x_f32, axis=-1, keepdims=True) + NORM_EPS)
    return x_f32 * inv_rms * gain_row


def gated(gate_f32, up_f32):
    return jax.nn.silu(gate_f32) * up_f32


def head_cols(index):
    return pl.ds(pl.multiple_of(index * HEAD_DIM, HEAD_DIM), HEAD_DIM)


def diagonal_mask():
    return lax.broadcasted_iota(jnp.int32, (Q_BLOCK, Q_BLOCK), 0) >= lax.broadcasted_iota(jnp.int32, (Q_BLOCK, Q_BLOCK), 1)


def attn_fwd_kernel(group, qkv_ref, cos_ref, sin_ref, rot_ref, out_ref, lse_ref):
    seq_len = qkv_ref.shape[0]
    scale = HEAD_DIM ** -0.5
    key, val = pl.ds(group * HEAD_DIM, HEAD_DIM), pl.ds((group + 1) * HEAD_DIM, HEAD_DIM)

    def rotate_head(head, carry):
        values = qkv_ref[:, head_cols(head)].astype(F32)
        rot_ref[:, head_cols(head)] = (values * cos_ref[...] + pltpu.roll(values, HEAD_DIM // 2, 1) * sin_ref[...]).astype(BF16)
        return carry

    lax.fori_loop(0, group + 1, rotate_head, 0)
    rot_ref[:, val] = qkv_ref[:, val]
    for block in range(seq_len // Q_BLOCK):
        start = block * Q_BLOCK
        rows = pl.ds(start, Q_BLOCK)

        def one_head(head, carry):
            query = rot_ref[rows, head_cols(head)]
            diag = jnp.where(diagonal_mask(), dot(query, rot_ref[rows, key], CONTRACT_LAST) * scale, -1e30)
            row_max = jnp.max(diag, axis=-1, keepdims=True)
            if start:
                past = dot(query, rot_ref[pl.ds(0, start), key], CONTRACT_LAST) * scale
                row_max = jnp.maximum(row_max, jnp.max(past, axis=-1, keepdims=True))
            diag = jnp.exp(diag - row_max)
            total = jnp.sum(diag, axis=-1, keepdims=True)
            if start:
                past = jnp.exp(past - row_max)
                total = total + jnp.sum(past, axis=-1, keepdims=True)
            inverse = 1.0 / total
            acc = dot((diag * inverse).astype(BF16), rot_ref[rows, val], MATMUL)
            if start:
                acc = acc + dot((past * inverse).astype(BF16), rot_ref[pl.ds(0, start), val], MATMUL)
            out_ref[rows, head_cols(head)] = acc.astype(BF16)
            lse_ref[rows, head_cols(head)] = jnp.broadcast_to(row_max + jnp.log(total), (Q_BLOCK, HEAD_DIM))
            return carry

        lax.fori_loop(0, group, one_head, 0)


def attn_fwd(qkv, cos_tab, sin_tab, group):
    seq_len = qkv.shape[0]
    pairs = group * seq_len * seq_len
    return pl.pallas_call(
        functools.partial(attn_fwd_kernel, group),
        out_shape=(
            jax.ShapeDtypeStruct(qkv.shape, BF16),
            jax.ShapeDtypeStruct((seq_len, group * HEAD_DIM), BF16),
            jax.ShapeDtypeStruct((seq_len, group * HEAD_DIM), F32),
        ),
        compiler_params=params(),
        cost_estimate=cost(4 * pairs * HEAD_DIM, 8 * qkv.size, pairs // 2),
        name="attn_fwd",
    )(qkv, cos_tab, sin_tab)


def attn_bwd_kernel(group, rot_ref, lse_ref, dout_ref, cos_ref, sin_ref, dqkv_ref, dkey_ref, dval_ref):
    seq_len = rot_ref.shape[0]
    scale = HEAD_DIM ** -0.5
    key, val = pl.ds(group * HEAD_DIM, HEAD_DIM), pl.ds((group + 1) * HEAD_DIM, HEAD_DIM)
    dkey_ref[...] = jnp.zeros_like(dkey_ref)
    dval_ref[...] = jnp.zeros_like(dval_ref)

    def unrotate(values, rows):
        values = values.astype(BF16).astype(F32)
        return (values * cos_ref[rows, :] - pltpu.roll(values, HEAD_DIM // 2, 1) * sin_ref[rows, :]).astype(BF16)

    for block in range(seq_len // Q_BLOCK):
        start = block * Q_BLOCK
        rows = pl.ds(start, Q_BLOCK)

        def one_head(head, carry):
            query = rot_ref[rows, head_cols(head)]
            dout = dout_ref[rows, head_cols(head)]
            lse = lse_ref[rows, head_cols(head)][:, :1]

            def probs(cols, masked):
                scores = dot(query, rot_ref[cols, key], CONTRACT_LAST) * scale
                if masked:
                    scores = jnp.where(diagonal_mask(), scores, -1e30)
                prob = jnp.exp(scores - lse)
                dprob = dot(dout, rot_ref[cols, val], CONTRACT_LAST).astype(BF16).astype(F32)
                dval_ref[cols, :] += dot(prob.astype(BF16), dout, CONTRACT_FIRST)
                return prob, dprob, jnp.sum(prob * dprob, axis=-1, keepdims=True)

            def finish(cols, prob, dprob, delta):
                dscore = (prob * (dprob - delta) * scale).astype(BF16)
                dkey_ref[cols, :] += dot(dscore, query, CONTRACT_FIRST)
                return dot(dscore, rot_ref[cols, key], MATMUL)

            prob, dprob, delta = probs(rows, True)
            if start:
                past = pl.ds(0, start)
                past_prob, past_dprob, past_delta = probs(past, False)
                delta = delta + past_delta
            dquery = finish(rows, prob, dprob, delta)
            if start:
                dquery = dquery + finish(past, past_prob, past_dprob, delta)
            dqkv_ref[rows, head_cols(head)] = unrotate(dquery, rows)
            return carry

        lax.fori_loop(0, group, one_head, 0)
    dqkv_ref[:, key] = unrotate(dkey_ref[...], pl.ds(0, seq_len))
    dqkv_ref[:, val] = dval_ref[...].astype(BF16)


def attn_bwd(rot, lse, dout, cos_tab, sin_tab, group):
    seq_len = rot.shape[0]
    pairs = group * seq_len * seq_len
    return pl.pallas_call(
        functools.partial(attn_bwd_kernel, group),
        out_shape=jax.ShapeDtypeStruct(rot.shape, BF16),
        scratch_shapes=[pltpu.VMEM((seq_len, HEAD_DIM), F32)] * 2,
        compiler_params=params(),
        cost_estimate=cost(10 * pairs * HEAD_DIM, 8 * rot.size, pairs // 2),
        name="attn_bwd",
    )(rot, lse, dout, cos_tab, sin_tab)


def grad_in_kernel(n_rhs, *refs):
    lhs = refs[0][...]
    rhs_refs, done_refs, out_refs = refs[1:1 + n_rhs], refs[1 + n_rhs:-n_rhs], refs[-n_rhs:]
    for idx, (rhs_ref, out_ref) in enumerate(zip(rhs_refs, out_refs)):
        out_ref[0] = dot(lhs, rhs_ref[...], CONTRACT_FIRST).astype(BF16)
        for place, done_ref in enumerate(done_refs[idx::n_rhs]):
            out_ref[1 + place] = done_ref[...]


def grad_in(lhs, rhs_list, done, tile=512):
    seq_len, depth = lhs.shape
    n_rhs, n_layers = len(rhs_list), 1 + len(done)
    width = sum(rhs.shape[1] for rhs in rhs_list)
    return pl.pallas_call(
        functools.partial(grad_in_kernel, n_rhs),
        out_shape=[jax.ShapeDtypeStruct((n_layers, depth, rhs.shape[1]), BF16) for rhs in rhs_list],
        grid=(depth // tile,),
        in_specs=[pl.BlockSpec((seq_len, tile), lambda step: (0, step))]
        + [pl.BlockSpec(rhs.shape, lambda step: (0, 0), pipeline_mode=pl.Buffered(1)) for rhs in rhs_list]
        + [pl.BlockSpec((tile, item.shape[1]), lambda step: (step, 0)) for layer_done in done for item in layer_done],
        out_specs=[pl.BlockSpec((n_layers, tile, rhs.shape[1]), lambda step: (0, step, 0)) for rhs in rhs_list],
        compiler_params=params(),
        cost_estimate=cost(2 * seq_len * depth * width, 2 * (seq_len * depth + seq_len * width + (2 * n_layers - 1) * depth * width)),
        name="grad_in",
    )(lhs, *rhs_list, *[item for layer_done in done for item in layer_done])


def grad_out_kernel(attn_ref, hidden_ref, dy_ref, *refs):
    out_ref, down_ref = refs[-2:]

    @pl.when(pl.program_id(0) == 0)
    def _():
        out_ref[...] = dot(attn_ref[...], dy_ref[...], CONTRACT_FIRST).astype(BF16)

    down_ref[...] = dot(hidden_ref[...], dy_ref[...], CONTRACT_FIRST).astype(BF16)


def grad_out(attn_out, hidden, dy_full, layer, n_layers, previous, tile=512):
    seq_len, depth = dy_full.shape
    heads, ff = attn_out.shape[1], hidden.shape[1]
    return pl.pallas_call(
        grad_out_kernel,
        out_shape=(jax.ShapeDtypeStruct((n_layers, heads, depth), BF16), jax.ShapeDtypeStruct((n_layers, ff, depth), BF16)),
        grid=(ff // tile,),
        in_specs=[
            pl.BlockSpec((seq_len, heads), lambda step: (0, 0)),
            pl.BlockSpec((seq_len, tile), lambda step: (0, step)),
            pl.BlockSpec((seq_len, depth), lambda step: (0, 0), pipeline_mode=pl.Buffered(1)),
        ]
        + [pl.BlockSpec(memory_space=pl.ANY) for _ in previous],
        out_specs=[
            pl.BlockSpec((None, heads, depth), lambda step: (layer, 0, 0)),
            pl.BlockSpec((None, tile, depth), lambda step: (layer, step, 0)),
        ],
        input_output_aliases={3: 0, 4: 1} if previous else {},
        compiler_params=params(),
        cost_estimate=cost(2 * seq_len * depth * (heads + ff), 2 * (seq_len * depth + (seq_len + depth) * (heads + ff))),
        name="grad_out",
    )(attn_out, hidden, dy_full, *previous)


MESH = pl.DeviceIdType.MESH
CORES = 2


def ring_place(chips):
    me = lax.axis_index('tp')
    chip, core = me // CORES, lax.rem(me, CORES)
    left, right = lax.rem(chip + chips - 1, chips), lax.rem(chip + 1, chips)
    return chip, core, (chip * CORES + 1 - core, left * CORES + core, right * CORES + core)


def enter_ring(peers):
    barrier = pltpu.get_barrier_semaphore()
    for peer in peers:
        pl.semaphore_signal(barrier, inc=1, device_id={'tp': peer}, device_id_type=MESH)
    pl.semaphore_wait(barrier, len(peers))


def remote(src, dst, send, recv, index, peer):
    return pltpu.make_async_remote_copy(src_ref=src, dst_ref=dst, send_sem=send.at[index], recv_sem=recv.at[index], device_id={'tp': peer}, device_id_type=MESH)


def ring_gather(chips, loc_ref, full, send, recv, consume, meanwhile=None):
    n_rows = loc_ref.shape[0]
    half, quarter = n_rows // 2, n_rows // 4
    chip, core, (partner, left, right) = ring_place(chips)
    left_chip, right_chip, far_chip = lax.rem(chip + chips - 1, chips), lax.rem(chip + 1, chips), lax.rem(chip + 2, chips)

    def first_row(core_idx, item):
        return pl.multiple_of((item[0] * CORES + core_idx) * n_rows + item[1], item[2])

    def piece(core_idx, item):
        return full.at[pl.ds(first_row(core_idx, item), item[2])]

    low, high = (chip, 0, half), (chip, half, half)
    received = [
        (left_chip, 0, half), (right_chip, half, half), (left_chip, half, half), (right_chip, 0, half),
        (far_chip, 0, quarter), (far_chip, half, quarter), (far_chip, quarter, quarter), (far_chip, half + quarter, quarter),
    ]
    passed_on = [(left_chip, 0, quarter), (right_chip, half, quarter), (left_chip, quarter, quarter), (right_chip, half + quarter, quarter)]
    sends = [
        remote(loc_ref.at[pl.ds(item[1], half)], piece(core, item), send, recv, idx, peer)
        for idx, (item, peer) in enumerate([(low, right), (high, left), (high, right), (low, left)])
    ]
    sends += [remote(piece(core, item), piece(core, item), send, recv, 4 + idx, (right, left)[idx % 2]) for idx, item in enumerate(passed_on)]
    sends += [remote(piece(core, item), piece(core, item), send, recv, 8 + idx, partner) for idx, item in enumerate(received)]
    own = full.at[pl.ds(pl.multiple_of((chip * CORES + core) * n_rows, n_rows), n_rows)]
    other = full.at[pl.ds(pl.multiple_of((chip * CORES + 1 - core) * n_rows, n_rows), n_rows)]
    sends.append(remote(loc_ref, own, send, recv, 16, partner))
    landing = [piece(core, item) for item in received] + [piece(1 - core, item) for item in received] + [other]

    def arrived(index):
        remote(landing[index], landing[index], send, recv, index, partner).wait_recv()

    def hand_over(*indices):
        for index in indices:
            arrived(index)
            if index < 2:
                sends[4 + index].start()
                sends[6 + index].start()
            sends[8 + index].start()

    def use(group, items):
        consume(group, [first_row(idx, item) for item in items for idx in range(CORES)], items[0][2])

    enter_ring((partner, left, right))
    for index in (0, 1, 2, 3, 16):
        sends[index].start()
    own[...] = loc_ref[...]
    if meanwhile is not None:
        meanwhile()
        hand_over(0, 1)
    arrived(16)
    use(0, (low, high))
    if meanwhile is None:
        hand_over(0, 1)
    for group in range(1, 5):
        pair = (2 * group - 2, 2 * group - 1)
        if group > 1:
            hand_over(*pair)
        for index in pair:
            arrived(8 + index)
        use(group, received[2 * group - 2:2 * group])
    for copy in sends:
        copy.wait_send()


def gather_dots_kernel(chips, layer, forward, with_hidden, attn_group, tile, n_inputs, n_outs, loc_ref, *refs):
    n_weights = 3 if forward else 2
    inputs, outs = refs[:n_inputs], refs[n_inputs:n_inputs + n_outs]
    full, scratch = refs[n_inputs + n_outs], refs[n_inputs + n_outs + 1:]
    held, staged = scratch[:n_inputs], scratch[n_inputs:-5]
    load_sem, store_sem, attn_sem, send, recv = scratch[-5:]
    n_tiles = staged[1].shape[1] // tile
    n_whole = 1 if forward else n_inputs
    loads = [
        pltpu.make_async_copy(src.at[layer] if idx < n_weights else src, dst, load_sem.at[idx, 0])
        for idx, (src, dst) in enumerate(zip(inputs[:n_whole], held[:n_whole]))
    ]

    def tile_loads(idx):
        cols = pl.ds(pl.multiple_of(idx * tile, tile), tile)
        return [pltpu.make_async_copy(inputs[place].at[layer, :, cols], held[place].at[:, cols], load_sem.at[place, idx]) for place in range(1, n_weights)]

    n_dots = n_weights + (1 if with_hidden else 0) if forward else 4
    attn_loads = loads[4:] if attn_group else []
    dot_loads = loads[:len(loads) - len(attn_loads)]
    for load in attn_loads + dot_loads:
        load.start()
    if forward:
        for idx in range(n_tiles):
            for load in tile_loads(idx):
                load.start()
    stores = []

    def attention():
        for load in attn_loads:
            load.wait()
        attn_fwd_kernel(attn_group, *held[4:], *staged[n_dots:])
        for idx, (src, dst) in enumerate(zip(staged[n_dots:], outs[-3:])):
            copy = pltpu.make_async_copy(src, dst, attn_sem.at[idx])
            copy.start()
            stores.append(copy)

    def consume(group, first_rows, count):
        pieces = [pl.ds(first, count) for first in first_rows]

        def rows_of(ref, cols=slice(None)):
            return jnp.concatenate([ref[rows, cols] for rows in pieces], axis=0)

        def put(ref, cols, value):
            for idx, rows in enumerate(pieces):
                ref[rows, cols] = value[idx * count:(idx + 1) * count]

        if not group:
            dot_loads[0].wait()
        put(staged[0], slice(None), dot(rows_of(full), held[0][...], MATMUL if forward else CONTRACT_LAST).astype(BF16))
        if not group:
            for load in dot_loads[1:]:
                load.wait()

        def one_tile(idx, carry):
            cols = pl.ds(pl.multiple_of(idx * tile, tile), tile)
            if forward and not group:
                for load in tile_loads(idx):
                    load.wait()
            if forward:
                gate = dot(rows_of(full), held[1][:, cols], MATMUL).astype(BF16)
                up = dot(rows_of(full), held[2][:, cols], MATMUL).astype(BF16)
                put(staged[1], cols, gate)
                put(staged[2], cols, up)
                if with_hidden:
                    put(staged[3], cols, gated(gate.astype(F32), up.astype(F32)).astype(BF16))
            else:
                d_hidden = dot(rows_of(full), held[1][cols, :], CONTRACT_LAST).astype(BF16).astype(F32)
                hidden, pull = jax.vjp(gated, rows_of(held[2], cols).astype(F32), rows_of(held[3], cols).astype(F32))
                d_gate, d_up = pull(d_hidden)
                put(staged[1], cols, hidden.astype(BF16))
                put(staged[2], cols, d_gate.astype(BF16))
                put(staged[3], cols, d_up.astype(BF16))
            return carry

        lax.fori_loop(0, n_tiles, one_tile, 0)
        sources = list(staged[:n_dots]) + ([] if forward else [full])
        for idx, source in enumerate(sources):
            for place, rows in enumerate(pieces):
                copy = pltpu.make_async_copy(source.at[rows], outs[idx].at[rows], store_sem.at[group, place, idx])
                copy.start()
                stores.append(copy)

    ring_gather(chips, loc_ref, full, send, recv, consume, attention if attn_group else None)
    for copy in stores:
        copy.wait()


def gather_dots(loc, inputs, layer, forward, with_hidden, tp_size, collective_id, name, attn_inputs=(), tile=512):
    n_rows, depth = loc.shape
    seq_len, chips = n_rows * tp_size, tp_size // CORES
    n_weights = 3 if forward else 2
    weights, saved = inputs[:n_weights], tuple(inputs[n_weights:]) + tuple(attn_inputs)
    if forward:
        widths = [weight.shape[2] for weight in weights] + ([weights[1].shape[2]] if with_hidden else [])
    else:
        widths = [weights[0].shape[1]] + [weights[1].shape[1]] * 3
    staged = [((seq_len, width), BF16) for width in widths]
    attn_group = weights[0].shape[1] // HEAD_DIM if attn_inputs else 0
    attn_outs = []
    if attn_inputs:
        attn_outs = [(attn_inputs[0].shape, BF16), ((seq_len, weights[0].shape[1]), BF16), ((seq_len, weights[0].shape[1]), F32)]
    outs = staged + ([] if forward else [((seq_len, depth), BF16)]) + attn_outs
    n_cols = sum(weight.size // (weight.shape[0] * depth) for weight in weights)
    all_inputs = tuple(inputs) + tuple(attn_inputs)
    return pl.pallas_call(
        functools.partial(gather_dots_kernel, chips, layer, forward, with_hidden, attn_group, tile, len(all_inputs), len(outs)),
        out_shape=[jax.ShapeDtypeStruct(*item) for item in outs],
        in_specs=[pl.BlockSpec(memory_space=pltpu.VMEM)] + [pl.BlockSpec(memory_space=pl.ANY)] * len(all_inputs),
        out_specs=[pl.BlockSpec(memory_space=pl.ANY)] * len(outs),
        scratch_shapes=[pltpu.VMEM((seq_len, depth), BF16)]
        + [pltpu.VMEM(weight.shape[1:], BF16) for weight in weights]
        + [pltpu.VMEM(item.shape, item.dtype) for item in saved]
        + [pltpu.VMEM(*item) for item in staged + attn_outs]
        + [
            pltpu.SemaphoreType.DMA((len(all_inputs), widths[1] // tile)),
            pltpu.SemaphoreType.DMA((5, 2 * CORES, len(outs))),
            pltpu.SemaphoreType.DMA((3,)),
            pltpu.SemaphoreType.DMA((17,)),
            pltpu.SemaphoreType.DMA((17,)),
        ],
        compiler_params=pltpu.CompilerParams(vmem_limit_bytes=VMEM_LIMIT, collective_id=collective_id, has_side_effects=True),
        cost_estimate=cost(2 * seq_len * depth * n_cols, 2 * (seq_len * depth + depth * n_cols + seq_len * n_cols)),
        name=name,
    )(loc, *all_inputs)


def weight_grads(u_ref, rhs_refs, grad_refs, u_held, grads_held, u_sem, grad_sem):
    tile = u_held.shape[2]
    n_tiles = u_ref.shape[1] // tile
    starts = [sum(rhs.shape[1] for rhs in rhs_refs[:idx]) for idx in range(len(rhs_refs))]

    def load(idx, slot):
        return pltpu.make_async_copy(u_ref.at[:, pl.ds(pl.multiple_of(idx * tile, tile), tile)], u_held.at[slot], u_sem.at[slot])

    def stores(idx, slot):
        rows = pl.ds(pl.multiple_of(idx * tile, tile), tile)
        return [
            pltpu.make_async_copy(grads_held.at[slot, :, pl.ds(start, rhs.shape[1])], grad.at[rows, :], grad_sem.at[slot, place])
            for place, (start, rhs, grad) in enumerate(zip(starts, rhs_refs, grad_refs))
        ]

    load(0, 0).start()

    def one_tile(idx, carry):
        slot = lax.rem(idx, 2)

        @pl.when(idx + 1 < n_tiles)
        def _():
            load(idx + 1, 1 - slot).start()

        @pl.when(idx >= 2)
        def _():
            for store in stores(idx - 2, slot):
                store.wait()

        load(idx, slot).wait()
        lhs = u_held[slot]
        for start, rhs in zip(starts, rhs_refs):
            grads_held[slot, :, pl.ds(start, rhs.shape[1])] = dot(lhs, rhs[...], CONTRACT_FIRST).astype(BF16)
        for store in stores(idx, slot):
            store.start()
        return carry

    lax.fori_loop(0, n_tiles, one_tile, 0)
    for idx in range(max(n_tiles - 2, 0), n_tiles):
        for store in stores(idx, idx % 2):
            store.wait()


def dots_scatter_kernel(chips, layer, dims, n_terms, n_rows_in, tile, with_grads, *refs):
    lhs_hbm, rhs_refs, refs = refs[:n_terms], refs[n_terms:2 * n_terms], refs[2 * n_terms:]
    rows_hbm, gain_ref, refs = refs[:n_rows_in], refs[n_rows_in], refs[n_rows_in + 1:]
    if with_grads:
        u_ref, refs = refs[0], refs[1:]
    out_ref, side_out_ref, refs = refs[0], refs[1], refs[2:]
    if with_grads:
        grad_refs, refs = refs[:n_terms], refs[n_terms:]
    lhs_refs, held, rows_in, row_sem, scratch = refs[:n_terms], refs[n_terms:2 * n_terms], refs[2 * n_terms:2 * n_terms + n_rows_in], refs[2 * n_terms + n_rows_in], refs[2 * n_terms + n_rows_in + 1:]
    part, acc, from_far, from_side, lhs_sem, load_sem, core_send, core_recv, send, recv = scratch[:10]
    n_rows, n_cols = out_ref.shape
    half = n_cols // 2
    n_tiles = half // tile
    chip, core, (partner, left, right) = ring_place(chips)
    dest_chips = [lax.rem(chip + offset, chips) for offset in (2, chips - 1, 1, 0)]

    chip_rows = CORES * n_rows

    def rows_of(step):
        return pl.ds(pl.multiple_of(dest_chips[step] * chip_rows, chip_rows), chip_rows)

    def cols_of(which, idx):
        return pl.ds(pl.multiple_of(which * half + idx * tile, tile), tile)

    def lhs_loads(step):
        return [pltpu.make_async_copy(src.at[rows_of(step)], dst.at[rows_of(step)], lhs_sem.at[step, place]) for place, (src, dst) in enumerate(zip(lhs_hbm, lhs_refs))]

    def rhs_loads(which, idx):
        cols = cols_of(which, idx)
        if dims is MATMUL:
            pairs = [(src.at[layer, :, cols], dst.at[:, cols]) for src, dst in zip(rhs_refs, held)]
        else:
            pairs = [(src.at[layer, cols, :], dst.at[cols, :]) for src, dst in zip(rhs_refs, held)]
        return [pltpu.make_async_copy(src, dst, load_sem.at[which * n_tiles + idx, place]) for place, (src, dst) in enumerate(pairs)]

    for load in lhs_loads(0):
        load.start()
    for idx in range(n_tiles):
        for which in range(2):
            for load in rhs_loads(which, idx):
                load.start()
    for step in range(1, 4):
        for load in lhs_loads(step):
            load.start()
    row_loads = [pltpu.make_async_copy(src, dst, row_sem.at[idx]) for idx, (src, dst) in enumerate(zip(rows_hbm, rows_in))]
    for load in row_loads:
        load.start()
    enter_ring((partner, left, right))

    def to_core(step, which, idx):
        slot = which * n_tiles + idx
        return remote(part.at[which, 1 - core], acc.at[step, slot], core_send, core_recv, step * 2 * n_tiles + slot, partner)

    def hop(step, which, idx):
        slot = which * n_tiles + idx
        if not step:
            return remote(acc.at[0, slot], from_far.at[slot], send, recv, slot, left if which else right)
        side = 1 if step == 1 else 0
        return remote(acc.at[step, slot], from_side.at[side, slot], send, recv, step * 2 * n_tiles + slot, left if side else right)

    def compute(step, which, idx):
        rows, rhs_cols = rows_of(step), cols_of(which, idx)
        if not step:
            for load in rhs_loads(which, idx):
                load.wait()
        total = None
        for lhs_ref, rhs_ref in zip(lhs_refs, held):
            rhs = rhs_ref[:, rhs_cols] if dims is MATMUL else rhs_ref[rhs_cols, :]
            product = dot(lhs_ref[rows, :], rhs, dims)
            total = product if total is None else total + product
        for idx_core in range(CORES):
            part[which, idx_core] = total[idx_core * n_rows:(idx_core + 1) * n_rows]
        to_core(step, which, idx).start()

    def add_core(step, which, idx, hop_now):
        copy = to_core(step, which, idx)
        copy.wait_recv()
        slot = which * n_tiles + idx
        acc[step, slot] = acc[step, slot] + part[which, core]
        copy.wait_send()
        if hop_now:
            hop(step, which, idx).start()

    for first, second, hop_now in (((0, 0), (0, 1), True), ((1, 0), (2, 1), True), ((2, 0), (1, 1), False), ((3, 0), (3, 1), False)):
        for step in {first[0]: 0, second[0]: 0} if hop_now else ():
            for load in lhs_loads(step):
                load.wait()
        if first[0] == 3:
            for load in lhs_loads(3):
                load.wait()

        def one_pair(idx, carry):
            compute(*first, idx)

            @pl.when(idx > 0)
            def _():
                add_core(*second, idx - 1, hop_now)

            compute(*second, idx)
            add_core(*first, idx, hop_now)
            return carry

        lax.fori_loop(0, n_tiles, one_pair, 0)
        add_core(*second, n_tiles - 1, hop_now)

    def pass_on(idx, carry):
        for step, which in ((2, 0), (1, 1)):
            slot = which * n_tiles + idx
            hop(0, which, idx).wait_recv()
            acc[step, slot] = acc[step, slot] + from_far[slot]
            hop(step, which, idx).start()
        return carry

    lax.fori_loop(0, n_tiles, pass_on, 0)
    if with_grads:
        weight_grads(u_ref, lhs_refs, grad_refs, *scratch[10:])
    for load in row_loads:
        load.wait()
    for which in range(2):
        for idx in range(n_tiles):
            hop(1, which, idx).wait_recv()
            hop(2, which, idx).wait_recv()
    if n_rows_in > 1:
        side_out_ref[...] = jnp.zeros_like(side_out_ref)

    def finish(idx, carry):
        rows = pl.ds(pl.multiple_of(idx * FINISH_ROWS, FINISH_ROWS), FINISH_ROWS)
        total = jnp.concatenate([acc[3, slot, rows, :] + from_side[0, slot, rows, :] + from_side[1, slot, rows, :] for slot in range(2 * n_tiles)], axis=1)
        x_rows = rows_in[0][rows, :].astype(F32)
        if n_rows_in == 1:
            x_next = (x_rows + total).astype(BF16)
            out_ref[rows, :] = x_next
            side_out_ref[rows, :] = rms_scale(x_next.astype(F32), gain_ref[...]).astype(BF16)
        else:
            d_x, gain_grad = jax.vjp(rms_scale, x_rows, gain_ref[...])[1](total.astype(BF16).astype(F32))
            out_ref[rows, :] = (rows_in[1][rows, :].astype(F32) + d_x).astype(BF16)
            side_out_ref[...] += gain_grad
        return carry

    lax.fori_loop(0, n_rows // FINISH_ROWS, finish, 0)
    for step in range(3):
        for which in range(2):
            for idx in range(n_tiles):
                hop(step, which, idx).wait_send()


def dots_scatter(terms, layer, dims, rows_in, gain_row, tp_size, collective_id, name, u_full=None, tile=512, grad_tile=512):
    seq_len = terms[0][0].shape[0]
    n_cols = terms[0][1].shape[2] if dims is MATMUL else terms[0][1].shape[1]
    n_rows = seq_len // tp_size
    depth = sum(lhs.shape[1] for lhs, _ in terms)
    with_grads = u_full is not None
    n_terms = len(terms)
    any_spec, vmem_spec = pl.BlockSpec(memory_space=pl.ANY), pl.BlockSpec(memory_space=pltpu.VMEM)
    side_out = jax.ShapeDtypeStruct((n_rows, n_cols), BF16) if len(rows_in) == 1 else jax.ShapeDtypeStruct((1, n_cols), F32)
    outs, extra_inputs, extra_scratch = [jax.ShapeDtypeStruct((n_rows, n_cols), BF16), side_out], (), []
    if with_grads:
        outs += [jax.ShapeDtypeStruct((n_cols, lhs.shape[1]), BF16) for lhs, _ in terms]
        extra_inputs = (u_full,)
        extra_scratch = [
            pltpu.VMEM((2, seq_len, grad_tile), BF16),
            pltpu.VMEM((2, grad_tile, depth), BF16),
            pltpu.SemaphoreType.DMA((2,)),
            pltpu.SemaphoreType.DMA((2, n_terms)),
        ]
    results = pl.pallas_call(
        functools.partial(dots_scatter_kernel, tp_size // CORES, layer, dims, n_terms, len(rows_in), tile, with_grads),
        out_shape=outs,
        in_specs=[any_spec] * (2 * n_terms + len(rows_in)) + [vmem_spec] + [any_spec] * len(extra_inputs),
        out_specs=[vmem_spec] * 2 + [any_spec] * (len(outs) - 2),
        scratch_shapes=[pltpu.VMEM(lhs.shape, BF16) for lhs, _ in terms]
        + [pltpu.VMEM(rhs.shape[1:], BF16) for _, rhs in terms]
        + [pltpu.VMEM((n_rows, n_cols), BF16)] * len(rows_in)
        + [
            pltpu.SemaphoreType.DMA((len(rows_in),)),
            pltpu.VMEM((2, CORES, n_rows, tile), F32),
            pltpu.VMEM((4, n_cols // tile, n_rows, tile), F32),
            pltpu.VMEM((n_cols // tile, n_rows, tile), F32),
            pltpu.VMEM((2, n_cols // tile, n_rows, tile), F32),
            pltpu.SemaphoreType.DMA((4, n_terms)),
            pltpu.SemaphoreType.DMA((n_cols // tile, n_terms)),
            pltpu.SemaphoreType.DMA((4 * n_cols // tile,)),
            pltpu.SemaphoreType.DMA((4 * n_cols // tile,)),
            pltpu.SemaphoreType.DMA((3 * n_cols // tile,)),
            pltpu.SemaphoreType.DMA((3 * n_cols // tile,)),
        ]
        + extra_scratch,
        compiler_params=pltpu.CompilerParams(vmem_limit_bytes=VMEM_LIMIT, collective_id=collective_id, has_side_effects=True),
        cost_estimate=cost(2 * seq_len * depth * n_cols * (2 if with_grads else 1), 2 * depth * (seq_len + n_cols) + 4 * n_rows * n_cols),
        name=name,
    )(*[lhs for lhs, _ in terms], *[rhs for _, rhs in terms], *rows_in, gain_row, *extra_inputs)
    return results[0], results[1], tuple(results[2:])


def gather_rows(rows_loc):
    return lax.all_gather(rows_loc, 'tp', axis=0, tiled=True)


def after(value, *others):
    return lax.optimization_barrier((value,) + others)[0]


def solution(mesh):
    tp_size = mesh.shape['tp']
    row_spec = P(('dp', 'tp'), None)
    col_spec = P(None, None, 'tp')
    inner_spec = P(None, 'tp', None)

    def sum_over_tp(value):
        stride = 1
        while stride < tp_size:
            value = value + lax.ppermute(value, 'tp', [(idx, idx ^ stride) for idx in range(tp_size)])
            stride *= 2
        return value

    def device_program(x_loc, dy_loc, norm_gain, w_qkv, w_out, w_gate, w_up, w_down):
        n_layers, depth = w_qkv.shape[0], w_qkv.shape[1]
        group = w_out.shape[1] // HEAD_DIM
        seq_len = x_loc.shape[0] * tp_size
        cos_tab, sin_tab = rope_tables(seq_len)
        saved_all = []
        x_cur = x_loc
        u_loc = rms_scale(x_loc.astype(F32), norm_gain[0]).astype(BF16)
        for layer in range(n_layers):
            last = layer == n_layers - 1
            outs = gather_dots(u_loc, (w_qkv, w_gate, w_up), layer, True, not last, tp_size, layer, "gather_in")
            qkv, gate, up = outs[:3]
            rot, attn_out, lse = (qkv, None, None) if last else attn_fwd(qkv, cos_tab, sin_tab, group)
            saved_all.append((x_cur, u_loc, rot, attn_out, lse, gate, up))
            if not last:
                terms = [(attn_out, w_out), (outs[3], w_down)]
                x_cur, u_loc, _ = dots_scatter(terms, layer, MATMUL, (x_cur,), norm_gain[layer + 1:layer + 2], tp_size, n_layers + layer, "scatter_out")

        out_grads, gain_grads, done_grads = (), [], []
        for layer in reversed(range(n_layers)):
            x_in, u_loc, rot, attn_out, lse, gate, up = saved_all[layer]
            last = layer == n_layers - 1
            attn_inputs = (rot, cos_tab, sin_tab) if last else ()
            outs = gather_dots(dy_loc, (w_out, w_down, gate, up), layer, False, True, tp_size, 2 * n_layers + layer, "gather_back", attn_inputs)
            d_attn, hidden, d_gate, d_up, dy_full = outs[:5]
            if last:
                rot, attn_out, lse = outs[5:]
            u_full = gather_rows(after(u_loc, attn_out, d_attn))
            d_qkv = attn_bwd(rot, lse, d_attn, cos_tab, sin_tab, group)
            out_grads = grad_out(attn_out, hidden, dy_full, layer, n_layers, out_grads)
            d_qkv, u_full, out_grads = lax.optimization_barrier((d_qkv, u_full, out_grads))
            terms = [(d_qkv, w_qkv), (d_gate, w_gate), (d_up, w_up)]
            dy_loc, gain_grad, done = dots_scatter(
                terms, layer, CONTRACT_LAST, (x_in, dy_loc), norm_gain[layer:layer + 1], tp_size, 3 * n_layers + layer, "scatter_back", u_full if layer else None
            )
            gain_grads.insert(0, gain_grad)
            if layer:
                done_grads.insert(0, done)
            else:
                gain_grads[0], u_full, d_qkv, d_gate, d_up = lax.optimization_barrier((gain_grad, u_full, d_qkv, d_gate, d_up))
                in_grads = grad_in(u_full, (d_qkv, d_gate, d_up), done_grads)
        grad_gain = sum_over_tp(jnp.concatenate(gain_grads))
        return (dy_loc, grad_gain, in_grads[0], out_grads[0], in_grads[1], in_grads[2], out_grads[1])

    return jax.shard_map(device_program, mesh=mesh, in_specs=(row_spec, row_spec, P(None, None), col_spec, inner_spec, col_spec, col_spec, inner_spec), out_specs=(row_spec, P('dp', None), P('dp', None, 'tp'), P('dp', 'tp', None), P('dp', None, 'tp'), P('dp', None, 'tp'), P('dp', 'tp', None)), check_vma=False)
```
